32 devices in a mesh: dp: 8 (over z, y), head: 4 (over x, core).
Axes of the slice: x: 2, y: 2, z: 4, core: 2. Of those that a mesh axis runs over, the one named last changes fastest.
Arguments:
- inputs: bfloat16 [8, 1024, 768], P('dp', 'head'), may hold values from -6 to 6
- norm_gains: bfloat16 [2, 768], replicated, may hold values from 0.5 to 1.5
- norm_shifts: bfloat16 [2, 768], replicated, may hold values from -1.75 to 1.75
- w_qkv: bfloat16 [768, 2304], replicated, may hold values from -0.21875 to 0.21875
- qv_bias: bfloat16 [2, 768], replicated, may hold values from -1.75 to 1.75
- w_out: bfloat16 [768, 768], replicated, may hold values from -1.75 to 1.75
- out_biases: bfloat16 [2, 768], replicated, may hold values from -1.75 to 1.75
- w_up: bfloat16 [768, 3072], replicated, may hold values from -0.21875 to 0.21875
- up_bias: bfloat16 [3072], replicated, may hold values from -1.75 to 1.75
- w_down: bfloat16 [3072, 768], replicated, may hold values from -0.21875 to 0.21875
- lengths: int32 [8, 4], P('dp'), may hold values from 0 to 1024, as said below
- d_out: bfloat16 [8, 1024, 768], P('dp', 'head'), may hold values from -8 to 8
Outputs:
- block_out: bfloat16 [8, 1024, 768], P('dp', 'head')
- grad_inputs: float32 [8, 1024, 768], P('dp', 'head')
- grad_norm_gains: float32 [2, 768], P(None, 'dp')
- grad_norm_shifts: float32 [2, 768], P(None, 'dp')
- grad_qkv: float32 [768, 2304], P(None, 'dp')
- grad_qv_bias: float32 [2, 768], P(None, 'dp')
- grad_out: float32 [768, 768], P(None, 'dp')
- grad_out_biases: float32 [2, 768], P(None, 'dp')
- grad_up: float32 [768, 3072], P(None, 'dp')
- grad_up_bias: float32 [3072], P('dp')
- grad_down: float32 [3072, 768], P(None, 'dp')
The draws below stay inside these ranges and needn't reach their ends.
Inputs may be any that keep to these rules, and one draw needn't show every extreme that they name: Each slot holds either one image of 1024 patches (lengths 1024, then zeros) or 1 to 4 images of 256 patches in its first entries, then zeros. The first slot holds one image of 1024 patches.
All inputs are finite; a program needn't handle non-finite values.
Results may differ from the reference program's by a relative error of at most 0.014.
Values may be sent and summed in bfloat16 or wider, within the bound.
A program may use at most 256 MiB of HBM per device.

```python
import math
import jax
import jax.numpy as jnp
from jax import lax

D = 768
HEADS = 12
HDIM = 64
FF = 3072
SLOT = 1024
SHORT = 256
ITEMS = 4
SLOTS = 8


def draw_lengths(key, part):
    slot_kind = jax.random.randint(key, (SLOTS,), 0, ITEMS + 1)
    slot_kind = jnp.where(jnp.arange(SLOTS) == 0, 0, slot_kind)
    columns = jnp.arange(ITEMS)
    short_rows = jnp.where(columns[None, :] < slot_kind[:, None], SHORT, 0)
    long_rows = jnp.where(columns[None, :] == 0, SLOT, 0)
    long_rows = jnp.broadcast_to(long_rows, short_rows.shape)
    return jnp.where(slot_kind[:, None] == 0, long_rows, short_rows).astype(jnp.int32)


def with_spikes(entries, stream_key, source, target, parts, factor):
    def block_of(axis_at):
        return (jnp.arange(entries.shape[axis_at]) // (entries.shape[axis_at] // parts)).reshape((-1,) + (1,) * (entries.ndim - 1 - axis_at))

    near = jax.random.permutation(stream_key, parts)[block_of(target)]
    far = (block_of(target) + parts // 2) % parts
    return jnp.where((block_of(source) == near) | (block_of(source) == far), factor * entries, entries)


def steps_of(own_key, dims, shards, smallest, top_value):
    gain, own = 1.0, jax.random.fold_in(own_key, 6)
    for axis_at, parts in shards:
        draws = jnp.exp(jax.random.uniform(jax.random.fold_in(own, axis_at), (parts,), jnp.float32, smallest / len(shards), top_value / len(shards)))
        gain = gain * jnp.repeat(draws, dims[axis_at] // parts).reshape([-1 if axis == axis_at else 1 for axis in range(len(dims))])
    return gain


def noise(stream_key, shape, deviation, most, cuts=(), held_as=jnp.bfloat16):
    entries = jax.random.normal(stream_key, shape, jnp.float32) * deviation
    if len(cuts) > 0:
        entries = steps_of(stream_key, shape, cuts, -0.22, 0.18) * entries
    return jnp.clip(entries, min=-most, max=most).astype(held_as)


def gaussian_with(rng, dims, width, reach, cuts, heavy, kind=jnp.bfloat16):
    array = width * jax.random.normal(rng, dims, jnp.float32)
    if cuts:
        array = array * steps_of(rng, dims, cuts, -0.22, 0.18)
    return jnp.clip(with_spikes(array, jax.random.fold_in(rng, 3), *heavy), -reach, reach).astype(kind)


def setup_inputs(seed: int = 0) -> dict:
    streams_of = jax.random.split(jax.random.key(seed), 13)
    return {
        "inputs": noise(streams_of[0], (SLOTS, SLOT, D), 1.0, 6.0, ((0, 8), (1, 4))),
        "norm_gains": jnp.clip(1.0 + 0.1 * jax.random.normal(streams_of[1], (2, D), jnp.float32), 0.5, 1.5).astype(jnp.bfloat16),
        "norm_shifts": noise(streams_of[2], (2, D), 0.3, 1.75),
        "w_qkv": noise(streams_of[3], (D, 3 * D), D ** -0.5, 0.21875),
        "qv_bias": noise(streams_of[4], (2, D), 0.3, 1.75),
        "w_out": noise(streams_of[5], (D, D), (D // 64) ** -0.5, 1.75),
        "out_biases": noise(streams_of[6], (2, D), 0.3, 1.75),
        "w_up": noise(streams_of[7], (D, FF), D ** -0.5, 0.21875),
        "up_bias": noise(streams_of[8], (FF,), 0.3, 1.75),
        "w_down": noise(streams_of[9], (FF, D), (FF // 4) ** -0.5, 0.21875),
        "lengths": draw_lengths(jax.random.fold_in(streams_of[12], 71), 0),
        "d_out": gaussian_with(streams_of[11], (SLOTS, SLOT, D), 1.0, 8.0, ((0, 8), (1, 4)), (0, 2, 8, 2.0)),
    }


@jax.custom_vjp
def low(v):
    return lax.optimization_barrier(v.astype(jnp.bfloat16)).astype(jnp.float32)

@jax.custom_vjp
def low_back(v):
    return v

def low_keep(v):
    return (low(v), None)

def low_pass(kept, grad):
    return (grad,)

def back_keep(v):
    return (v, None)

def back_low(kept, grad):
    return (low(grad),)
low.defvjp(low_keep, low_pass)
low_back.defvjp(back_keep, back_low)

def layer_norm(values, norm_gain, norm_shift):
    average = lax.optimization_barrier(jnp.mean(values, axis=-1, keepdims=True))
    centered = values - average
    variance = lax.optimization_barrier(jnp.mean(centered * centered, axis=-1, keepdims=True))
    return centered * lax.rsqrt(variance + 1e-06) * norm_gain + norm_shift

def slot_allowed(lengths_row):
    item_ends = jnp.cumsum(lengths_row).astype(jnp.int32)
    positions = jnp.arange(SLOT, dtype=jnp.int32)
    segment = lax.optimization_barrier(jnp.sum((positions[:, None] >= item_ends[None, :]).astype(jnp.int32), axis=1))
    is_real = positions < item_ends[ITEMS - 1]
    same_item = (segment[:, None] == segment[None, :]) & is_real[None, :]
    return same_item | (positions[:, None] == positions[None, :])

def slot_forward(params, tokens, lengths_row):
    gains, shifts, w_qkv, qv_bias, w_out, out_biases, w_up, up_bias, w_down = params
    highest = lax.Precision.HIGHEST
    allowed = slot_allowed(lengths_row)
    normed = low(layer_norm(tokens, gains[0], shifts[0]))
    full_bias = jnp.concatenate([qv_bias[0], jnp.zeros_like(qv_bias[0]), qv_bias[1]])
    projected = low(low_back(jnp.dot(normed, w_qkv, precision=highest) + full_bias))
    head_split = projected.reshape(SLOT, 3, HEADS, HDIM).transpose(1, 2, 0, 3)
    scores = low_back(jnp.einsum('hqe,hke->hqk', head_split[0], head_split[1], precision=highest) * HDIM ** (-0.5))
    masked = jnp.where(allowed[None], scores, -jnp.inf)
    row_max = lax.optimization_barrier(jnp.max(masked, axis=-1, keepdims=True))
    weights = jnp.exp(masked - row_max)
    attn_probs = weights / lax.optimization_barrier(jnp.sum(weights, axis=-1, keepdims=True))
    mixed_out = low_back(low(jnp.einsum('hqk,hke->hqe', low(attn_probs), head_split[2], precision=highest)))
    joined = mixed_out.transpose(1, 0, 2).reshape(SLOT, D)
    hidden = tokens + low_back(jnp.dot(joined, w_out, precision=highest)) + out_biases[0]
    normed_two = low(layer_norm(hidden, gains[1], shifts[1]))
    up_values = low_back(jnp.dot(normed_two, w_up, precision=highest)) + up_bias
    activated = low(jax.nn.gelu(up_values, approximate=False))
    return hidden + low_back(jnp.dot(activated, w_down, precision=highest)) + out_biases[1]

def forward(params, tokens, lengths):
    group_size = math.gcd(SLOTS, 4)
    grouped = tokens.reshape(SLOTS // group_size, group_size, SLOT, D)
    grouped_lengths = lengths.reshape(SLOTS // group_size, group_size, ITEMS)

    def group_step(carried, pieces):
        return (carried, jax.vmap(slot_forward, in_axes=(None, 0, 0))(params, pieces[0], pieces[1]))
    unused, results = lax.scan(jax.checkpoint(group_step), jnp.zeros((), jnp.float32), (grouped, grouped_lengths))
    return results.reshape(SLOTS, SLOT, D)

def reference(inputs, norm_gains, norm_shifts, w_qkv, qv_bias, w_out, out_biases, w_up, up_bias, w_down, lengths, d_out):
    params = (norm_gains.astype(jnp.float32), norm_shifts.astype(jnp.float32), w_qkv.astype(jnp.float32), qv_bias.astype(jnp.float32), w_out.astype(jnp.float32), out_biases.astype(jnp.float32), w_up.astype(jnp.float32), up_bias.astype(jnp.float32), w_down.astype(jnp.float32))
    tokens = inputs.astype(jnp.float32)

    def run_block(params_in, tokens_in):
        return forward(params_in, tokens_in, lengths)
    block_out, pullback = jax.vjp(run_block, params, tokens)
    totals = lax.optimization_barrier(jnp.sum(lengths, axis=1)).astype(jnp.int32)
    is_real = jnp.arange(SLOT, dtype=jnp.int32)[None, :] < totals[:, None]
    cotangent = d_out.astype(jnp.float32) * is_real[:, :, None].astype(jnp.float32)
    grad_params, grad_inputs = pullback(cotangent)
    return (block_out.astype(jnp.bfloat16), grad_inputs, grad_params[0], grad_params[1], grad_params[2], grad_params[3], grad_params[4], grad_params[5], grad_params[6], grad_params[7], grad_params[8])
```

```python
import functools

import jax
import jax.numpy as jnp
from jax import lax
from jax.experimental import pallas as pl
from jax.experimental.pallas import tpu as pltpu
from jax.sharding import PartitionSpec as P

D = 768
HEADS = 12
HDIM = 64
FF = 3072
SLOT = 1024
EPSILON = 1e-06
BF = jnp.bfloat16
F32 = jnp.float32
FAR = -1e30
VMEM_LIMIT = 60 * 1024 * 1024


def nn(a, b):
    return lax.dot_general(a, b, (((1,), (0,)), ((), ())), preferred_element_type=F32)


def nt(a, b):
    return lax.dot_general(a, b, (((1,), (1,)), ((), ())), preferred_element_type=F32)


def tn(a, b):
    return lax.dot_general(a, b, (((0,), (0,)), ((), ())), preferred_element_type=F32)


def norm_parts(values, norm_gain, norm_shift):
    average = jnp.mean(values, axis=-1, keepdims=True)
    centered = values - average
    variance = jnp.mean(centered * centered, axis=-1, keepdims=True)
    inverse = lax.rsqrt(variance + EPSILON)
    unit = centered * inverse
    return unit, inverse, unit * norm_gain + norm_shift


def norm_back(grad_normed, unit, inverse, norm_gain):
    grad_unit = grad_normed * norm_gain
    first_mean = jnp.mean(grad_unit, axis=-1, keepdims=True)
    second_mean = jnp.mean(grad_unit * unit, axis=-1, keepdims=True)
    return inverse * (grad_unit - first_mean - unit * second_mean)


def gelu_parts(values):
    cumulative = 0.5 + 0.5 * lax.erf(values * 0.7071067811865476)
    density = jnp.exp(values * values * -0.5) * 0.3989422804014327
    return values * cumulative, cumulative + values * density


def lanes_of(width=256):
    return lax.broadcasted_iota(jnp.int32, (1, width), 1)


def head_mask(head):
    lane = lanes_of()
    return jnp.where((lane >= head * HDIM) & (lane < (head + 1) * HDIM), 1.0, 0.0)


def lane_is(index):
    return jnp.where(lanes_of() == index, 1.0, 0.0)


def split_three(column):
    high = column.astype(BF).astype(F32)
    rest = column - high
    middle = rest.astype(BF).astype(F32)
    return high, middle, rest - middle


def attend_forward(normed, weight, bias, lengths, q_ref, k_ref, v_ref, mixed_ref, exact_ref, lse_ref):
    whole = lengths[:, 0:1] == SLOT
    total = jnp.sum(lengths, axis=1, keepdims=True)
    onlane = lanes_of()
    aux_k = jnp.where((onlane >= 196) & (onlane < 199), 1.0, 0.0)
    aux_v = jnp.where((onlane >= 192) & (onlane < 199) & (onlane != 195), 1.0, 0.0)
    for block in range(4):
        rows = pl.ds(block * 256, 256)
        projected = nn(normed[rows, :], weight[...]) + bias
        projected = projected.astype(BF).astype(F32)
        q_ref[rows, :] = (projected[:, :256] * 0.125 + lane_is(192 + block)).astype(BF)
        other = jnp.where((onlane >= 192) & (onlane < 196) & (onlane != 192 + block), 1.0, 0.0)
        far = other * jnp.where(whole, 0.0, FAR)
        k_ref[rows, :] = (projected[:, 256:512] + (aux_k + far)).astype(BF)
        v_ref[rows, :] = (projected[:, 512:] + aux_v).astype(BF)
    on_aux = jnp.where(onlane >= 192, 1.0, 0.0)

    def block_step(block, carry):
        rows = pl.ds(pl.multiple_of(block * 256, 256), 256)
        queries = q_ref[rows, :]
        mixed = jnp.zeros((256, 256), F32)
        tops = []
        for head in range(3):
            scores = nt(queries * (head_mask(head) + on_aux).astype(BF), k_ref[...])
            top = jnp.max(scores, axis=1, keepdims=True)
            weights = jnp.exp(scores - top).astype(BF)
            mixed += nn(weights, v_ref[...] * (head_mask(head) + lane_is(192 + head)).astype(BF))
            tops.append(top)
        lse = jnp.zeros((256, 128), F32)
        scale = jnp.zeros((256, 256), F32)
        small = lax.broadcasted_iota(jnp.int32, (1, 128), 1)
        for head in range(3):
            row_sum = jnp.sum(mixed * lane_is(192 + head), axis=1, keepdims=True)
            lse += (tops[head] + jnp.log(row_sum)) * jnp.where(small == head, 1.0, 0.0)
            scale += (1.0 / row_sum) * head_mask(head)
        mixed = mixed * scale
        position = block * 256 + lax.broadcasted_iota(jnp.int32, (256, 1), 0)
        on_heads = jnp.where(onlane < 192, 1.0, 0.0)
        mixed = jnp.where(position < total, mixed, v_ref[rows, :].astype(F32) * on_heads)
        exact_ref[rows, :] = mixed
        mixed_ref[rows, :] = mixed[:, :192].astype(BF)
        lse_ref[rows, :] = lse
        return carry

    lax.fori_loop(0, 4, block_step, 0)


def attend_backward(q_ref, k_ref, v_ref, exact_ref, lse_ref, grad_mixed, q_aug, g_aug, scores_low, dq_acc, dk_acc, dv_acc):
    for head in range(3):
        mask = head_mask(head)

        def augment(block, carry):
            rows = pl.ds(pl.multiple_of(block * 256, 256), 256)
            grads = grad_mixed[rows, :].astype(F32) * mask
            inner = jnp.sum(grads * exact_ref[rows, :], axis=1, keepdims=True)
            lse = lse_ref[rows, :][:, head : head + 1]
            queries = q_ref[rows, :].astype(F32) * (mask + jnp.where(lanes_of() >= 192, 1.0, 0.0))
            for place, part in enumerate(split_three(-lse)):
                queries = queries + part * lane_is(196 + place)
            for place, part in enumerate(split_three(-inner)):
                grads = grads + part * lane_is(196 + place)
            q_aug[rows, :] = queries.astype(BF)
            g_aug[rows, :] = grads.astype(BF)
            return carry

        lax.fori_loop(0, 4, augment, 0)

        def block_step(block, carry):
            rows = pl.ds(pl.multiple_of(block * 256, 256), 256)
            probs = jnp.exp(nt(k_ref[rows, :], q_aug[...]))
            grad_probs = nt(v_ref[rows, :], g_aug[...])
            grad_scores = (probs * grad_probs).astype(BF)
            scores_low[rows, :] = grad_scores
            key_part = nn(grad_scores, q_aug[...]) * mask
            value_part = nn(probs.astype(BF), g_aug[...]) * mask
            if head == 0:
                dk_acc[rows, :] = key_part
                dv_acc[rows, :] = value_part
            else:
                dk_acc[rows, :] += key_part
                dv_acc[rows, :] += value_part
            return carry

        lax.fori_loop(0, 4, block_step, 0)
        query_part = tn(scores_low[...], k_ref[...] * mask.astype(BF)) * 0.125
        if head == 0:
            dq_acc[...] = query_part
        else:
            dq_acc[...] += query_part


def forward_kernel(normed, weight, bias, lengths, q_ref, k_ref, v_ref, mixed_ref, exact_ref, lse_ref):
    attend_forward(normed, weight, bias[...], lengths[...], q_ref, k_ref, v_ref, mixed_ref, exact_ref, lse_ref)


def middle_kernel(
    mixed_in, x_in, d_low, w_out, w_up, w_down, gains, shifts, biases, up_bias,
    block_ref, second_ref, hid_ref, low_ref, sums_ref, mixed_rows, act_ref,
):
    rows = x_in.shape[0]
    for group in range(4):
        mixed_rows[:, group * 192 : (group + 1) * 192] = mixed_in[group]
    hidden = x_in[...].astype(F32) + nn(mixed_rows[...], w_out[...]) + biases[0:1, :]
    unit, inverse, normed = norm_parts(hidden, gains[1:2, :], shifts[1:2, :])
    second = normed.astype(BF)
    second_ref[...] = second
    grad_low = d_low[...]
    down = jnp.zeros((rows, D), F32)
    back = jnp.zeros((rows, D), F32)
    step = 768
    for tile in range(FF // step):
        cut = slice(tile * step, (tile + 1) * step)
        up = nn(second, w_up[:, cut]) + up_bias[:, cut]
        value, slope = gelu_parts(up)
        down += nn(value.astype(BF), w_down[cut, :])
        grad_up = nt(grad_low, w_down[cut, :]) * slope
        back += nt(grad_up.astype(BF), w_up[:, cut])
    block_ref[...] = (hidden + down + biases[1:2, :]).astype(BF)
    grad_block = grad_low.astype(F32)
    grad_hidden = grad_block + norm_back(back, unit, inverse, gains[1:2, :])
    hid_ref[...] = grad_hidden
    low_ref[...] = grad_hidden.astype(BF)
    sums_ref[...] = jnp.zeros_like(sums_ref)
    sums_ref[0:1, :] = jnp.sum(back * unit, axis=0, keepdims=True)
    sums_ref[1:2, :] = jnp.sum(back, axis=0, keepdims=True)
    sums_ref[2:3, :] = jnp.sum(grad_hidden, axis=0, keepdims=True)
    sums_ref[3:4, :] = jnp.sum(grad_block, axis=0, keepdims=True)


def feed_kernel(second, d_low, w_up, w_down, up_bias, up_grad, down_grad, bias_grad, act_ref, grad_ref):
    width = w_up.shape[1]
    bias_grad[...] = jnp.zeros_like(bias_grad)

    def step(block, carry):
        rows = pl.ds(pl.multiple_of(block * 256, 256), 256)
        up = nn(second[rows, :], w_up[...]) + up_bias[...]
        value, slope = gelu_parts(up)
        act_ref[rows, :] = value.astype(BF)
        grad_up = nt(d_low[rows, :], w_down[...]) * slope
        bias_grad[0:1, :] += jnp.sum(grad_up, axis=0, keepdims=True)
        grad_ref[rows, :] = grad_up.astype(BF)
        return carry

    lax.fori_loop(0, 4, step, 0)
    down_grad[...] = tn(d_low[...], act_ref[...]).astype(BF)
    up_grad[...] = tn(grad_ref[...], second[...]).astype(BF)


def backward_kernel(
    grad_low, w_out, normed, mixed, q_ref, k_ref, v_ref, exact_ref, lse_ref,
    grad_ref, out_grad, qkv_grad, bias_grad,
    grad_mixed, q_aug, g_aug, scores_low, dq_acc, dk_acc, dv_acc,
):
    padded = jnp.zeros((64, D), BF)
    weight = jnp.concatenate([w_out[...], padded], axis=0)
    grad_mixed[...] = nt(grad_low[...], weight).astype(BF)
    out_grad[...] = tn(grad_low[...], mixed[...]).astype(BF)
    attend_backward(q_ref, k_ref, v_ref, exact_ref, lse_ref, grad_mixed, q_aug, g_aug, scores_low, dq_acc, dk_acc, dv_acc)
    for place, part in enumerate((dq_acc, dk_acc, dv_acc)):
        grad_ref[:, place * 192 : (place + 1) * 192] = part[:, :192].astype(BF)
    bias_grad[...] = jnp.zeros_like(bias_grad)
    bias_grad[0:1, :] = jnp.sum(grad_ref[...].astype(F32), axis=0, keepdims=True)
    qkv_grad[...] = tn(grad_ref[...], normed[...]).astype(BF)


def last_kernel(grad_in, w_qkv, x_in, hid, gains, shifts, out_ref, sums_ref, grad_rows):
    for part in range(3):
        for group in range(4):
            place = part * D + group * 192
            grad_rows[:, place : place + 192] = grad_in[group][:, part * 192 : (part + 1) * 192]
    grad_first = nt(grad_rows[...], w_qkv[...])
    unit, inverse, _ = norm_parts(x_in[...].astype(F32), gains[0:1, :], shifts[0:1, :])
    out_ref[...] = hid[...] + norm_back(grad_first, unit, inverse, gains[0:1, :])
    sums_ref[...] = jnp.zeros_like(sums_ref)
    sums_ref[0:1, :] = jnp.sum(grad_first * unit, axis=0, keepdims=True)
    sums_ref[1:2, :] = jnp.sum(grad_first, axis=0, keepdims=True)


def whole_call(kernel, outs, scratch=(), name=None):
    return pl.pallas_call(
        kernel,
        out_shape=[jax.ShapeDtypeStruct(*out) for out in outs],
        scratch_shapes=[pltpu.VMEM(*item) for item in scratch],
        compiler_params=pltpu.CompilerParams(vmem_limit_bytes=VMEM_LIMIT),
        name=name,
    )


def per_device(x, norm_gains, norm_shifts, w_qkv, qv_bias, w_out, out_biases, w_up, up_bias, w_down, lengths, d_out):
    groups = lax.axis_size("head")
    shards = lax.axis_size("dp")
    group = lax.axis_index("head")
    rows = x.shape[1]
    own = D // groups
    x = x[0]
    gains = norm_gains.astype(F32)
    shifts = norm_shifts.astype(F32)
    biases = out_biases.astype(F32)
    up_shift = up_bias.astype(F32)
    full_bias = jnp.stack([qv_bias[0], jnp.zeros_like(qv_bias[0]), qv_bias[1]]).astype(F32)

    weight_own = lax.dynamic_index_in_dim(w_qkv.reshape(D, 3, groups, own), group, 2, False)
    weight_own = jnp.pad(weight_own, ((0, 0), (0, 0), (0, 256 - own))).reshape(D, 768)
    bias_own = lax.dynamic_index_in_dim(full_bias.reshape(3, groups, own), group, 1, False)
    bias_own = jnp.pad(bias_own, ((0, 0), (0, 256 - own))).reshape(1, 768)
    out_own = lax.dynamic_slice_in_dim(w_out, group * own, own, 0)
    unit_ff = FF // (shards * groups)
    up_own = lax.dynamic_index_in_dim(w_up.reshape(D, shards, groups, unit_ff), group, 2, False).reshape(D, D)
    down_own = lax.dynamic_index_in_dim(w_down.reshape(shards, groups, unit_ff, D), group, 1, False).reshape(D, D)
    ub_own = lax.dynamic_index_in_dim(up_shift.reshape(shards, groups, unit_ff), group, 1, False).reshape(1, D)

    normed = norm_parts(x.astype(F32), gains[0], shifts[0])[2].astype(BF)
    normed_all = lax.all_gather(normed, "head", axis=0, tiled=True)
    total = jnp.sum(lengths[0])
    position = group * rows + jnp.arange(rows, dtype=jnp.int32)
    d_low = jnp.where((position < total)[:, None], d_out[0], jnp.zeros_like(d_out[0]))
    d_all = lax.all_gather(d_low, "head", axis=0, tiled=True)

    q, k, v, mixed, exact, lse = whole_call(
        forward_kernel,
        [((SLOT, 256), BF)] * 3 + [((SLOT, own), BF), ((SLOT, 256), F32), ((SLOT, 128), F32)],
        name="attend_forward",
    )(normed_all, weight_own, bias_own, lengths)
    mixed_in = lax.all_to_all(mixed.reshape(groups, rows, own), "head", 0, 0, tiled=True)
    block_out, second, hid, hid_low, sums_mid = whole_call(
        middle_kernel,
        [((rows, D), BF), ((rows, D), BF), ((rows, D), F32), ((rows, D), BF), ((8, D), F32)],
        [((rows, D), BF), ((rows, FF), BF)],
        name="middle",
    )(mixed_in, x, d_low, w_out, w_up, w_down, gains, shifts, biases, up_shift.reshape(1, FF))
    second_all = lax.all_gather(second, "head", axis=0, tiled=True)
    low_all = lax.all_gather(hid_low, "head", axis=0, tiled=True)
    up_grad, down_grad, ub_grad = whole_call(
        feed_kernel,
        [((D, D), BF), ((D, D), BF), ((8, D), F32)],
        [((SLOT, D), BF), ((SLOT, D), BF)],
        name="feed",
    )(second_all, d_all, up_own, down_own, ub_own)
    grad_own, out_grad, qkv_grad, qkv_sum = whole_call(
        backward_kernel,
        [((SLOT, 3 * own), BF), ((D, own), BF), ((3 * own, D), BF), ((8, 3 * own), F32)],
        [((SLOT, 256), BF)] * 3 + [((SLOT, SLOT), BF)] + [((SLOT, 256), F32)] * 3,
        name="attend_backward",
    )(low_all, out_own, normed_all, mixed, q, k, v, exact, lse)
    grad_in = lax.all_to_all(grad_own.reshape(groups, rows, 3 * own), "head", 0, 0, tiled=True)
    grad_inputs, sums_last = whole_call(
        last_kernel,
        [((rows, D), F32), ((8, D), F32)],
        [((rows, 3 * D), BF)],
        name="last",
    )(grad_in, w_qkv, x, hid, gains, shifts)

    def scatter(values):
        return lax.psum_scatter(values, "dp", scatter_dimension=0, tiled=True)

    up_part = lax.all_gather(scatter(up_grad), "head", axis=0, tiled=True)
    down_part = lax.all_gather(scatter(down_grad), "head", axis=1, tiled=True)
    out_part = lax.all_gather(scatter(out_grad), "head", axis=1, tiled=True)
    down_out = down_part.astype(F32).T.reshape(groups, shards, unit_ff, D // shards)
    down_out = down_out.transpose(1, 0, 2, 3).reshape(FF, D // shards)
    spread = jnp.zeros((3, groups, own, D), BF)
    spread = lax.dynamic_update_slice(spread, qkv_grad.reshape(3, 1, own, D), (0, group, 0, 0))
    qkv_part = lax.psum(scatter(spread.reshape(3 * D, D)), "head")

    def place_rows(values):
        parts = values.reshape(3, own)
        empty = jnp.zeros((3, groups, own), F32)
        return lax.dynamic_update_slice(empty, parts[:, None], (0, group, 0)).reshape(3, D)

    bias_rows = place_rows(qkv_sum[0])
    ub_rows = lax.dynamic_update_slice(
        jnp.zeros((shards, groups, unit_ff), F32), ub_grad[0].reshape(shards, 1, unit_ff), (0, group, 0)
    ).reshape(4, D)
    small = jnp.concatenate([sums_last[0:2], sums_mid[0:4], bias_rows[0:1], bias_rows[2:3], ub_rows], axis=0)
    small = lax.psum(small, ("dp", "head"))
    shard = lax.axis_index("dp")

    def cut(values):
        width = D // shards
        return lax.dynamic_slice_in_dim(values, shard * width, width, 1)

    ub_out = lax.dynamic_slice_in_dim(small[8:12].reshape(FF), shard * (FF // shards), FF // shards, 0)
    return (
        block_out[None],
        grad_inputs[None],
        cut(jnp.stack([small[0], small[2]])),
        cut(jnp.stack([small[1], small[3]])),
        qkv_part.astype(F32).T,
        cut(small[6:8]),
        out_part.astype(F32).T,
        cut(small[4:6]),
        up_part.astype(F32).T,
        ub_out,
        down_out,
    )


def solution(mesh):
    split = P("dp", "head", None)
    placed = (split,) + (P(),) * 9 + (P("dp", None), split)
    return jax.shard_map(
        per_device,
        mesh=mesh,
        in_specs=placed,
        out_specs=(split, split) + (P(None, "dp"),) * 7 + (P("dp"), P(None, "dp")),
        check_vma=False,
    )
```

```python
import functools

import jax
import jax.numpy as jnp
from jax import lax
from jax.experimental import pallas as pl
from jax.experimental.pallas import tpu as pltpu
from jax.sharding import PartitionSpec as P

D = 768
HEADS = 12
HDIM = 64
FF = 3072
SLOT = 1024
EPSILON = 1e-06
BF = jnp.bfloat16
F32 = jnp.float32
FAR = -1e30
VMEM_LIMIT = 63 * 1024 * 1024


def nn(a, b):
    return lax.dot_general(a, b, (((1,), (0,)), ((), ())), preferred_element_type=F32)


def nt(a, b):
    return lax.dot_general(a, b, (((1,), (1,)), ((), ())), preferred_element_type=F32)


def tn(a, b):
    return lax.dot_general(a, b, (((0,), (0,)), ((), ())), preferred_element_type=F32)


def norm_parts(values, norm_gain, norm_shift):
    average = jnp.mean(values, axis=-1, keepdims=True)
    centered = values - average
    variance = jnp.mean(centered * centered, axis=-1, keepdims=True)
    inverse = lax.rsqrt(variance + EPSILON)
    unit = centered * inverse
    return unit, inverse, unit * norm_gain + norm_shift


def norm_back(grad_normed, unit, inverse, norm_gain):
    grad_unit = grad_normed * norm_gain
    first_mean = jnp.mean(grad_unit, axis=-1, keepdims=True)
    second_mean = jnp.mean(grad_unit * unit, axis=-1, keepdims=True)
    return inverse * (grad_unit - first_mean - unit * second_mean)


def gelu_parts(values):
    cumulative = 0.5 + 0.5 * lax.erf(values * 0.7071067811865476)
    density = jnp.exp(values * values * -0.5) * 0.3989422804014327
    return values * cumulative, cumulative + values * density


def lanes_of(width=256):
    return lax.broadcasted_iota(jnp.int32, (1, width), 1)


def head_mask(head):
    lane = lanes_of()
    return jnp.where((lane >= head * HDIM) & (lane < (head + 1) * HDIM), 1.0, 0.0)


def lane_is(index):
    return jnp.where(lanes_of() == index, 1.0, 0.0)


def split_three(column):
    high = column.astype(BF).astype(F32)
    rest = column - high
    middle = rest.astype(BF).astype(F32)
    return high, middle, rest - middle


def attend_forward(normed, weight, bias, lengths, q_ref, k_ref, v_ref, mixed_ref, exact_ref, lse_ref):
    whole = lengths[:, 0:1] == SLOT
    total = jnp.sum(lengths, axis=1, keepdims=True)
    onlane = lanes_of()
    aux_k = jnp.where((onlane >= 196) & (onlane < 199), 1.0, 0.0)
    aux_v = jnp.where((onlane >= 192) & (onlane < 199) & (onlane != 195), 1.0, 0.0)
    for block in range(4):
        rows = pl.ds(block * 256, 256)
        projected = nn(normed[rows, :], weight[...]) + bias
        projected = projected.astype(BF).astype(F32)
        q_ref[rows, :] = (projected[:, :256] * 0.125 + lane_is(192 + block)).astype(BF)
        other = jnp.where((onlane >= 192) & (onlane < 196) & (onlane != 192 + block), 1.0, 0.0)
        far = other * jnp.where(whole, 0.0, FAR)
        k_ref[rows, :] = (projected[:, 256:512] + (aux_k + far)).astype(BF)
        v_ref[rows, :] = (projected[:, 512:] + aux_v).astype(BF)
    on_aux = jnp.where(onlane >= 192, 1.0, 0.0)

    def block_step(block, carry):
        rows = pl.ds(pl.multiple_of(block * 256, 256), 256)
        queries = q_ref[rows, :]
        mixed = jnp.zeros((256, 256), F32)
        tops = []
        for head in range(3):
            scores = nt(queries * (head_mask(head) + on_aux).astype(BF), k_ref[...])
            top = jnp.max(scores, axis=1, keepdims=True)
            weights = jnp.exp(scores - top).astype(BF)
            mixed += nn(weights, v_ref[...] * (head_mask(head) + lane_is(192 + head)).astype(BF))
            tops.append(top)
        lse = jnp.zeros((256, 128), F32)
        scale = jnp.zeros((256, 256), F32)
        small = lax.broadcasted_iota(jnp.int32, (1, 128), 1)
        for head in range(3):
            row_sum = jnp.sum(mixed * lane_is(192 + head), axis=1, keepdims=True)
            lse += (tops[head] + jnp.log(row_sum)) * jnp.where(small == head, 1.0, 0.0)
            scale += (1.0 / row_sum) * head_mask(head)
        mixed = mixed * scale
        position = block * 256 + lax.broadcasted_iota(jnp.int32, (256, 1), 0)
        on_heads = jnp.where(onlane < 192, 1.0, 0.0)
        mixed = jnp.where(position < total, mixed, v_ref[rows, :].astype(F32) * on_heads)
        exact_ref[rows, :] = mixed
        mixed_ref[rows, :] = mixed[:, :192].astype(BF)
        lse_ref[rows, :] = lse
        return carry

    lax.fori_loop(0, 4, block_step, 0)


def attend_backward(q_ref, k_ref, v_ref, exact_ref, lse_ref, grad_mixed, q_aug, g_aug, scores_low, dq_acc, dk_acc, dv_acc):
    for head in range(3):
        mask = head_mask(head)

        def augment(block, carry):
            rows = pl.ds(pl.multiple_of(block * 256, 256), 256)
            grads = grad_mixed[rows, :].astype(F32) * mask
            inner = jnp.sum(grads * exact_ref[rows, :], axis=1, keepdims=True)
            lse = lse_ref[rows, :][:, head : head + 1]
            queries = q_ref[rows, :].astype(F32) * (mask + jnp.where(lanes_of() >= 192, 1.0, 0.0))
            for place, part in enumerate(split_three(-lse)):
                queries = queries + part * lane_is(196 + place)
            for place, part in enumerate(split_three(-inner)):
                grads = grads + part * lane_is(196 + place)
            q_aug[rows, :] = queries.astype(BF)
            g_aug[rows, :] = grads.astype(BF)
            return carry

        lax.fori_loop(0, 4, augment, 0)

        def block_step(block, carry):
            rows = pl.ds(pl.multiple_of(block * 256, 256), 256)
            probs = jnp.exp(nt(k_ref[rows, :], q_aug[...]))
            grad_probs = nt(v_ref[rows, :], g_aug[...])
            grad_scores = (probs * grad_probs).astype(BF)
            scores_low[rows, :] = grad_scores
            key_part = nn(grad_scores, q_aug[...]) * mask
            value_part = nn(probs.astype(BF), g_aug[...]) * mask
            if head == 0:
                dk_acc[rows, :] = key_part
                dv_acc[rows, :] = value_part
            else:
                dk_acc[rows, :] += key_part
                dv_acc[rows, :] += value_part
            return carry

        lax.fori_loop(0, 4, block_step, 0)
        query_part = tn(scores_low[...], k_ref[...] * mask.astype(BF)) * 0.125
        if head == 0:
            dq_acc[...] = query_part
        else:
            dq_acc[...] += query_part


def forward_kernel(normed, weight, bias, lengths, q_ref, k_ref, v_ref, mixed_ref, exact_ref, lse_ref):
    attend_forward(normed, weight, bias[...], lengths[...], q_ref, k_ref, v_ref, mixed_ref, exact_ref, lse_ref)


def middle_kernel(
    mixed_in, x_in, d_low, w_out, w_up, w_down, gains, shifts, biases, up_bias,
    block_ref, second_ref, hid_ref, low_ref, sums_ref, mixed_rows, act_ref,
):
    rows = x_in.shape[0]
    for group in range(4):
        mixed_rows[:, group * 192 : (group + 1) * 192] = mixed_in[group]
    hidden = x_in[...].astype(F32) + nn(mixed_rows[...], w_out[...]) + biases[0:1, :]
    unit, inverse, normed = norm_parts(hidden, gains[1:2, :], shifts[1:2, :])
    second = normed.astype(BF)
    second_ref[...] = second
    grad_low = d_low[...]
    down = jnp.zeros((rows, D), F32)
    back = jnp.zeros((rows, D), F32)
    step = 768
    for tile in range(FF // step):
        cut = slice(tile * step, (tile + 1) * step)
        up = nn(second, w_up[:, cut]) + up_bias[:, cut]
        value, slope = gelu_parts(up)
        down += nn(value.astype(BF), w_down[cut, :])
        grad_up = nt(grad_low, w_down[cut, :]) * slope
        back += nt(grad_up.astype(BF), w_up[:, cut])
    block_ref[...] = (hidden + down + biases[1:2, :]).astype(BF)
    grad_block = grad_low.astype(F32)
    grad_hidden = grad_block + norm_back(back, unit, inverse, gains[1:2, :])
    hid_ref[...] = grad_hidden
    low_ref[...] = grad_hidden.astype(BF)
    sums_ref[...] = jnp.zeros_like(sums_ref)
    sums_ref[0:1, :] = jnp.sum(back * unit, axis=0, keepdims=True)
    sums_ref[1:2, :] = jnp.sum(back, axis=0, keepdims=True)
    sums_ref[2:3, :] = jnp.sum(grad_hidden, axis=0, keepdims=True)
    sums_ref[3:4, :] = jnp.sum(grad_block, axis=0, keepdims=True)


def feed_kernel(second, d_low, w_up, w_down, up_bias, up_grad, down_grad, bias_grad, act_ref, grad_ref):
    width = w_up.shape[1]
    bias_grad[...] = jnp.zeros_like(bias_grad)

    def step(block, carry):
        rows = pl.ds(pl.multiple_of(block * 256, 256), 256)
        up = nn(second[rows, :], w_up[...]) + up_bias[...]
        value, slope = gelu_parts(up)
        act_ref[rows, :] = value.astype(BF)
        grad_up = nt(d_low[rows, :], w_down[...]) * slope
        bias_grad[0:1, :] += jnp.sum(grad_up, axis=0, keepdims=True)
        grad_ref[rows, :] = grad_up.astype(BF)
        return carry

    lax.fori_loop(0, 4, step, 0)
    down_grad[...] = tn(d_low[...], act_ref[...]).astype(BF)
    up_grad[...] = tn(grad_ref[...], second[...]).astype(BF)


def backward_kernel(
    grad_low, w_out, normed, mixed, q_ref, k_ref, v_ref, exact_ref, lse_ref,
    grad_ref, out_grad, qkv_grad, bias_grad,
    grad_mixed, q_aug, g_aug, scores_low, dq_acc, dk_acc, dv_acc,
):
    padded = jnp.zeros((64, D), BF)
    weight = jnp.concatenate([w_out[...], padded], axis=0)
    grad_mixed[...] = nt(grad_low[...], weight).astype(BF)
    out_grad[...] = tn(grad_low[...], mixed[...]).astype(BF)
    attend_backward(q_ref, k_ref, v_ref, exact_ref, lse_ref, grad_mixed, q_aug, g_aug, scores_low, dq_acc, dk_acc, dv_acc)
    for place, part in enumerate((dq_acc, dk_acc, dv_acc)):
        grad_ref[:, place * 192 : (place + 1) * 192] = part[:, :192].astype(BF)
    bias_grad[...] = jnp.zeros_like(bias_grad)
    bias_grad[0:1, :] = jnp.sum(grad_ref[...].astype(F32), axis=0, keepdims=True)
    qkv_grad[...] = tn(grad_ref[...], normed[...]).astype(BF)


def last_kernel(grad_in, w_qkv, x_in, hid, gains, shifts, out_ref, sums_ref, grad_rows):
    for part in range(3):
        for group in range(4):
            place = part * D + group * 192
            grad_rows[:, place : place + 192] = grad_in[group][:, part * 192 : (part + 1) * 192]
    grad_first = nt(grad_rows[...], w_qkv[...])
    unit, inverse, _ = norm_parts(x_in[...].astype(F32), gains[0:1, :], shifts[0:1, :])
    out_ref[...] = hid[...] + norm_back(grad_first, unit, inverse, gains[0:1, :])
    sums_ref[...] = jnp.zeros_like(sums_ref)
    sums_ref[0:1, :] = jnp.sum(grad_first * unit, axis=0, keepdims=True)
    sums_ref[1:2, :] = jnp.sum(grad_first, axis=0, keepdims=True)


def whole_call(kernel, outs, scratch=(), name=None):
    return pl.pallas_call(
        kernel,
        out_shape=[jax.ShapeDtypeStruct(*out) for out in outs],
        scratch_shapes=[pltpu.VMEM(*item) for item in scratch],
        compiler_params=pltpu.CompilerParams(vmem_limit_bytes=VMEM_LIMIT),
        name=name,
    )


def general_device(x, norm_gains, norm_shifts, w_qkv, qv_bias, w_out, out_biases, w_up, up_bias, w_down, lengths, d_out):
    groups = lax.axis_size("head")
    shards = lax.axis_size("dp")
    group = lax.axis_index("head")
    rows = x.shape[1]
    own = D // groups
    x = x[0]
    gains = norm_gains.astype(F32)
    shifts = norm_shifts.astype(F32)
    biases = out_biases.astype(F32)
    up_shift = up_bias.astype(F32)
    full_bias = jnp.stack([qv_bias[0], jnp.zeros_like(qv_bias[0]), qv_bias[1]]).astype(F32)

    weight_own = lax.dynamic_index_in_dim(w_qkv.reshape(D, 3, groups, own), group, 2, False)
    weight_own = jnp.pad(weight_own, ((0, 0), (0, 0), (0, 256 - own))).reshape(D, 768)
    bias_own = lax.dynamic_index_in_dim(full_bias.reshape(3, groups, own), group, 1, False)
    bias_own = jnp.pad(bias_own, ((0, 0), (0, 256 - own))).reshape(1, 768)
    out_own = lax.dynamic_slice_in_dim(w_out, group * own, own, 0)
    unit_ff = FF // (shards * groups)
    up_own = lax.dynamic_index_in_dim(w_up.reshape(D, shards, groups, unit_ff), group, 2, False).reshape(D, D)
    down_own = lax.dynamic_index_in_dim(w_down.reshape(shards, groups, unit_ff, D), group, 1, False).reshape(D, D)
    ub_own = lax.dynamic_index_in_dim(up_shift.reshape(shards, groups, unit_ff), group, 1, False).reshape(1, D)

    normed = norm_parts(x.astype(F32), gains[0], shifts[0])[2].astype(BF)
    normed_all = lax.all_gather(normed, "head", axis=0, tiled=True)
    total = jnp.sum(lengths[0])
    position = group * rows + jnp.arange(rows, dtype=jnp.int32)
    d_low = jnp.where((position < total)[:, None], d_out[0], jnp.zeros_like(d_out[0]))
    d_all = lax.all_gather(d_low, "head", axis=0, tiled=True)

    q, k, v, mixed, exact, lse = whole_call(
        forward_kernel,
        [((SLOT, 256), BF)] * 3 + [((SLOT, own), BF), ((SLOT, 256), F32), ((SLOT, 128), F32)],
        name="attend_forward",
    )(normed_all, weight_own, bias_own, lengths)
    mixed_in = lax.all_to_all(mixed.reshape(groups, rows, own), "head", 0, 0, tiled=True)
    block_out, second, hid, hid_low, sums_mid = whole_call(
        middle_kernel,
        [((rows, D), BF), ((rows, D), BF), ((rows, D), F32), ((rows, D), BF), ((8, D), F32)],
        [((rows, D), BF), ((rows, FF), BF)],
        name="middle",
    )(mixed_in, x, d_low, w_out, w_up, w_down, gains, shifts, biases, up_shift.reshape(1, FF))
    second_all = lax.all_gather(second, "head", axis=0, tiled=True)
    low_all = lax.all_gather(hid_low, "head", axis=0, tiled=True)
    up_grad, down_grad, ub_grad = whole_call(
        feed_kernel,
        [((D, D), BF), ((D, D), BF), ((8, D), F32)],
        [((SLOT, D), BF), ((SLOT, D), BF)],
        name="feed",
    )(second_all, d_all, up_own, down_own, ub_own)
    grad_own, out_grad, qkv_grad, qkv_sum = whole_call(
        backward_kernel,
        [((SLOT, 3 * own), BF), ((D, own), BF), ((3 * own, D), BF), ((8, 3 * own), F32)],
        [((SLOT, 256), BF)] * 3 + [((SLOT, SLOT), BF)] + [((SLOT, 256), F32)] * 3,
        name="attend_backward",
    )(low_all, out_own, normed_all, mixed, q, k, v, exact, lse)
    grad_in = lax.all_to_all(grad_own.reshape(groups, rows, 3 * own), "head", 0, 0, tiled=True)
    grad_inputs, sums_last = whole_call(
        last_kernel,
        [((rows, D), F32), ((8, D), F32)],
        [((rows, 3 * D), BF)],
        name="last",
    )(grad_in, w_qkv, x, hid, gains, shifts)

    def scatter(values):
        return lax.psum_scatter(values, "dp", scatter_dimension=0, tiled=True)

    up_part = lax.all_gather(scatter(up_grad), "head", axis=0, tiled=True)
    down_part = lax.all_gather(scatter(down_grad), "head", axis=1, tiled=True)
    out_part = lax.all_gather(scatter(out_grad), "head", axis=1, tiled=True)
    down_out = down_part.astype(F32).T.reshape(groups, shards, unit_ff, D // shards)
    down_out = down_out.transpose(1, 0, 2, 3).reshape(FF, D // shards)
    spread = jnp.zeros((3, groups, own, D), BF)
    spread = lax.dynamic_update_slice(spread, qkv_grad.reshape(3, 1, own, D), (0, group, 0, 0))
    qkv_part = lax.psum(scatter(spread.reshape(3 * D, D)), "head")

    def place_rows(values):
        parts = values.reshape(3, own)
        empty = jnp.zeros((3, groups, own), F32)
        return lax.dynamic_update_slice(empty, parts[:, None], (0, group, 0)).reshape(3, D)

    bias_rows = place_rows(qkv_sum[0])
    ub_rows = lax.dynamic_update_slice(
        jnp.zeros((shards, groups, unit_ff), F32), ub_grad[0].reshape(shards, 1, unit_ff), (0, group, 0)
    ).reshape(4, D)
    small = jnp.concatenate([sums_last[0:2], sums_mid[0:4], bias_rows[0:1], bias_rows[2:3], ub_rows], axis=0)
    small = lax.psum(small, ("dp", "head"))
    shard = lax.axis_index("dp")

    def cut(values):
        width = D // shards
        return lax.dynamic_slice_in_dim(values, shard * width, width, 1)

    ub_out = lax.dynamic_slice_in_dim(small[8:12].reshape(FF), shard * (FF // shards), FF // shards, 0)
    return (
        block_out[None],
        grad_inputs[None],
        cut(jnp.stack([small[0], small[2]])),
        cut(jnp.stack([small[1], small[3]])),
        qkv_part.astype(F32).T,
        cut(small[6:8]),
        out_part.astype(F32).T,
        cut(small[4:6]),
        up_part.astype(F32).T,
        ub_out,
        down_out,
    )


MESH = pl.DeviceIdType.MESH
BLOCK = 256

BUFFERS = (
    ("xv", (256, D), BF),
    ("dv", (256, D), BF),
    ("wqkv", (D, 3 * D), BF),
    ("wout", (D, D), BF),
    ("wup", (D, FF), BF),
    ("big", (3 * SLOT, SLOT), BF),
    ("wqo", (D, D), BF),
    ("wuo", (D, D), BF),
    ("wdo", (D, D), BF),
    ("woo", (256, D), BF),
    ("nall", (SLOT, D), BF),
    ("dall", (SLOT, D), BF),
    ("sall", (SLOT, D), BF),
    ("lall", (SLOT, D), BF),
    ("qb", (SLOT, 256), BF),
    ("kb", (SLOT, 256), BF),
    ("vb", (SLOT, 256), BF),
    ("mix", (SLOT, 256), BF),
    ("exact", (SLOT, 256), F32),
    ("lse", (SLOT, 128), F32),
    ("mixin", (4, 256, 256), BF),
    ("gh", (256, D), F32),
    ("act", (SLOT, D), BF),
    ("gup", (SLOT, D), BF),
    ("gm", (SLOT, 256), BF),
    ("dkv", (SLOT, 384), BF),
    ("dq", (SLOT, 256), BF),
    ("kvin", (4, 256, 384), BF),
    ("qin", (4, 256, 256), BF),
    ("pdn", (8, 96, D), BF),
    ("pup", (6, 128, D), BF),
    ("pou", (8, 96, 256), BF),
    ("pqk", (6, 96, D), BF),
    ("ydn", (4, 96, D), BF),
    ("yup", (6, 128, D), BF),
    ("you", (4, 96, 256), BF),
    ("yqk", (6, 96, D), BF),
    ("zdn", (4, 96, D), BF),
    ("zup", (9, 128, D), BF),
    ("zou", (4, 96, 256), BF),
    ("zqk", (9, 96, D), BF),
    ("vec", (8, D), F32),
    ("small", (2, 4, 16, 128), F32),
    ("ysm", (4, 16, 128), F32),
    ("zsm", (4, 16, 128), F32),
    ("fsm", (4, 16, 128), F32),
)
SEMAPHORES = (
    ("load", 22),
    ("ns", 5), ("nr", 5), ("ds", 5), ("dr", 5), ("ss", 5), ("sr", 5), ("ls", 5), ("lr", 5),
    ("ms", 3), ("mr", 3), ("kvs", 3), ("kvr", 3), ("qs", 3), ("qr", 3),
    ("ydns", 4), ("ydnr", 4), ("zdns", 4), ("zdnr", 4), ("fdns", 3), ("fdnr", 3),
    ("yous", 4), ("your", 4), ("zous", 4), ("zour", 4), ("fous", 3), ("four", 3),
    ("yups", 6), ("yupr", 6), ("zups", 6), ("zupr", 9), ("fups", 9), ("fupr", 9),
    ("yqks", 6), ("yqkr", 6), ("zqks", 6), ("zqkr", 9), ("fqks", 9), ("fqkr", 9),
    ("ysms", 1), ("ysmr", 1), ("zsms", 4), ("zsmr", 4), ("fsms", 3), ("fsmr", 3),
)
INPUTS = ("x", "gains", "shifts", "w_qkv", "full_bias", "w_out", "biases", "w_up", "up_bias", "w_down", "lengths", "d_out")
IN_PLACE = ("x", "w_qkv", "w_out", "w_up", "w_down", "d_out")
OUTPUTS = (
    ("block_out", (256, D), BF),
    ("grad_inputs", (256, D), F32),
    ("fup", (3, 128, D), BF),
    ("fqk", (3, 96, D), BF),
    ("fdn", (4, 96, D), BF),
    ("fou", (4, 96, 256), BF),
    ("fsum", (16, 128), F32),
)


class Refs:
    pass


def block_rows(block, size=BLOCK, offset=0):
    return pl.ds(pl.multiple_of(block * BLOCK + offset, 128), size)


def one_kernel(*args):
    r = Refs()
    names = [*INPUTS] + [o[0] for o in OUTPUTS] + [b[0] for b in BUFFERS] + [s[0] for s in SEMAPHORES]
    for name, ref in zip(names, args, strict=True):
        setattr(r, name, ref)
    dp, head = lax.axis_index("dp"), lax.axis_index("head")
    z, y = lax.div(dp, 2), lax.rem(dp, 2)
    px, pc = lax.div(head, 2), lax.rem(head, 2)

    def peer(code):
        return lax.rem(px + (code // 2 if isinstance(code, int) else lax.div(code, 2)), 2) * 2 + lax.rem(
            pc + (code % 2 if isinstance(code, int) else lax.rem(code, 2)), 2
        )

    sib, far, diag = peer(1), peer(2), peer(3)
    other_y = z * 2 + (1 - y)

    def z_shard(k):
        return lax.rem(z + k, 4)

    sent = []

    def push(src, dst, send, recv, to):
        return pltpu.make_async_remote_copy(
            src_ref=src, dst_ref=dst, send_sem=send, recv_sem=recv, device_id=to, device_id_type=MESH
        )

    def when(cond, body):
        if cond is None:
            body()
        else:
            pl.when(cond)(body)

    def start(make, cond=None):
        when(cond, lambda: make().start())
        sent.append((make, cond))

    loads = {}

    def load(name, src, dst):
        loads.setdefault(name, []).append(pltpu.make_async_copy(src, dst, r.load.at[sum(map(len, loads.values()))]))

    load("x", r.x, r.xv)
    load("d", r.d_out, r.dv)
    load("wqkv", r.w_qkv, r.wqkv)
    load("wout", r.w_out, r.wout)
    load("wup", r.w_up, r.wup)
    load("wdown", r.w_down, r.big.at[:, 0:D])
    load("woo", r.w_out.at[pl.ds(pl.multiple_of(head * 192, 64), 192), :], r.woo.at[0:192, :])
    for j in range(6):
        unit = pl.ds(pl.multiple_of((4 * j + head) * 128, 128), 128)
        load("wuo", r.w_up.at[:, unit], r.wuo.at[:, j * 128 : (j + 1) * 128])
        load("wdo", r.w_down.at[unit, :], r.wdo.at[j * 128 : (j + 1) * 128, :])
    for copies in loads.values():
        for copy in copies:
            copy.start()

    def loaded(name):
        for copy in loads[name]:
            copy.wait()

    barrier = pltpu.get_barrier_semaphore()
    for to in [(dp, sib), (dp, far), (dp, diag), (other_y, head)] + [(z_shard(k) * 2 + y, head) for k in (1, 2, 3)]:
        pl.semaphore_signal(barrier, inc=1, device_id=to, device_id_type=MESH)

    gains = r.gains[...].astype(F32)
    shifts = r.shifts[...].astype(F32)
    biases = r.biases[...].astype(F32)
    onlane = lanes_of()
    lengths = r.lengths[...]
    whole = lengths[:, 0:1] == SLOT
    total = jnp.sum(lengths, axis=1, keepdims=True)

    def gather(buf, send, recv):
        def copy_of(index):
            if index == 0:
                rows, to = block_rows(head), sib
            elif index < 3:
                rows, to = block_rows(head, 128, (index - 1) * 128), far
            else:
                rows, to = block_rows(far, 128, (index - 3) * 128), sib
            return push(buf.at[rows, :], buf.at[rows, :], send.at[index], recv.at[index], (dp, to))

        def arrival(index):
            return copy_of(index)

        def begin():
            for index in (1, 2, 0):
                start(lambda index=index: copy_of(index))

        def wait(index):
            copy_of(index).wait_recv()

        def relay():
            for index in (1, 2):
                wait(index)
                start(lambda index=index: copy_of(index + 2))

        def rest():
            for index in (3, 4):
                wait(index)

        return begin, wait, relay, rest

    n_begin, n_wait, n_relay, n_rest = gather(r.nall, r.ns, r.nr)
    d_begin, d_wait, d_relay, d_rest = gather(r.dall, r.ds, r.dr)
    s_begin, s_wait, s_relay, s_rest = gather(r.sall, r.ss, r.sr)
    l_begin, l_wait, l_relay, l_rest = gather(r.lall, r.ls, r.lr)

    loaded("x")
    first = norm_parts(r.xv[...].astype(F32), gains[0:1, :], shifts[0:1, :])[2]
    r.nall[block_rows(head), :] = first.astype(BF)
    pl.semaphore_wait(barrier, 7)
    n_begin()
    position = head * BLOCK + lax.broadcasted_iota(jnp.int32, (BLOCK, 1), 0)
    loaded("d")
    r.dall[block_rows(head), :] = (r.dv[...].astype(F32) * jnp.where(position < total, 1.0, 0.0)).astype(BF)
    loaded("wqkv")
    aligned = lax.div(3 * head, 2) * 128
    odd = jnp.where(lax.rem(head, 2) == 1, 1.0, 0.0)
    on_heads = jnp.where(onlane < 192, 1.0, 0.0)

    def own_window(values):
        moved = pltpu.roll(values, 192, 1)
        return (values * (1.0 - odd) + moved * odd) * on_heads

    bias = []
    for part in range(3):
        window = pl.ds(pl.multiple_of(part * D + aligned, 128), 256)
        r.wqo[:, part * 256 : (part + 1) * 256] = own_window(r.wqkv[:, window].astype(F32)).astype(BF)
        bias.append(own_window(jnp.broadcast_to(r.full_bias[:, window], (8, 256)))[0:1])
    bias = jnp.concatenate(bias, axis=1)

    aux_k = jnp.where((onlane >= 196) & (onlane < 199), 1.0, 0.0)
    aux_v = jnp.where((onlane >= 192) & (onlane < 199) & (onlane != 195), 1.0, 0.0)
    on_aux = jnp.where(onlane >= 192, 1.0, 0.0)

    def project(block):
        rows = block_rows(block)
        projected = (nn(r.nall[rows, :], r.wqo[...]) + bias).astype(BF).astype(F32)
        r.qb[rows, :] = (projected[:, :256] * 0.125 + lane_is(192 + block)).astype(BF)
        off = jnp.where((onlane >= 192) & (onlane < 196) & (onlane != 192 + block), 1.0, 0.0)
        r.kb[rows, :] = (projected[:, 256:512] + (aux_k + off * jnp.where(whole, 0.0, FAR))).astype(BF)
        r.vb[rows, :] = (projected[:, 512:] + aux_v).astype(BF)

    project(head)
    n_wait(0)
    project(sib)
    n_relay()
    project(far)
    d_begin()
    n_rest()
    project(diag)

    def mix_copy(code):
        rows = block_rows(peer(code))
        return push(r.mix.at[rows, :], r.mixin.at[head], r.ms.at[code - 1], r.mr.at[code - 1], (dp, peer(code)))

    small_lane = lax.broadcasted_iota(jnp.int32, (1, 128), 1)

    def attend(step, carry):
        code = 3 - step
        block = peer(code)
        rows = block_rows(block)
        queries = r.qb[rows, :]
        mixed = jnp.zeros((BLOCK, 256), F32)
        tops = []
        for n in range(3):
            scores = nt(queries * (head_mask(n) + on_aux).astype(BF), r.kb[...])
            top = jnp.max(scores, axis=1, keepdims=True)
            weights = jnp.exp(scores - top).astype(BF)
            mixed += nn(weights, r.vb[...] * (head_mask(n) + lane_is(192 + n)).astype(BF))
            tops.append(top)
        lse = jnp.zeros((BLOCK, 128), F32)
        scale = jnp.zeros((BLOCK, 256), F32)
        for n in range(3):
            row_sum = jnp.sum(mixed * lane_is(192 + n), axis=1, keepdims=True)
            lse += (tops[n] + jnp.log(row_sum)) * jnp.where(small_lane == n, 1.0, 0.0)
            scale += (1.0 / row_sum) * head_mask(n)
        place = block * BLOCK + lax.broadcasted_iota(jnp.int32, (BLOCK, 1), 0)
        mixed = jnp.where(place < total, mixed * scale, r.vb[rows, :].astype(F32) * on_heads)
        r.exact[rows, :] = mixed
        r.lse[rows, :] = lse
        r.mix[rows, :] = mixed.astype(BF)

        @pl.when(step < 3)
        def _():
            mix_copy(code).start()

        return carry

    lax.fori_loop(0, 4, attend, 0)
    r.mixin[head] = r.mix[block_rows(head), :]
    d_relay()

    loaded("wout")
    loaded("wup")
    loaded("wdown")
    for code in (3, 2, 1):
        mix_copy(code).wait_recv()
    for group in range(4):
        r.wqo[0:256, group * 192 : (group + 1) * 192] = r.mixin[group][:, :192]
    hidden = r.xv[...].astype(F32) + nn(r.wqo[0:256, :], r.wout[...]) + biases[0:1, :]
    unit, inverse, normed = norm_parts(hidden, gains[1:2, :], shifts[1:2, :])
    second = normed.astype(BF)
    r.sall[block_rows(head), :] = second
    s_begin()
    grad_low = r.dall[block_rows(head), :]
    down = jnp.zeros((BLOCK, D), F32)
    back = jnp.zeros((BLOCK, D), F32)
    for tile in range(4):
        cut = slice(tile * D, (tile + 1) * D)
        up = nn(second, r.wup[:, cut]) + r.up_bias[:, cut]
        value, slope = gelu_parts(up)
        w_down = r.big[cut, 0:D]
        down += nn(value.astype(BF), w_down)
        grad_up = nt(grad_low, w_down) * slope
        back += nt(grad_up.astype(BF), r.wup[:, cut])
        if tile == 2:
            s_relay()
    r.block_out[...] = (hidden + down + biases[1:2, :]).astype(BF)
    grad_block = grad_low.astype(F32)
    grad_hidden = grad_block + norm_back(back, unit, inverse, gains[1:2, :])
    r.gh[...] = grad_hidden
    r.lall[block_rows(head), :] = grad_hidden.astype(BF)
    l_begin()
    r.vec[...] = jnp.zeros_like(r.vec)
    r.vec[1:2, :] = jnp.sum(back * unit, axis=0, keepdims=True)
    r.vec[3:4, :] = jnp.sum(back, axis=0, keepdims=True)
    r.vec[6:7, :] = jnp.sum(grad_hidden, axis=0, keepdims=True)
    r.vec[7:8, :] = jnp.sum(grad_block, axis=0, keepdims=True)

    loaded("wuo")
    loaded("wdo")
    loaded("woo")
    for wait in (s_wait, d_wait):
        wait(0)
    s_rest()
    d_rest()
    own_bias = jnp.concatenate(
        [r.up_bias[:, pl.ds(pl.multiple_of((4 * j + head) * 128, 128), 128)] for j in range(6)], axis=1
    )

    def feed(step, sums):
        rows = block_rows(peer(step))
        up = nn(r.sall[rows, :], r.wuo[...]) + own_bias
        value, slope = gelu_parts(up)
        r.act[rows, :] = value.astype(BF)
        grad_up = nt(r.dall[rows, :], r.wdo[...]) * slope
        r.gup[rows, :] = grad_up.astype(BF)
        return sums + jnp.sum(grad_up, axis=0, keepdims=True)

    sums = lax.fori_loop(0, 3, feed, jnp.zeros((1, D), F32))
    l_relay()
    sums = feed(jnp.int32(3), sums)
    r.small[...] = jnp.zeros_like(r.small)
    for j in range(6):
        number = 4 * j + head
        shard = lax.div(number, 3)
        r.small[lax.rem(shard, 2), lax.div(shard, 2), pl.ds(8 + lax.rem(number, 3), 1), :] = sums[
            :, j * 128 : (j + 1) * 128
        ]

    def regular(name):
        own, ybuf, zbuf, fin = (getattr(r, part + name) for part in ("p", "y", "z", "f"))
        sems = [getattr(r, part + name + end) for part in ("y", "z", "f") for end in ("s", "r")]
        ys, yr, zs, zr, fs, fr = sems

        def y_copy(k):
            src = own.at[z_shard(k) * 2 + (1 - y)]
            return push(src, ybuf.at[k], ys.at[k], yr.at[k], (other_y, head))

        def z_copy(k):
            shard = z_shard(k) * 2 + y
            return push(own.at[shard], zbuf.at[k], zs.at[k], zr.at[k], (shard, head))

        def f_copy(code):
            place = far if code == 3 else head
            to = far if code == 2 else sib
            return push(fin.at[place], fin.at[place], fs.at[code - 1], fr.at[code - 1], (dp, to))

        def begin():
            for k in (1, 2, 3, 0):
                start(lambda k=k: y_copy(k))

        def pair(k, last=None):
            y_copy(k).wait_recv()
            at = z_shard(k) * 2 + y
            own[at] = (own[at].astype(F32) + ybuf[k].astype(F32)).astype(BF)
            if isinstance(k, int):
                if k:
                    start(lambda: z_copy(k))
            else:

                @pl.when(k > 0)
                def _():
                    z_copy(k).start()

        def total_up():
            for k in (1, 2, 3):
                z_copy(k).wait_recv()
            value = own[dp].astype(F32)
            for k in (1, 2, 3):
                value += zbuf[k].astype(F32)
            fin[head] = value.astype(BF)
            for code in (2, 1):
                start(lambda code=code: f_copy(code))

        def relay():
            f_copy(2).wait_recv()
            start(lambda: f_copy(3))

        def rest():
            f_copy(1).wait_recv()
            f_copy(3).wait_recv()

        def pair_sends():
            for k in (1, 2, 3):
                sent.append((lambda k=k: z_copy(k), None))

        return begin, pair, total_up, relay, rest, pair_sends

    def irregular(name, number_of, owner_of):
        own, ybuf, zbuf, fin = (getattr(r, part + name) for part in ("p", "y", "z", "f"))
        sems = [getattr(r, part + name + end) for part in ("y", "z", "f") for end in ("s", "r")]
        ys, yr, zs, zr, fs, fr = sems

        def facts(j):
            number = number_of(j)
            shard = lax.div(number, 3)
            return shard, lax.div(shard, 2), lax.rem(shard, 2), lax.rem(number, 3)

        def y_copy(j):
            return push(own.at[j], ybuf.at[j], ys.at[j], yr.at[j], (other_y, head))

        def z_copy(j):
            shard, shard_z, shard_y, place = facts(j)
            slot = (lax.rem(shard_z + 4 - z, 4) - 1) * 3 + place
            return push(own.at[j], zbuf.at[slot], zs.at[j], zr.at[slot], (shard, head))

        def z_arrival(j, k):
            slot = (k - 1) * 3 + facts(j)[3]
            return push(own.at[j], zbuf.at[slot], zs.at[j], zr.at[slot], (dp, sib)), slot

        def f_copy(code, place):
            index = (code - 1) * 3 + place
            to = far if code == 2 else sib
            return push(fin.at[place], fin.at[place], fs.at[index], fr.at[index], (dp, to))

        def begin(these=range(6)):
            for j in these:
                start(lambda j=j: y_copy(j), facts(j)[2] != y)

        def z_goes(j):
            shard, shard_z, shard_y, place = facts(j)
            return (shard_y == y) & (shard_z != z)

        def pair(j):
            @pl.when(facts(j)[2] == y)
            def _():
                y_copy(j).wait_recv()
                own[j] = (own[j].astype(F32) + ybuf[j].astype(F32)).astype(BF)

            @pl.when(z_goes(j))
            def _():
                z_copy(j).start()

        def pair_sends():
            for j in range(6):
                sent.append((lambda j=j: z_copy(j), z_goes(j)))

        def total_up():
            for j in range(6):
                shard, shard_z, shard_y, place = facts(j)

                def body(j=j, place=place):
                    value = own[j].astype(F32)
                    for k in (1, 2, 3):
                        copy, slot = z_arrival(j, k)
                        copy.wait_recv()
                        value += zbuf[slot].astype(F32)
                    fin[place] = value.astype(BF)
                    f_copy(2, place).start()
                    f_copy(1, place).start()

                pl.when(shard == dp)(body)

        def relay():
            for place in range(3):
                owner = owner_of(3 * dp + place)
                for code in (1, 2):
                    sent.append((lambda code=code, place=place: f_copy(code, place), owner == head))

                def body(place=place):
                    f_copy(2, place).wait_recv()
                    f_copy(3, place).start()

                pl.when(owner == far)(body)
                sent.append((lambda place=place: f_copy(3, place), owner == far))

        def rest():
            for place in range(3):
                owner = owner_of(3 * dp + place)
                for code, source in ((1, sib), (3, diag)):
                    pl.when(owner == source)(lambda code=code, place=place: f_copy(code, place).wait_recv())

        return begin, pair, total_up, relay, rest, pair_sends

    dn_begin, dn_pair, dn_total, dn_relay, dn_rest, dn_sends = regular("dn")
    ou_begin, ou_pair, ou_total, ou_relay, ou_rest, ou_sends = regular("ou")
    up_begin, up_pair, up_total, up_relay, up_rest, up_sends = irregular(
        "up", lambda j: 4 * j + head, lambda number: lax.rem(number, 4)
    )
    qk_begin, qk_pair, qk_total, qk_relay, qk_rest, qk_sends = irregular(
        "qk",
        lambda j: (j // 2) * 8 + 2 * head + j % 2,
        lambda number: lax.div(lax.rem(number, 8), 2),
    )

    r.pdn[...] = tn(r.dall[...], r.act[...]).astype(BF).reshape(8, 96, D)
    dn_begin()
    r.pup[...] = tn(r.gup[...], r.sall[...]).astype(BF).reshape(6, 128, D)
    up_begin()

    l_wait(0)
    l_rest()
    r.woo[192:256, :] = jnp.zeros((64, D), BF)
    r.gm[...] = nt(r.lall[...], r.woo[...]).astype(BF)
    r.pou[...] = tn(r.lall[...], r.mix[...]).astype(BF).reshape(8, 96, 256)
    ou_begin()
    q_aug, g_aug = r.act, r.gup
    for n in range(3):
        mask = head_mask(n)

        def augment(block, carry, n=n, mask=mask):
            rows = pl.ds(pl.multiple_of(block * 256, 256), 256)
            grads = r.gm[rows, :].astype(F32) * mask
            inner = jnp.sum(grads * r.exact[rows, :], axis=1, keepdims=True)
            queries = r.qb[rows, :].astype(F32) * (mask + on_aux)
            for place, part in enumerate(split_three(-r.lse[rows, :][:, n : n + 1])):
                queries = queries + part * lane_is(196 + place)
            for place, part in enumerate(split_three(-inner)):
                grads = grads + part * lane_is(196 + place)
            q_aug[rows, n * 256 : (n + 1) * 256] = queries.astype(BF)
            g_aug[rows, n * 256 : (n + 1) * 256] = grads.astype(BF)
            return carry

        lax.fori_loop(0, 4, augment, 0)

    def kv_copy(code):
        rows = block_rows(peer(code))
        return push(r.dkv.at[rows, :], r.kvin.at[head], r.kvs.at[code - 1], r.kvr.at[code - 1], (dp, peer(code)))

    def q_copy(code):
        rows = block_rows(peer(code))
        return push(r.dq.at[rows, :], r.qin.at[head], r.qs.at[code - 1], r.qr.at[code - 1], (dp, peer(code)))

    def attend_back(step, carry):
        code = 3 - step
        block = peer(code)
        rows = block_rows(block)
        key_grad = jnp.zeros((BLOCK, 256), F32)
        value_grad = jnp.zeros((BLOCK, 256), F32)
        for n in range(3):
            mask = head_mask(n)
            lanes = slice(n * 256, (n + 1) * 256)
            probs = jnp.exp(nt(r.kb[rows, :], q_aug[:, lanes]))
            grad_scores = (probs * nt(r.vb[rows, :], g_aug[:, lanes])).astype(BF)
            r.big[pl.ds(pl.multiple_of(n * SLOT + block * BLOCK, 256), BLOCK), :] = grad_scores
            key_grad += nn(grad_scores, q_aug[:, lanes]) * mask
            value_grad += nn(probs.astype(BF), g_aug[:, lanes]) * mask
        r.dkv[rows, 0:192] = key_grad[:, :192].astype(BF)
        r.dkv[rows, 192:384] = value_grad[:, :192].astype(BF)

        @pl.when(step < 3)
        def _():
            kv_copy(code).start()

        dn_pair(lax.rem(step + 1, 4))
        up_pair(step)
        return carry

    lax.fori_loop(0, 4, attend_back, 0)
    r.kvin[head] = r.dkv[block_rows(head), :]

    def query_back(step, carry):
        code = 3 - step
        block = peer(code)
        rows = block_rows(block)
        query_grad = jnp.zeros((BLOCK, 256), F32)
        for n in range(3):
            part = r.big[n * SLOT : (n + 1) * SLOT, pl.ds(pl.multiple_of(block * BLOCK, 256), BLOCK)]
            query_grad += tn(part, r.kb[...] * head_mask(n).astype(BF))
        r.dq[rows, :] = (query_grad * 0.125).astype(BF)

        @pl.when(step < 3)
        def _():
            q_copy(code).start()

        return carry

    lax.fori_loop(0, 4, query_back, 0)
    r.qin[head] = r.dq[block_rows(head), :]
    up_pair(4)
    up_pair(5)
    for k in (1, 2, 3, 0):
        ou_pair(k)
    dn_sends()
    up_sends()
    r.pqk[2:6] = tn(r.dkv[...], r.nall[...]).astype(BF).reshape(4, 96, D)
    qk_begin(range(2, 6))
    r.pqk[0:2] = tn(r.dq[...], r.nall[...])[:192].astype(BF).reshape(2, 96, D)
    qk_begin(range(2))
    query_sum = jnp.sum(r.dq[...].astype(F32), axis=0, keepdims=True)
    value_sum = jnp.sum(r.dkv[:, 128:384].astype(F32), axis=0, keepdims=True)
    for group in range(4):
        mine = jnp.where(head == group, 1.0, 0.0)
        r.vec[4:5, group * 192 : (group + 1) * 192] = query_sum[:, :192] * mine
        r.vec[5:6, group * 192 : (group + 1) * 192] = value_sum[:, 64:] * mine
    dn_total()
    up_total()
    ou_total()

    for code in (3, 2, 1):
        kv_copy(code).wait_recv()
        q_copy(code).wait_recv()
    for group in range(4):
        lanes = slice(group * 192, (group + 1) * 192)
        r.wuo[0:256, lanes] = r.qin[group][:, :192]
        r.wuo[256:512, lanes] = r.kvin[group][:, :192]
        r.wuo[512:768, lanes] = r.kvin[group][:, 192:]
    grad_first = nt(r.wuo[0:256, :], r.wqkv[:, 0:D])
    grad_first += nt(r.wuo[256:512, :], r.wqkv[:, D : 2 * D])
    grad_first += nt(r.wuo[512:768, :], r.wqkv[:, 2 * D :])
    unit, inverse, _ = norm_parts(r.xv[...].astype(F32), gains[0:1, :], shifts[0:1, :])
    r.grad_inputs[...] = r.gh[...] + norm_back(grad_first, unit, inverse, gains[0:1, :])
    r.vec[0:1, :] = jnp.sum(grad_first * unit, axis=0, keepdims=True)
    r.vec[2:3, :] = jnp.sum(grad_first, axis=0, keepdims=True)
    for shard in range(8):
        r.small[shard % 2, shard // 2, 0:8, 0:96] = r.vec[:, shard * 96 : (shard + 1) * 96]

    def small_y():
        return push(r.small.at[1 - y], r.ysm, r.ysms.at[0], r.ysmr.at[0], (other_y, head))

    def small_z(k):
        return push(
            r.small.at[y, z_shard(k)], r.zsm.at[k], r.zsms.at[k], r.zsmr.at[k], (z_shard(k) * 2 + y, head)
        )

    def small_f(code):
        return push(r.fsm.at[head], r.fsm.at[head], r.fsms.at[code - 1], r.fsmr.at[code - 1], (dp, peer(code)))

    start(small_y)
    for step in (2, 3, 4, 5, 0, 1):
        qk_pair(step)
    qk_sends()
    small_y().wait_recv()
    r.small[y] = r.small[y] + r.ysm[...]
    for k in (1, 2, 3):
        start(lambda k=k: small_z(k))
    dn_relay()
    up_relay()
    ou_relay()
    qk_total()
    for k in (1, 2, 3):
        small_z(k).wait_recv()
    r.fsm[head] = r.small[y, z] + r.zsm[1] + r.zsm[2] + r.zsm[3]
    for code in (2, 3, 1):
        start(lambda code=code: small_f(code))
    qk_relay()
    dn_rest()
    up_rest()
    ou_rest()
    qk_rest()
    for code in (2, 3, 1):
        small_f(code).wait_recv()
    r.fsum[...] = r.fsm[0] + r.fsm[1] + r.fsm[2] + r.fsm[3]
    for make, cond in sent:
        when(cond, lambda make=make: make().wait_send())
    for code in (1, 2, 3):
        mix_copy(code).wait_send()
        kv_copy(code).wait_send()
        q_copy(code).wait_send()


def per_device(x, norm_gains, norm_shifts, w_qkv, qv_bias, w_out, out_biases, w_up, up_bias, w_down, lengths, d_out):
    full_bias = jnp.concatenate([qv_bias[0], jnp.zeros_like(qv_bias[0]), qv_bias[1]]).astype(F32).reshape(1, 3 * D)
    values = dict(
        x=x[0], gains=norm_gains, shifts=norm_shifts, w_qkv=w_qkv, full_bias=full_bias, w_out=w_out, biases=out_biases,
        w_up=w_up, up_bias=up_bias.astype(F32).reshape(1, FF), w_down=w_down, lengths=lengths, d_out=d_out[0],
    )
    place = {True: pl.BlockSpec(memory_space=pl.ANY), False: pl.BlockSpec(memory_space=pltpu.VMEM)}
    block_out, grad_inputs, fup, fqk, fdn, fou, fsum = pl.pallas_call(
        one_kernel,
        out_shape=[jax.ShapeDtypeStruct(shape, kind) for _, shape, kind in OUTPUTS],
        in_specs=[place[name in IN_PLACE] for name in INPUTS],
        out_specs=[place[False]] * len(OUTPUTS),
        scratch_shapes=[pltpu.VMEM(shape, kind) for _, shape, kind in BUFFERS]
        + [pltpu.SemaphoreType.DMA((count,)) for _, count in SEMAPHORES],
        compiler_params=pltpu.CompilerParams(
            collective_id=0, has_side_effects=True, vmem_limit_bytes=VMEM_LIMIT
        ),
        name="block",
    )(*(values[name] for name in INPUTS))
    down = fdn.reshape(4, 96, 6, 128).transpose(2, 0, 3, 1).reshape(FF, 96)
    return (
        block_out[None],
        grad_inputs[None],
        fsum[0:2, 0:96],
        fsum[2:4, 0:96],
        fqk.reshape(288, D).T.astype(F32),
        fsum[4:6, 0:96],
        fou[:, :, :192].transpose(0, 2, 1).reshape(D, 96).astype(F32),
        fsum[6:8, 0:96],
        fup.reshape(384, D).T.astype(F32),
        fsum[8:11].reshape(384),
        down.astype(F32),
    )


def solution(mesh):
    split = P("dp", "head", None)
    placed = (split,) + (P(),) * 9 + (P("dp", None), split)
    return jax.shard_map(
        per_device if dict(mesh.shape) == {"dp": 8, "head": 4} else general_device,
        mesh=mesh,
        in_specs=placed,
        out_specs=(split, split) + (P(None, "dp"),) * 7 + (P("dp"), P(None, "dp")),
        check_vma=False,
    )
```

```python
import functools

import jax
import jax.numpy as jnp
from jax import lax
from jax.experimental import pallas as pl
from jax.experimental.pallas import tpu as pltpu
from jax.sharding import PartitionSpec as P

D = 768
HEADS = 12
HDIM = 64
FF = 3072
SLOT = 1024
EPSILON = 1e-06
BF = jnp.bfloat16
F32 = jnp.float32
FAR = -1e30
VMEM_LIMIT = 63 * 1024 * 1024


def nn(a, b):
    return lax.dot_general(a, b, (((1,), (0,)), ((), ())), preferred_element_type=F32)


def nt(a, b):
    return lax.dot_general(a, b, (((1,), (1,)), ((), ())), preferred_element_type=F32)


def tn(a, b):
    return lax.dot_general(a, b, (((0,), (0,)), ((), ())), preferred_element_type=F32)


def norm_parts(values, norm_gain, norm_shift):
    average = jnp.mean(values, axis=-1, keepdims=True)
    centered = values - average
    variance = jnp.mean(centered * centered, axis=-1, keepdims=True)
    inverse = lax.rsqrt(variance + EPSILON)
    unit = centered * inverse
    return unit, inverse, unit * norm_gain + norm_shift


def norm_back(grad_normed, unit, inverse, norm_gain):
    grad_unit = grad_normed * norm_gain
    first_mean = jnp.mean(grad_unit, axis=-1, keepdims=True)
    second_mean = jnp.mean(grad_unit * unit, axis=-1, keepdims=True)
    return inverse * (grad_unit - first_mean - unit * second_mean)


def gelu_parts(values):
    cumulative = 0.5 + 0.5 * lax.erf(values * 0.7071067811865476)
    density = jnp.exp(values * values * -0.5) * 0.3989422804014327
    return values * cumulative, cumulative + values * density


def lanes_of(width=256):
    return lax.broadcasted_iota(jnp.int32, (1, width), 1)


def head_mask(head):
    lane = lanes_of()
    return jnp.where((lane >= head * HDIM) & (lane < (head + 1) * HDIM), 1.0, 0.0)


def lane_is(index):
    return jnp.where(lanes_of() == index, 1.0, 0.0)


def split_three(column):
    high = column.astype(BF).astype(F32)
    rest = column - high
    middle = rest.astype(BF).astype(F32)
    return high, middle, rest - middle


def attend_forward(normed, weight, bias, lengths, q_ref, k_ref, v_ref, mixed_ref, exact_ref, lse_ref):
    whole = lengths[:, 0:1] == SLOT
    total = jnp.sum(lengths, axis=1, keepdims=True)
    onlane = lanes_of()
    aux_k = jnp.where((onlane >= 196) & (onlane < 199), 1.0, 0.0)
    aux_v = jnp.where((onlane >= 192) & (onlane < 199) & (onlane != 195), 1.0, 0.0)
    for block in range(4):
        rows = pl.ds(block * 256, 256)
        projected = nn(normed[rows, :], weight[...]) + bias
        projected = projected.astype(BF).astype(F32)
        q_ref[rows, :] = (projected[:, :256] * 0.125 + lane_is(192 + block)).astype(BF)
        other = jnp.where((onlane >= 192) & (onlane < 196) & (onlane != 192 + block), 1.0, 0.0)
        far = other * jnp.where(whole, 0.0, FAR)
        k_ref[rows, :] = (projected[:, 256:512] + (aux_k + far)).astype(BF)
        v_ref[rows, :] = (projected[:, 512:] + aux_v).astype(BF)
    on_aux = jnp.where(onlane >= 192, 1.0, 0.0)

    def block_step(block, carry):
        rows = pl.ds(pl.multiple_of(block * 256, 256), 256)
        queries = q_ref[rows, :]
        mixed = jnp.zeros((256, 256), F32)
        tops = []
        for head in range(3):
            scores = nt(queries * (head_mask(head) + on_aux).astype(BF), k_ref[...])
            top = jnp.max(scores, axis=1, keepdims=True)
            weights = jnp.exp(scores - top).astype(BF)
            mixed += nn(weights, v_ref[...] * (head_mask(head) + lane_is(192 + head)).astype(BF))
            tops.append(top)
        lse = jnp.zeros((256, 128), F32)
        scale = jnp.zeros((256, 256), F32)
        small = lax.broadcasted_iota(jnp.int32, (1, 128), 1)
        for head in range(3):
            row_sum = jnp.sum(mixed * lane_is(192 + head), axis=1, keepdims=True)
            lse += (tops[head] + jnp.log(row_sum)) * jnp.where(small == head, 1.0, 0.0)
            scale += (1.0 / row_sum) * head_mask(head)
        mixed = mixed * scale
        position = block * 256 + lax.broadcasted_iota(jnp.int32, (256, 1), 0)
        on_heads = jnp.where(onlane < 192, 1.0, 0.0)
        mixed = jnp.where(position < total, mixed, v_ref[rows, :].astype(F32) * on_heads)
        exact_ref[rows, :] = mixed
        mixed_ref[rows, :] = mixed[:, :192].astype(BF)
        lse_ref[rows, :] = lse
        return carry

    lax.fori_loop(0, 4, block_step, 0)


def attend_backward(q_ref, k_ref, v_ref, exact_ref, lse_ref, grad_mixed, q_aug, g_aug, scores_low, dq_acc, dk_acc, dv_acc):
    for head in range(3):
        mask = head_mask(head)

        def augment(block, carry):
            rows = pl.ds(pl.multiple_of(block * 256, 256), 256)
            grads = grad_mixed[rows, :].astype(F32) * mask
            inner = jnp.sum(grads * exact_ref[rows, :], axis=1, keepdims=True)
            lse = lse_ref[rows, :][:, head : head + 1]
            queries = q_ref[rows, :].astype(F32) * (mask + jnp.where(lanes_of() >= 192, 1.0, 0.0))
            for place, part in enumerate(split_three(-lse)):
                queries = queries + part * lane_is(196 + place)
            for place, part in enumerate(split_three(-inner)):
                grads = grads + part * lane_is(196 + place)
            q_aug[rows, :] = queries.astype(BF)
            g_aug[rows, :] = grads.astype(BF)
            return carry

        lax.fori_loop(0, 4, augment, 0)

        def block_step(block, carry):
            rows = pl.ds(pl.multiple_of(block * 256, 256), 256)
            probs = jnp.exp(nt(k_ref[rows, :], q_aug[...]))
            grad_probs = nt(v_ref[rows, :], g_aug[...])
            grad_scores = (probs * grad_probs).astype(BF)
            scores_low[rows, :] = grad_scores
            key_part = nn(grad_scores, q_aug[...]) * mask
            value_part = nn(probs.astype(BF), g_aug[...]) * mask
            if head == 0:
                dk_acc[rows, :] = key_part
                dv_acc[rows, :] = value_part
            else:
                dk_acc[rows, :] += key_part
                dv_acc[rows, :] += value_part
            return carry

        lax.fori_loop(0, 4, block_step, 0)
        query_part = tn(scores_low[...], k_ref[...] * mask.astype(BF)) * 0.125
        if head == 0:
            dq_acc[...] = query_part
        else:
            dq_acc[...] += query_part


def forward_kernel(normed, weight, bias, lengths, q_ref, k_ref, v_ref, mixed_ref, exact_ref, lse_ref):
    attend_forward(normed, weight, bias[...], lengths[...], q_ref, k_ref, v_ref, mixed_ref, exact_ref, lse_ref)


def middle_kernel(
    mixed_in, x_in, d_low, w_out, w_up, w_down, gains, shifts, biases, up_bias,
    block_ref, second_ref, hid_ref, low_ref, sums_ref, mixed_rows, act_ref,
):
    rows = x_in.shape[0]
    for group in range(4):
        mixed_rows[:, group * 192 : (group + 1) * 192] = mixed_in[group]
    hidden = x_in[...].astype(F32) + nn(mixed_rows[...], w_out[...]) + biases[0:1, :]
    unit, inverse, normed = norm_parts(hidden, gains[1:2, :], shifts[1:2, :])
    second = normed.astype(BF)
    second_ref[...] = second
    grad_low = d_low[...]
    down = jnp.zeros((rows, D), F32)
    back = jnp.zeros((rows, D), F32)
    step = 768
    for tile in range(FF // step):
        cut = slice(tile * step, (tile + 1) * step)
        up = nn(second, w_up[:, cut]) + up_bias[:, cut]
        value, slope = gelu_parts(up)
        down += nn(value.astype(BF), w_down[cut, :])
        grad_up = nt(grad_low, w_down[cut, :]) * slope
        back += nt(grad_up.astype(BF), w_up[:, cut])
    block_ref[...] = (hidden + down + biases[1:2, :]).astype(BF)
    grad_block = grad_low.astype(F32)
    grad_hidden = grad_block + norm_back(back, unit, inverse, gains[1:2, :])
    hid_ref[...] = grad_hidden
    low_ref[...] = grad_hidden.astype(BF)
    sums_ref[...] = jnp.zeros_like(sums_ref)
    sums_ref[0:1, :] = jnp.sum(back * unit, axis=0, keepdims=True)
    sums_ref[1:2, :] = jnp.sum(back, axis=0, keepdims=True)
    sums_ref[2:3, :] = jnp.sum(grad_hidden, axis=0, keepdims=True)
    sums_ref[3:4, :] = jnp.sum(grad_block, axis=0, keepdims=True)


def feed_kernel(second, d_low, w_up, w_down, up_bias, up_grad, down_grad, bias_grad, act_ref, grad_ref):
    width = w_up.shape[1]
    bias_grad[...] = jnp.zeros_like(bias_grad)

    def step(block, carry):
        rows = pl.ds(pl.multiple_of(block * 256, 256), 256)
        up = nn(second[rows, :], w_up[...]) + up_bias[...]
        value, slope = gelu_parts(up)
        act_ref[rows, :] = value.astype(BF)
        grad_up = nt(d_low[rows, :], w_down[...]) * slope
        bias_grad[0:1, :] += jnp.sum(grad_up, axis=0, keepdims=True)
        grad_ref[rows, :] = grad_up.astype(BF)
        return carry

    lax.fori_loop(0, 4, step, 0)
    down_grad[...] = tn(d_low[...], act_ref[...]).astype(BF)
    up_grad[...] = tn(grad_ref[...], second[...]).astype(BF)


def backward_kernel(
    grad_low, w_out, normed, mixed, q_ref, k_ref, v_ref, exact_ref, lse_ref,
    grad_ref, out_grad, qkv_grad, bias_grad,
    grad_mixed, q_aug, g_aug, scores_low, dq_acc, dk_acc, dv_acc,
):
    padded = jnp.zeros((64, D), BF)
    weight = jnp.concatenate([w_out[...], padded], axis=0)
    grad_mixed[...] = nt(grad_low[...], weight).astype(BF)
    out_grad[...] = tn(grad_low[...], mixed[...]).astype(BF)
    attend_backward(q_ref, k_ref, v_ref, exact_ref, lse_ref, grad_mixed, q_aug, g_aug, scores_low, dq_acc, dk_acc, dv_acc)
    for place, part in enumerate((dq_acc, dk_acc, dv_acc)):
        grad_ref[:, place * 192 : (place + 1) * 192] = part[:, :192].astype(BF)
    bias_grad[...] = jnp.zeros_like(bias_grad)
    bias_grad[0:1, :] = jnp.sum(grad_ref[...].astype(F32), axis=0, keepdims=True)
    qkv_grad[...] = tn(grad_ref[...], normed[...]).astype(BF)


def last_kernel(grad_in, w_qkv, x_in, hid, gains, shifts, out_ref, sums_ref, grad_rows):
    for part in range(3):
        for group in range(4):
            place = part * D + group * 192
            grad_rows[:, place : place + 192] = grad_in[group][:, part * 192 : (part + 1) * 192]
    grad_first = nt(grad_rows[...], w_qkv[...])
    unit, inverse, _ = norm_parts(x_in[...].astype(F32), gains[0:1, :], shifts[0:1, :])
    out_ref[...] = hid[...] + norm_back(grad_first, unit, inverse, gains[0:1, :])
    sums_ref[...] = jnp.zeros_like(sums_ref)
    sums_ref[0:1, :] = jnp.sum(grad_first * unit, axis=0, keepdims=True)
    sums_ref[1:2, :] = jnp.sum(grad_first, axis=0, keepdims=True)


def whole_call(kernel, outs, scratch=(), name=None):
    return pl.pallas_call(
        kernel,
        out_shape=[jax.ShapeDtypeStruct(*out) for out in outs],
        scratch_shapes=[pltpu.VMEM(*item) for item in scratch],
        compiler_params=pltpu.CompilerParams(vmem_limit_bytes=VMEM_LIMIT),
        name=name,
    )


def general_device(x, norm_gains, norm_shifts, w_qkv, qv_bias, w_out, out_biases, w_up, up_bias, w_down, lengths, d_out):
    groups = lax.axis_size("head")
    shards = lax.axis_size("dp")
    group = lax.axis_index("head")
    rows = x.shape[1]
    own = D // groups
    x = x[0]
    gains = norm_gains.astype(F32)
    shifts = norm_shifts.astype(F32)
    biases = out_biases.astype(F32)
    up_shift = up_bias.astype(F32)
    full_bias = jnp.stack([qv_bias[0], jnp.zeros_like(qv_bias[0]), qv_bias[1]]).astype(F32)

    weight_own = lax.dynamic_index_in_dim(w_qkv.reshape(D, 3, groups, own), group, 2, False)
    weight_own = jnp.pad(weight_own, ((0, 0), (0, 0), (0, 256 - own))).reshape(D, 768)
    bias_own = lax.dynamic_index_in_dim(full_bias.reshape(3, groups, own), group, 1, False)
    bias_own = jnp.pad(bias_own, ((0, 0), (0, 256 - own))).reshape(1, 768)
    out_own = lax.dynamic_slice_in_dim(w_out, group * own, own, 0)
    unit_ff = FF // (shards * groups)
    up_own = lax.dynamic_index_in_dim(w_up.reshape(D, shards, groups, unit_ff), group, 2, False).reshape(D, D)
    down_own = lax.dynamic_index_in_dim(w_down.reshape(shards, groups, unit_ff, D), group, 1, False).reshape(D, D)
    ub_own = lax.dynamic_index_in_dim(up_shift.reshape(shards, groups, unit_ff), group, 1, False).reshape(1, D)

    normed = norm_parts(x.astype(F32), gains[0], shifts[0])[2].astype(BF)
    normed_all = lax.all_gather(normed, "head", axis=0, tiled=True)
    total = jnp.sum(lengths[0])
    position = group * rows + jnp.arange(rows, dtype=jnp.int32)
    d_low = jnp.where((position < total)[:, None], d_out[0], jnp.zeros_like(d_out[0]))
    d_all = lax.all_gather(d_low, "head", axis=0, tiled=True)

    q, k, v, mixed, exact, lse = whole_call(
        forward_kernel,
        [((SLOT, 256), BF)] * 3 + [((SLOT, own), BF), ((SLOT, 256), F32), ((SLOT, 128), F32)],
        name="attend_forward",
    )(normed_all, weight_own, bias_own, lengths)
    mixed_in = lax.all_to_all(mixed.reshape(groups, rows, own), "head", 0, 0, tiled=True)
    block_out, second, hid, hid_low, sums_mid = whole_call(
        middle_kernel,
        [((rows, D), BF), ((rows, D), BF), ((rows, D), F32), ((rows, D), BF), ((8, D), F32)],
        [((rows, D), BF), ((rows, FF), BF)],
        name="middle",
    )(mixed_in, x, d_low, w_out, w_up, w_down, gains, shifts, biases, up_shift.reshape(1, FF))
    second_all = lax.all_gather(second, "head", axis=0, tiled=True)
    low_all = lax.all_gather(hid_low, "head", axis=0, tiled=True)
    up_grad, down_grad, ub_grad = whole_call(
        feed_kernel,
        [((D, D), BF), ((D, D), BF), ((8, D), F32)],
        [((SLOT, D), BF), ((SLOT, D), BF)],
        name="feed",
    )(second_all, d_all, up_own, down_own, ub_own)
    grad_own, out_grad, qkv_grad, qkv_sum = whole_call(
        backward_kernel,
        [((SLOT, 3 * own), BF), ((D, own), BF), ((3 * own, D), BF), ((8, 3 * own), F32)],
        [((SLOT, 256), BF)] * 3 + [((SLOT, SLOT), BF)] + [((SLOT, 256), F32)] * 3,
        name="attend_backward",
    )(low_all, out_own, normed_all, mixed, q, k, v, exact, lse)
    grad_in = lax.all_to_all(grad_own.reshape(groups, rows, 3 * own), "head", 0, 0, tiled=True)
    grad_inputs, sums_last = whole_call(
        last_kernel,
        [((rows, D), F32), ((8, D), F32)],
        [((rows, 3 * D), BF)],
        name="last",
    )(grad_in, w_qkv, x, hid, gains, shifts)

    def scatter(values):
        return lax.psum_scatter(values, "dp", scatter_dimension=0, tiled=True)

    up_part = lax.all_gather(scatter(up_grad), "head", axis=0, tiled=True)
    down_part = lax.all_gather(scatter(down_grad), "head", axis=1, tiled=True)
    out_part = lax.all_gather(scatter(out_grad), "head", axis=1, tiled=True)
    down_out = down_part.astype(F32).T.reshape(groups, shards, unit_ff, D // shards)
    down_out = down_out.transpose(1, 0, 2, 3).reshape(FF, D // shards)
    spread = jnp.zeros((3, groups, own, D), BF)
    spread = lax.dynamic_update_slice(spread, qkv_grad.reshape(3, 1, own, D), (0, group, 0, 0))
    qkv_part = lax.psum(scatter(spread.reshape(3 * D, D)), "head")

    def place_rows(values):
        parts = values.reshape(3, own)
        empty = jnp.zeros((3, groups, own), F32)
        return lax.dynamic_update_slice(empty, parts[:, None], (0, group, 0)).reshape(3, D)

    bias_rows = place_rows(qkv_sum[0])
    ub_rows = lax.dynamic_update_slice(
        jnp.zeros((shards, groups, unit_ff), F32), ub_grad[0].reshape(shards, 1, unit_ff), (0, group, 0)
    ).reshape(4, D)
    small = jnp.concatenate([sums_last[0:2], sums_mid[0:4], bias_rows[0:1], bias_rows[2:3], ub_rows], axis=0)
    small = lax.psum(small, ("dp", "head"))
    shard = lax.axis_index("dp")

    def cut(values):
        width = D // shards
        return lax.dynamic_slice_in_dim(values, shard * width, width, 1)

    ub_out = lax.dynamic_slice_in_dim(small[8:12].reshape(FF), shard * (FF // shards), FF // shards, 0)
    return (
        block_out[None],
        grad_inputs[None],
        cut(jnp.stack([small[0], small[2]])),
        cut(jnp.stack([small[1], small[3]])),
        qkv_part.astype(F32).T,
        cut(small[6:8]),
        out_part.astype(F32).T,
        cut(small[4:6]),
        up_part.astype(F32).T,
        ub_out,
        down_out,
    )


MESH = pl.DeviceIdType.MESH
BLOCK = 256

BUFFERS = (
    ("xv", (256, D), BF),
    ("dv", (256, D), BF),
    ("wqkv", (D, 3 * D), BF),
    ("wout", (D, D), BF),
    ("wup", (D, FF), BF),
    ("big", (3 * SLOT, SLOT), BF),
    ("wqo", (D, D), BF),
    ("wuo", (D, D), BF),
    ("wdo", (D, D), BF),
    ("woo", (256, D), BF),
    ("nall", (SLOT, D), BF),
    ("dall", (SLOT, D), BF),
    ("sall", (SLOT, D), BF),
    ("lall", (SLOT, D), BF),
    ("qb", (SLOT, 256), BF),
    ("kb", (SLOT, 256), BF),
    ("vb", (SLOT, 256), BF),
    ("mix", (SLOT, 256), BF),
    ("exact", (SLOT, 256), F32),
    ("lse", (SLOT, 128), F32),
    ("mixs", (4, 384, 128), BF),
    ("mixin", (4, 384, 128), BF),
    ("gh", (256, D), F32),
    ("act", (SLOT, D), BF),
    ("gup", (SLOT, D), BF),
    ("gm", (SLOT, 256), BF),
    ("dkv", (SLOT, 384), BF),
    ("dq", (SLOT, 256), BF),
    ("kvin", (4, 256, 384), BF),
    ("qs_", (4, 384, 128), BF),
    ("qin", (4, 384, 128), BF),
    ("pdy", (8, 96, 384), BF),
    ("pdz", (8, 96, 384), BF),
    ("pup", (6, D, 128), BF),
    ("pou", (8, 96, 256), BF),
    ("pqk", (6, 96, D), BF),
    ("ydy", (4, 96, 384), BF),
    ("ydz", (1, 96, 384), BF),
    ("yup", (6, D, 128), BF),
    ("you", (4, 96, 256), BF),
    ("yqk", (6, 96, D), BF),
    ("zdy", (4, 96, 384), BF),
    ("zdz", (4, 2, 96, 384), BF),
    ("zup", (12, D, 128), BF),
    ("zou", (4, 96, 256), BF),
    ("zqk", (9, 96, D), BF),
    ("vec", (8, D), F32),
    ("small", (2, 4, 16, 128), F32),
    ("ysm", (4, 16, 128), F32),
    ("zsm", (4, 16, 128), F32),
    ("fsm", (4, 16, 128), F32),
)
SEMAPHORES = (
    ("load", 22),
    ("ns", 5), ("nr", 5), ("ds", 5), ("dr", 5), ("ss", 5), ("sr", 5), ("ls", 5), ("lr", 5),
    ("ms", 3), ("mr", 3), ("kvs", 3), ("kvr", 3), ("qs", 3), ("qr", 3),
    ("ydys", 4), ("ydyr", 4), ("zdys", 4), ("zdyr", 4), ("fdys", 3), ("fdyr", 3),
    ("ydzs", 1), ("ydzr", 1), ("zdzs", 4), ("zdzr", 4), ("fdzs", 3), ("fdzr", 3),
    ("yous", 4), ("your", 4), ("zous", 4), ("zour", 4), ("fous", 3), ("four", 3),
    ("yups", 6), ("yupr", 6), ("zups", 6), ("zupr", 12), ("fups", 9), ("fupr", 9),
    ("yqks", 6), ("yqkr", 6), ("zqks", 6), ("zqkr", 9), ("fqks", 9), ("fqkr", 9),
    ("ysms", 1), ("ysmr", 1), ("zsms", 4), ("zsmr", 4), ("fsms", 3), ("fsmr", 3),
)
INPUTS = ("x", "gains", "shifts", "w_qkv", "qv_bias", "w_out", "biases", "w_up", "up_bias", "w_down", "lengths", "d_out")
IN_PLACE = ("x", "w_qkv", "w_out", "w_up", "w_down", "d_out")
OUTPUTS = (
    ("block_out", (256, D), BF),
    ("grad_inputs", (256, D), F32),
    ("fup", (3, D, 128), BF),
    ("fqk", (3, 96, D), BF),
    ("fdy", (4, 96, 384), BF),
    ("fdz", (4, 96, 384), BF),
    ("fou", (4, 96, 256), BF),
    ("fsum", (16, 128), F32),
)


class Refs:
    pass


def block_rows(block, size=BLOCK, offset=0):
    return pl.ds(pl.multiple_of(block * BLOCK + offset, 128), size)


def one_kernel(*args):
    r = Refs()
    names = [*INPUTS] + [o[0] for o in OUTPUTS] + [b[0] for b in BUFFERS] + [s[0] for s in SEMAPHORES]
    for name, ref in zip(names, args, strict=True):
        setattr(r, name, ref)
    dp, head = lax.axis_index("dp"), lax.axis_index("head")
    z, y = lax.div(dp, 2), lax.rem(dp, 2)
    px, pc = lax.div(head, 2), lax.rem(head, 2)

    def peer(code):
        return lax.rem(px + (code // 2 if isinstance(code, int) else lax.div(code, 2)), 2) * 2 + lax.rem(
            pc + (code % 2 if isinstance(code, int) else lax.rem(code, 2)), 2
        )

    sib, far, diag = peer(1), peer(2), peer(3)
    other_y = z * 2 + (1 - y)

    def z_shard(k):
        return lax.rem(z + k, 4)

    half = lax.div(z, 2)
    inner = (z == 1) | (z == 2)
    outer = (z == 0) | (z == 3)
    beside = half * 2 + 1 - lax.rem(z, 2)
    z_order = (3 * (1 - half), 2 - half, beside, z)

    sent = []

    def push(src, dst, send, recv, to):
        return pltpu.make_async_remote_copy(
            src_ref=src, dst_ref=dst, send_sem=send, recv_sem=recv, device_id=to, device_id_type=MESH
        )

    def when(cond, body):
        if cond is None:
            body()
        else:
            pl.when(cond)(body)

    def start(make, cond=None):
        when(cond, lambda: make().start())
        sent.append((make, cond))

    loads = {}

    def load(name, src, dst):
        loads.setdefault(name, []).append(pltpu.make_async_copy(src, dst, r.load.at[sum(map(len, loads.values()))]))

    load("x", r.x, r.xv)
    load("d", r.d_out, r.dv)
    load("wqkv", r.w_qkv, r.wqkv)
    load("wout", r.w_out, r.wout)
    load("wup", r.w_up, r.wup)
    load("wdown", r.w_down, r.big.at[:, 0:D])
    load("woo", r.w_out.at[pl.ds(pl.multiple_of(head * 192, 64), 192), :], r.woo.at[0:192, :])
    for j in range(6):
        unit = pl.ds(pl.multiple_of((4 * j + head) * 128, 128), 128)
        load("wuo", r.w_up.at[:, unit], r.wuo.at[:, j * 128 : (j + 1) * 128])
        load("wdo", r.w_down.at[unit, :], r.wdo.at[j * 128 : (j + 1) * 128, :])
    for copies in loads.values():
        for copy in copies:
            copy.start()

    def loaded(name):
        for copy in loads[name]:
            copy.wait()

    barrier = pltpu.get_barrier_semaphore()
    for to in [(dp, sib), (dp, far), (dp, diag), (other_y, head)] + [(z_shard(k) * 2 + y, head) for k in (1, 2, 3)]:
        pl.semaphore_signal(barrier, inc=1, device_id=to, device_id_type=MESH)

    gains = r.gains[...].astype(F32)
    shifts = r.shifts[...].astype(F32)
    biases = r.biases[...].astype(F32)
    onlane = lanes_of()
    lengths = r.lengths[...]
    whole = lengths[:, 0:1] == SLOT
    total = jnp.sum(lengths, axis=1, keepdims=True)

    def gather(buf, send, recv):
        def copy_of(index):
            if index == 0:
                rows, to = block_rows(head), sib
            elif index < 3:
                rows, to = block_rows(head, 128, (index - 1) * 128), far
            else:
                rows, to = block_rows(far, 128, (index - 3) * 128), sib
            return push(buf.at[rows, :], buf.at[rows, :], send.at[index], recv.at[index], (dp, to))

        def begin(these=(1, 2, 0)):
            for index in these:
                start(lambda index=index: copy_of(index))

        def wait(index):
            copy_of(index).wait_recv()

        def relay(these=(1, 2)):
            for index in these:
                wait(index)
                start(lambda index=index: copy_of(index + 2))

        def rest():
            for index in (3, 4):
                wait(index)

        return begin, wait, relay, rest

    n_begin, n_wait, n_relay, n_rest = gather(r.nall, r.ns, r.nr)
    d_begin, d_wait, d_relay, d_rest = gather(r.dall, r.ds, r.dr)
    s_begin, s_wait, s_relay, s_rest = gather(r.sall, r.ss, r.sr)
    l_begin, l_wait, l_relay, l_rest = gather(r.lall, r.ls, r.lr)

    loaded("x")
    first = norm_parts(r.xv[...].astype(F32), gains[0:1, :], shifts[0:1, :])[2]
    r.nall[block_rows(head), :] = first.astype(BF)
    pl.semaphore_wait(barrier, 7)
    n_begin()
    position = head * BLOCK + lax.broadcasted_iota(jnp.int32, (BLOCK, 1), 0)
    loaded("d")
    r.dall[block_rows(head), :] = (r.dv[...].astype(F32) * jnp.where(position < total, 1.0, 0.0)).astype(BF)
    d_begin((1, 0))
    loaded("wqkv")
    aligned = lax.div(3 * head, 2) * 128
    odd = jnp.where(lax.rem(head, 2) == 1, 1.0, 0.0)
    on_heads = jnp.where(onlane < 192, 1.0, 0.0)

    def own_window(values):
        moved = pltpu.roll(values, 192, 1)
        return (values * (1.0 - odd) + moved * odd) * on_heads

    r.vec[0:2, :] = r.qv_bias[...].astype(F32)
    pair_bias = own_window(r.vec[:, pl.ds(pl.multiple_of(aligned, 128), 256)])
    bias = jnp.concatenate([pair_bias[0:1], jnp.zeros((1, 256), F32), pair_bias[1:2]], axis=1)
    for part in range(3):
        window = pl.ds(pl.multiple_of(part * D + aligned, 128), 256)
        r.wqo[:, part * 256 : (part + 1) * 256] = own_window(r.wqkv[:, window].astype(F32)).astype(BF)

    aux_k = jnp.where((onlane >= 196) & (onlane < 199), 1.0, 0.0)
    aux_v = jnp.where((onlane >= 192) & (onlane < 199) & (onlane != 195), 1.0, 0.0)
    on_aux = jnp.where(onlane >= 192, 1.0, 0.0)

    def project(block):
        rows = block_rows(block)
        projected = (nn(r.nall[rows, :], r.wqo[...]) + bias).astype(BF).astype(F32)
        r.qb[rows, :] = (projected[:, :256] * 0.125 + lane_is(192 + block)).astype(BF)
        off = jnp.where((onlane >= 192) & (onlane < 196) & (onlane != 192 + block), 1.0, 0.0)
        r.kb[rows, :] = (projected[:, 256:512] + (aux_k + off * jnp.where(whole, 0.0, FAR))).astype(BF)
        r.vb[rows, :] = (projected[:, 512:] + aux_v).astype(BF)

    project(head)
    n_wait(0)
    project(sib)
    n_relay()
    project(far)
    n_rest()
    project(diag)

    def packed(values):
        third = values[:, 128:]
        return jnp.concatenate([values[:, :128], third[:128] + pltpu.roll(third[128:], 64, 1)], axis=0).astype(BF)

    def unpack(source, dst, base):
        for group in range(4):
            lane = group * 192
            dst[base : base + 256, lane : lane + 128] = source[group, 0:256, :]
            dst[base : base + 128, lane + 128 : lane + 192] = source[group, 256:384, 0:64]
            dst[base + 128 : base + 256, lane + 128 : lane + 192] = source[group, 256:384, 64:128]

    def mix_copy(code):
        return push(r.mixs.at[code], r.mixin.at[head], r.ms.at[code - 1], r.mr.at[code - 1], (dp, peer(code)))

    small_lane = lax.broadcasted_iota(jnp.int32, (1, 128), 1)

    def attend(step, carry):
        code = 3 - step
        block = peer(code)
        rows = block_rows(block)
        queries = r.qb[rows, :]
        mixed = jnp.zeros((BLOCK, 256), F32)
        tops = []
        for n in range(3):
            scores = nt(queries * (head_mask(n) + on_aux).astype(BF), r.kb[...])
            top = jnp.max(scores, axis=1, keepdims=True)
            weights = jnp.exp(scores - top).astype(BF)
            mixed += nn(weights, r.vb[...] * (head_mask(n) + lane_is(192 + n)).astype(BF))
            tops.append(top)
        lse = jnp.zeros((BLOCK, 128), F32)
        scale = jnp.zeros((BLOCK, 256), F32)
        for n in range(3):
            row_sum = jnp.sum(mixed * lane_is(192 + n), axis=1, keepdims=True)
            lse += (tops[n] + jnp.log(row_sum)) * jnp.where(small_lane == n, 1.0, 0.0)
            scale += (1.0 / row_sum) * head_mask(n)
        place = block * BLOCK + lax.broadcasted_iota(jnp.int32, (BLOCK, 1), 0)
        mixed = jnp.where(place < total, mixed * scale, r.vb[rows, :].astype(F32) * on_heads)
        r.exact[rows, :] = mixed
        r.lse[rows, :] = lse
        r.mix[rows, :] = mixed.astype(BF)
        r.mixs[code] = packed(mixed)

        @pl.when(step < 3)
        def _():
            mix_copy(code).start()

        return carry

    lax.fori_loop(0, 4, attend, 0)
    d_begin((2,))
    r.mixin[head] = r.mixs[0]
    d_relay((1,))

    loaded("wout")
    loaded("wup")
    loaded("wdown")
    for code in (3, 2, 1):
        mix_copy(code).wait_recv()
    unpack(r.mixin, r.wqo, 0)
    hidden = r.xv[...].astype(F32) + nn(r.wqo[0:256, :], r.wout[...]) + biases[0:1, :]
    unit, inverse, normed = norm_parts(hidden, gains[1:2, :], shifts[1:2, :])
    second = normed.astype(BF)
    r.sall[block_rows(head), :] = second
    s_begin()
    grad_low = r.dall[block_rows(head), :]
    down = jnp.zeros((BLOCK, D), F32)
    back = jnp.zeros((BLOCK, D), F32)
    for tile in range(4):
        cut = slice(tile * D, (tile + 1) * D)
        up = nn(second, r.wup[:, cut]) + r.up_bias[:, cut].astype(F32)
        value, slope = gelu_parts(up)
        w_down = r.big[cut, 0:D]
        down += nn(value.astype(BF), w_down)
        grad_up = nt(grad_low, w_down) * slope
        back += nt(grad_up.astype(BF), r.wup[:, cut])
    r.block_out[...] = (hidden + down + biases[1:2, :]).astype(BF)
    grad_block = grad_low.astype(F32)
    grad_hidden = grad_block + norm_back(back, unit, inverse, gains[1:2, :])
    r.gh[...] = grad_hidden
    r.lall[block_rows(head), :] = grad_hidden.astype(BF)
    l_begin()
    r.vec[...] = jnp.zeros_like(r.vec)
    r.vec[1:2, :] = jnp.sum(back * unit, axis=0, keepdims=True)
    r.vec[3:4, :] = jnp.sum(back, axis=0, keepdims=True)
    r.vec[6:7, :] = jnp.sum(grad_hidden, axis=0, keepdims=True)
    r.vec[7:8, :] = jnp.sum(grad_block, axis=0, keepdims=True)

    loaded("wuo")
    loaded("wdo")
    loaded("woo")
    own_bias = jnp.concatenate(
        [r.up_bias[:, pl.ds(pl.multiple_of((4 * j + head) * 128, 128), 128)] for j in range(6)], axis=1
    ).astype(F32)

    def feed(step, sums):
        @pl.when(step == 1)
        def _():
            d_wait(0)
            s_wait(0)

        @pl.when(step == 2)
        def _():
            d_relay((2,))
            s_relay()

        @pl.when(step == 3)
        def _():
            d_rest()
            s_rest()

        rows = block_rows(peer(step))
        up = nn(r.sall[rows, :], r.wuo[...]) + own_bias
        value, slope = gelu_parts(up)
        r.act[rows, :] = value.astype(BF)
        grad_up = nt(r.dall[rows, :], r.wdo[...]) * slope
        r.gup[rows, :] = grad_up.astype(BF)
        return sums + jnp.sum(grad_up, axis=0, keepdims=True)

    sums = lax.fori_loop(0, 4, feed, jnp.zeros((1, D), F32))
    def parts_of(name):
        refs = [getattr(r, part + name) for part in ("p", "y", "z", "f")]
        return refs + [getattr(r, part + name + end) for part in ("y", "z", "f") for end in ("s", "r")]

    def finals(fin, fs, fr):
        def f_copy(code):
            place = far if code == 3 else head
            to = far if code == 2 else sib
            return push(fin.at[place], fin.at[place], fs.at[code - 1], fr.at[code - 1], (dp, to))

        def begin():
            for code in (2, 1):
                start(lambda code=code: f_copy(code))

        def relay():
            f_copy(2).wait_recv()
            start(lambda: f_copy(3))

        def rest():
            f_copy(1).wait_recv()
            f_copy(3).wait_recv()

        return begin, relay, rest

    def add_to(ref, at, more):
        ref[at] = (ref[at].astype(F32) + more.astype(F32)).astype(BF)

    def y_first(name):
        own, ybuf, zbuf, fin, ys, yr, zs, zr, fs, fr = parts_of(name)
        f_begin, relay, rest = finals(fin, fs, fr)

        def y_copy(t):
            src = own.at[z_order[t] * 2 + (1 - y)]
            return push(src, ybuf.at[t], ys.at[t], yr.at[t], (other_y, head))

        def near_copy(t):
            return push(own.at[z_order[t] * 2 + y], zbuf.at[t], zs.at[t], zr.at[t], (beside * 2 + y, head))

        def across_copy(t):
            shard = z_order[t] * 2 + y
            return push(own.at[shard], zbuf.at[3], zs.at[t], zr.at[3], (shard, head))

        def begin():
            for t in range(4):
                start(lambda t=t: y_copy(t))

        def pair(t):
            y_copy(t).wait_recv()
            add_to(own, z_order[t] * 2 + y, ybuf[t])
            if t == 2:
                near_copy(t).start()
            elif t < 2:
                pl.when(outer)(lambda: near_copy(t).start())

        def fold(t):
            @pl.when(inner)
            def _():
                near_copy(t).wait_recv()
                add_to(own, z_order[t] * 2 + y, zbuf[t])
                across_copy(t).start()

        def total_up():
            near_copy(2).wait_recv()
            across_copy(0).wait_recv()
            fin[head] = (own[dp].astype(F32) + zbuf[2].astype(F32) + zbuf[3].astype(F32)).astype(BF)
            f_begin()
            sent.append((lambda: near_copy(2), None))
            for t in (0, 1):
                sent.append((lambda t=t: near_copy(t), outer))
                sent.append((lambda t=t: across_copy(t), inner))

        return begin, pair, fold, total_up, relay, rest

    def z_first(name):
        own, ybuf, zbuf, fin, ys, yr, zs, zr, fs, fr = parts_of(name)
        f_begin, relay, rest = finals(fin, fs, fr)

        def both(t):
            return pl.ds(z_order[t] * 2, 2)

        def near_copy(t):
            return push(own.at[both(t)], zbuf.at[t], zs.at[t], zr.at[t], (beside * 2 + y, head))

        def across_copy(t):
            return push(own.at[both(t)], zbuf.at[3], zs.at[t], zr.at[3], (z_order[t] * 2 + y, head))

        def y_copy():
            return push(own.at[z * 2 + (1 - y)], ybuf.at[0], ys.at[0], yr.at[0], (other_y, head))

        def begin():
            for t in (0, 1):
                start(lambda t=t: near_copy(t), outer)
            start(lambda: near_copy(2))

        def fold(t):
            @pl.when(inner)
            def _():
                near_copy(t).wait_recv()
                add_to(own, both(t), zbuf[t])
                across_copy(t).start()

        def pair():
            near_copy(2).wait_recv()
            across_copy(0).wait_recv()
            add_to(own, both(3), zbuf[2].astype(F32) + zbuf[3].astype(F32))
            y_copy().start()

        def total_up():
            y_copy().wait_recv()
            fin[head] = (own[dp].astype(F32) + ybuf[0].astype(F32)).astype(BF)
            f_begin()
            for t in (0, 1):
                sent.append((lambda t=t: across_copy(t), inner))
            sent.append((y_copy, None))

        return begin, fold, pair, total_up, relay, rest

    def direct(name):
        own, ybuf, zbuf, fin, ys, yr, zs, zr, fs, fr = parts_of(name)
        f_begin, relay, rest = finals(fin, fs, fr)

        def y_copy(k):
            src = own.at[z_shard(k) * 2 + (1 - y)]
            return push(src, ybuf.at[k], ys.at[k], yr.at[k], (other_y, head))

        def z_copy(k):
            shard = z_shard(k) * 2 + y
            return push(own.at[shard], zbuf.at[k], zs.at[k], zr.at[k], (shard, head))

        def begin():
            for k in (2, 1, 3, 0):
                start(lambda k=k: y_copy(k))

        def pair(k):
            y_copy(k).wait_recv()
            add_to(own, z_shard(k) * 2 + y, ybuf[k])
            if k:
                start(lambda: z_copy(k))

        def total_up():
            value = own[dp].astype(F32)
            for k in (1, 2, 3):
                z_copy(k).wait_recv()
                value += zbuf[k].astype(F32)
            fin[head] = value.astype(BF)
            f_begin()

        return begin, pair, total_up, relay, rest

    def irregular(name, number_of, owner_of, straight):
        own, ybuf, zbuf, fin, ys, yr, zs, zr, fs, fr = parts_of(name)

        def facts(j):
            number = number_of(j)
            shard = lax.div(number, 3)
            return shard, lax.div(shard, 2), lax.rem(shard, 2), lax.rem(number, 3)

        def y_copy(j):
            return push(own.at[j], ybuf.at[j], ys.at[j], yr.at[j], (other_y, head))

        def near_copy(j):
            slot = jnp.where(facts(j)[1] == beside, 6 + facts(j)[3], j)
            return push(own.at[j], zbuf.at[slot], zs.at[j], zr.at[slot], (beside * 2 + y, head))

        def near_arrival(j):
            return push(own.at[j], zbuf.at[j], zs.at[j], zr.at[j], (beside * 2 + y, head))

        def across_copy(j):
            shard, _, _, place = facts(j)
            return push(own.at[j], zbuf.at[9 + place], zs.at[j], zr.at[9 + place], (shard, head))

        def z_copy(j):
            shard, shard_z, _, place = facts(j)
            slot = (lax.rem(shard_z + 4 - z, 4) - 1) * 3 + place
            return push(own.at[j], zbuf.at[slot], zs.at[j], zr.at[slot], (shard, head))

        def last_arrival(j, base):
            place = base + facts(j)[3]
            return push(own.at[j], zbuf.at[place], zs.at[j], zr.at[place], (dp, sib)), place

        def f_copy(code, place):
            index = (code - 1) * 3 + place
            to = far if code == 2 else sib
            return push(fin.at[place], fin.at[place], fs.at[index], fr.at[index], (dp, to))

        def begin(these=range(6)):
            for j in these:
                start(lambda j=j: y_copy(j), facts(j)[2] != y)

        def mine(j):
            return facts(j)[2] == y

        def other_half(j):
            return lax.div(facts(j)[1], 2) != half

        def to_near(j):
            return mine(j) & ((facts(j)[1] == beside) | (other_half(j) & outer))

        def to_across(j):
            return mine(j) & other_half(j) & inner

        def fold(j):
            @pl.when(to_across(j))
            def _():
                near_arrival(j).wait_recv()
                add_to(own, j, zbuf[j])
                across_copy(j).start()

        def to_shard(j):
            return mine(j) & (facts(j)[1] != z)

        def pair(j):
            @pl.when(mine(j))
            def _():
                y_copy(j).wait_recv()
                add_to(own, j, ybuf[j])

            if straight:
                pl.when(to_shard(j))(lambda: z_copy(j).start())
            else:
                pl.when(to_near(j))(lambda: near_copy(j).start())

        def total_up():
            for j in range(6):
                if straight:
                    sent.append((lambda j=j: z_copy(j), to_shard(j)))
                else:
                    sent.append((lambda j=j: near_copy(j), to_near(j)))
                    sent.append((lambda j=j: across_copy(j), to_across(j)))
                shard, _, _, place = facts(j)

                def body(j=j, place=place):
                    value = own[j].astype(F32)
                    for base in (0, 3, 6) if straight else (6, 9):
                        copy, slot = last_arrival(j, base)
                        copy.wait_recv()
                        value += zbuf[slot].astype(F32)
                    fin[place] = value.astype(BF)
                    f_copy(2, place).start()
                    f_copy(1, place).start()

                pl.when(shard == dp)(body)

        def relay():
            for place in range(3):
                owner = owner_of(3 * dp + place)
                for code in (1, 2):
                    sent.append((lambda code=code, place=place: f_copy(code, place), owner == head))

                def body(place=place):
                    f_copy(2, place).wait_recv()
                    f_copy(3, place).start()

                pl.when(owner == far)(body)
                sent.append((lambda place=place: f_copy(3, place), owner == far))

        def rest():
            for place in range(3):
                owner = owner_of(3 * dp + place)
                for code, source in ((1, sib), (3, diag)):
                    pl.when(owner == source)(lambda code=code, place=place: f_copy(code, place).wait_recv())

        return begin, pair, fold, total_up, relay, rest

    dy_begin, dy_pair, dy_fold, dy_total, dy_relay, dy_rest = y_first("dy")
    dz_begin, dz_fold, dz_pair, dz_total, dz_relay, dz_rest = z_first("dz")
    ou_begin, ou_pair, ou_total, ou_relay, ou_rest = direct("ou")
    up_begin, up_pair, up_fold, up_total, up_relay, up_rest = irregular(
        "up", lambda j: 4 * j + head, lambda number: lax.rem(number, 4), False
    )
    qk_begin, qk_pair, _, qk_total, qk_relay, qk_rest = irregular(
        "qk",
        lambda j: (j // 2) * 8 + 2 * head + j % 2,
        lambda number: lax.div(lax.rem(number, 8), 2),
        True,
    )

    down_grad = tn(r.dall[...], r.act[...]).astype(BF)
    r.pdz[...] = down_grad[:, 384:].reshape(8, 96, 384)
    dz_begin()
    r.pdy[...] = down_grad[:, :384].reshape(8, 96, 384)
    dy_begin()
    up_grad = tn(r.sall[...], r.gup[...]).astype(BF)
    for j in range(6):
        r.pup[j] = up_grad[:, j * 128 : (j + 1) * 128]
    up_begin()

    r.small[...] = jnp.zeros_like(r.small)
    for j in range(6):
        number = 4 * j + head
        shard = lax.div(number, 3)
        r.small[lax.rem(shard, 2), lax.div(shard, 2), pl.ds(8 + lax.rem(number, 3), 1), :] = sums[
            :, j * 128 : (j + 1) * 128
        ]

    q_aug, g_aug = r.act, r.gup
    tile_lane = lanes_of(128)
    spot_row, spot_lane = (lax.broadcasted_iota(jnp.int32, (128, 128), axis) for axis in (0, 1))
    spots = [
        jnp.where((spot_lane == 68 + lax.div(spot_row, 3)) & (lax.rem(spot_row, 3) == n) & (spot_row < 9), 1.0, 0.0)
        for n in range(3)
    ]
    spots = [spot.astype(BF) for spot in spots]

    def aux_of(columns):
        high, middle, low = split_three(columns)
        return (high + pltpu.roll(middle, 3, 1) + pltpu.roll(low, 6, 1)).astype(BF)

    def write_aug(dst, rows, source, aux, keep):
        left = source[:, :128]
        right = source[:, 128:].astype(F32)
        for n in range(3):
            if n < 2:
                part = left * jnp.where(lax.div(tile_lane, 64) == n, 1.0, 0.0).astype(BF)
            else:
                part = jnp.zeros((256, 128), BF)
            dst[rows, n * 256 : n * 256 + 128] = part
            mask = jnp.where(tile_lane < 64, 1.0 if n == 2 else 0.0, keep)
            dst[rows, n * 256 + 128 : (n + 1) * 256] = (right * mask + nn(aux, spots[n])).astype(BF)

    def augment_q(block, carry):
        rows = pl.ds(pl.multiple_of(block * 256, 256), 256)
        write_aug(q_aug, rows, r.qb[rows, :], aux_of(-r.lse[rows, :]), 1.0)
        return carry

    lax.fori_loop(0, 4, augment_q, 0)
    sum_row, sum_lane = (lax.broadcasted_iota(jnp.int32, (256, 128), axis) for axis in (0, 1))
    head_sums = jnp.where((lax.div(sum_row, 64) == sum_lane) & (sum_row < 192), 1.0, 0.0).astype(BF)
    r.woo[192:256, :] = jnp.zeros((64, D), BF)
    dy_pair(0)
    dy_pair(1)
    dz_fold(0)
    l_wait(0)
    l_relay()
    l_rest()
    r.gm[...] = nt(r.lall[...], r.woo[...]).astype(BF)

    def augment_g(block, carry):
        rows = pl.ds(pl.multiple_of(block * 256, 256), 256)
        grads = r.gm[rows, :]
        product = grads.astype(F32) * r.exact[rows, :]
        inner = jnp.zeros((256, 128), F32)
        for part in split_three(product):
            inner += nn(part.astype(BF), head_sums)
        write_aug(g_aug, rows, grads, aux_of(-inner), 0.0)
        return carry

    lax.fori_loop(0, 4, augment_g, 0)
    dy_pair(2)
    dy_pair(3)
    dz_fold(1)

    def kv_copy(code):
        rows = block_rows(peer(code))
        return push(r.dkv.at[rows, :], r.kvin.at[head], r.kvs.at[code - 1], r.kvr.at[code - 1], (dp, peer(code)))

    def q_copy(code):
        return push(r.qs_.at[code], r.qin.at[head], r.qs.at[code - 1], r.qr.at[code - 1], (dp, peer(code)))

    def attend_back(step, carry):
        code = 3 - step
        block = peer(code)
        rows = block_rows(block)
        key_grad = jnp.zeros((BLOCK, 256), F32)
        value_grad = jnp.zeros((BLOCK, 256), F32)
        for n in range(3):
            mask = head_mask(n)
            lanes = slice(n * 256, (n + 1) * 256)
            probs = jnp.exp(nt(r.kb[rows, :], q_aug[:, lanes]))
            grad_scores = (probs * nt(r.vb[rows, :], g_aug[:, lanes])).astype(BF)
            r.big[pl.ds(pl.multiple_of(n * SLOT + block * BLOCK, 256), BLOCK), :] = grad_scores
            key_grad += nn(grad_scores, q_aug[:, lanes]) * mask
            value_grad += nn(probs.astype(BF), g_aug[:, lanes]) * mask
        r.dkv[rows, 0:192] = key_grad[:, :192].astype(BF)
        r.dkv[rows, 192:384] = value_grad[:, :192].astype(BF)

        @pl.when(step < 3)
        def _():
            kv_copy(code).start()

        @pl.when(step == 1)
        def _():
            dz_pair()
            up_pair(0)
            up_pair(1)

        @pl.when(step == 2)
        def _():
            dy_fold(0)
            up_pair(2)

        @pl.when(step == 3)
        def _():
            dy_fold(1)
            up_pair(3)

        return carry

    lax.fori_loop(0, 4, attend_back, 0)
    r.kvin[head] = r.dkv[block_rows(head), :]
    r.pqk[2:6] = tn(r.dkv[...], r.nall[...]).astype(BF).reshape(4, 96, D)
    qk_begin(range(2, 6))

    def query_back(step, carry):
        code = 3 - step
        block = peer(code)
        rows = block_rows(block)
        query_grad = jnp.zeros((BLOCK, 256), F32)
        for n in range(3):
            part = r.big[n * SLOT : (n + 1) * SLOT, pl.ds(pl.multiple_of(block * BLOCK, 256), BLOCK)]
            query_grad += tn(part, r.kb[...] * head_mask(n).astype(BF))
        query_grad = query_grad * 0.125
        r.dq[rows, :] = query_grad.astype(BF)
        r.qs_[code] = packed(query_grad)

        @pl.when(step < 3)
        def _():
            q_copy(code).start()

        return carry

    lax.fori_loop(0, 4, query_back, 0)
    r.qin[head] = r.qs_[0]
    r.pqk[0:2] = tn(r.dq[...], r.nall[...])[:192].astype(BF).reshape(2, 96, D)
    qk_begin(range(2))
    for j in (4, 5):
        up_pair(j)
    r.pou[...] = tn(r.lall[...], r.mix[...]).astype(BF).reshape(8, 96, 256)
    ou_begin()
    up_fold(0)
    up_fold(1)
    dy_total()
    query_sum = jnp.sum(r.dq[...].astype(F32), axis=0, keepdims=True)
    value_sum = jnp.sum(r.dkv[:, 128:384].astype(F32), axis=0, keepdims=True)
    for group in range(4):
        mine = jnp.where(head == group, 1.0, 0.0)
        r.vec[4:5, group * 192 : (group + 1) * 192] = query_sum[:, :192] * mine
        r.vec[5:6, group * 192 : (group + 1) * 192] = value_sum[:, 64:] * mine
    dz_total()
    up_fold(2)
    qk_pair(2)

    for code in (3, 2, 1):
        kv_copy(code).wait_recv()
        q_copy(code).wait_recv()
    unpack(r.qin, r.wuo, 0)
    for group in range(4):
        lanes = slice(group * 192, (group + 1) * 192)
        r.wuo[256:512, lanes] = r.kvin[group][:, :192]
        r.wuo[512:768, lanes] = r.kvin[group][:, 192:]
    grad_first = nt(r.wuo[0:256, :], r.wqkv[:, 0:D])
    grad_first += nt(r.wuo[256:512, :], r.wqkv[:, D : 2 * D])
    grad_first += nt(r.wuo[512:768, :], r.wqkv[:, 2 * D :])
    unit, inverse, _ = norm_parts(r.xv[...].astype(F32), gains[0:1, :], shifts[0:1, :])
    r.grad_inputs[...] = r.gh[...] + norm_back(grad_first, unit, inverse, gains[0:1, :])
    r.vec[0:1, :] = jnp.sum(grad_first * unit, axis=0, keepdims=True)
    r.vec[2:3, :] = jnp.sum(grad_first, axis=0, keepdims=True)
    for shard in range(8):
        r.small[shard % 2, shard // 2, 0:8, 0:96] = r.vec[:, shard * 96 : (shard + 1) * 96]

    def small_y():
        return push(r.small.at[1 - y], r.ysm, r.ysms.at[0], r.ysmr.at[0], (other_y, head))

    def small_z(k):
        return push(
            r.small.at[y, z_shard(k)], r.zsm.at[k], r.zsms.at[k], r.zsmr.at[k], (z_shard(k) * 2 + y, head)
        )

    def small_f(code):
        return push(r.fsm.at[head], r.fsm.at[head], r.fsms.at[code - 1], r.fsmr.at[code - 1], (dp, peer(code)))

    start(small_y)
    up_fold(3)
    qk_pair(3)
    up_fold(4)
    up_fold(5)
    for j in (4, 5):
        qk_pair(j)
    qk_pair(0)
    qk_pair(1)
    for k in (2, 1, 3, 0):
        ou_pair(k)
    dy_relay()
    dz_relay()
    up_total()
    small_y().wait_recv()
    r.small[y] = r.small[y] + r.ysm[...]
    for k in (1, 2, 3):
        start(lambda k=k: small_z(k))
    qk_total()
    ou_total()
    up_relay()
    for k in (1, 2, 3):
        small_z(k).wait_recv()
    r.fsm[head] = r.small[y, z] + r.zsm[1] + r.zsm[2] + r.zsm[3]
    for code in (2, 3, 1):
        start(lambda code=code: small_f(code))
    qk_relay()
    ou_relay()
    dy_rest()
    dz_rest()
    up_rest()
    qk_rest()
    ou_rest()
    for code in (2, 3, 1):
        small_f(code).wait_recv()
    r.fsum[...] = r.fsm[0] + r.fsm[1] + r.fsm[2] + r.fsm[3]
    for make, cond in sent:
        when(cond, lambda make=make: make().wait_send())
    for code in (1, 2, 3):
        mix_copy(code).wait_send()
        kv_copy(code).wait_send()
        q_copy(code).wait_send()


def emit_kernel(
    block_in, inputs_in, fup, fqk, fdy, fdz, fou, fsum,
    block_out, grad_inputs, gains, shifts, qkv, qv_bias, out, out_biases, up, up_bias, down,
    block_v, inputs_v, fup_v, fqk_v, fdy_v, fdz_v, fou_v, fsum_v, up_v, qkv_v, down_v, out_v, sems,
):
    count = []

    def begin(src, dst):
        count.append(pltpu.make_async_copy(src, dst, sems.at[len(count)]))
        count[-1].start()
        return count[-1]

    pairs = (
        (fdy, fdy_v), (fdz, fdz_v), (fup, fup_v), (inputs_in, inputs_v), (block_in, block_v), (fqk, fqk_v), (fou, fou_v),
        (fsum, fsum_v),
    )
    arrivals = [begin(src, dst) for src, dst in pairs]
    results = []
    arrivals[0].wait()
    arrivals[1].wait()
    for group in range(4):
        for j in range(6):
            place = (4 * j + group) * 128
            source, at = (fdy_v, j * 128) if j < 3 else (fdz_v, j * 128 - 384)
            down_v[:, place : place + 128] = source[group, :, at : at + 128].astype(F32)
    results.append(begin(down_v, down))
    arrivals[2].wait()
    for i in range(3):
        up_v[:, i * 128 : (i + 1) * 128] = fup_v[i].astype(F32)
    results.append(begin(up_v, up))
    for arrival, src, dst in ((3, inputs_v, grad_inputs), (4, block_v, block_out)):
        arrivals[arrival].wait()
        results.append(begin(src, dst))
    arrivals[5].wait()
    qkv_v[...] = fqk_v[...].reshape(288, D).astype(F32)
    results.append(begin(qkv_v, qkv))
    arrivals[6].wait()
    for group in range(4):
        out_v[:, group * 192 : (group + 1) * 192] = fou_v[group][:, :192].astype(F32)
    results.append(begin(out_v, out))
    arrivals[7].wait()
    for index, ref in enumerate((gains, shifts, qv_bias, out_biases)):
        ref[...] = fsum_v[2 * index : 2 * index + 2, 0:96]
    up_bias[...] = fsum_v[8:11, :]
    for copy in results:
        copy.wait()


def per_device(x, norm_gains, norm_shifts, w_qkv, qv_bias, w_out, out_biases, w_up, up_bias, w_down, lengths, d_out):
    values = dict(
        x=x[0], gains=norm_gains, shifts=norm_shifts, w_qkv=w_qkv, qv_bias=qv_bias, w_out=w_out, biases=out_biases,
        w_up=w_up, up_bias=up_bias.reshape(1, FF), w_down=w_down, lengths=lengths, d_out=d_out[0],
    )
    place = {True: pl.BlockSpec(memory_space=pl.ANY), False: pl.BlockSpec(memory_space=pltpu.VMEM)}
    block_out, grad_inputs, fup, fqk, fdy, fdz, fou, fsum = pl.pallas_call(
        one_kernel,
        out_shape=[jax.ShapeDtypeStruct(shape, kind) for _, shape, kind in OUTPUTS],
        in_specs=[place[name in IN_PLACE] for name in INPUTS],
        out_specs=[place[False]] * len(OUTPUTS),
        scratch_shapes=[pltpu.VMEM(shape, kind) for _, shape, kind in BUFFERS]
        + [pltpu.SemaphoreType.DMA((count,)) for _, count in SEMAPHORES],
        compiler_params=pltpu.CompilerParams(
            collective_id=0, has_side_effects=True, vmem_limit_bytes=VMEM_LIMIT
        ),
        name="block",
    )(*(values[name] for name in INPUTS))
    anywhere = pl.BlockSpec(memory_space=pl.ANY)
    shapes = [(256, D), (256, D), (2, 96), (2, 96), (288, D), (2, 96), (96, D), (2, 96), (D, 384), (3, 128), (96, FF)]
    outs = pl.pallas_call(
        emit_kernel,
        out_shape=[jax.ShapeDtypeStruct(shape, F32 if n else BF) for n, shape in enumerate(shapes)],
        in_specs=[anywhere] * 8,
        out_specs=[anywhere] * 2 + [anywhere if shape[0] > 16 else place[False] for shape in shapes[2:]],
        scratch_shapes=[pltpu.VMEM(shape, kind) for _, shape, kind in OUTPUTS]
        + [pltpu.VMEM(shape, F32) for shape in ((D, 384), (288, D), (96, FF), (96, D))]
        + [pltpu.SemaphoreType.DMA((14,))],
        compiler_params=pltpu.CompilerParams(vmem_limit_bytes=VMEM_LIMIT),
        name="emit",
    )(block_out, grad_inputs, fup, fqk, fdy, fdz, fou, fsum)
    return (
        outs[0][None], outs[1][None], outs[2], outs[3], outs[4].T, outs[5], outs[6].T, outs[7], outs[8],
        outs[9].reshape(384), outs[10].T,
    )


def solution(mesh):
    split = P("dp", "head", None)
    placed = (split,) + (P(),) * 9 + (P("dp", None), split)
    return jax.shard_map(
        per_device if dict(mesh.shape) == {"dp": 8, "head": 4} else general_device,
        mesh=mesh,
        in_specs=placed,
        out_specs=(split, split) + (P(None, "dp"),) * 7 + (P("dp"), P(None, "dp")),
        check_vma=False,
    )
```

```python
import functools

import jax
import jax.numpy as jnp
from jax import lax
from jax.experimental import pallas as pl
from jax.experimental.pallas import tpu as pltpu
from jax.sharding import PartitionSpec as P

D = 768
HEADS = 12
HDIM = 64
FF = 3072
SLOT = 1024
EPSILON = 1e-06
BF = jnp.bfloat16
F32 = jnp.float32
FAR = -1e30
VMEM_LIMIT = 63 * 1024 * 1024


def nn(a, b):
    return lax.dot_general(a, b, (((1,), (0,)), ((), ())), preferred_element_type=F32)


def nt(a, b):
    return lax.dot_general(a, b, (((1,), (1,)), ((), ())), preferred_element_type=F32)


def tn(a, b):
    return lax.dot_general(a, b, (((0,), (0,)), ((), ())), preferred_element_type=F32)


def norm_parts(values, norm_gain, norm_shift):
    average = jnp.mean(values, axis=-1, keepdims=True)
    centered = values - average
    variance = jnp.mean(centered * centered, axis=-1, keepdims=True)
    inverse = lax.rsqrt(variance + EPSILON)
    unit = centered * inverse
    return unit, inverse, unit * norm_gain + norm_shift


def norm_back(grad_normed, unit, inverse, norm_gain):
    grad_unit = grad_normed * norm_gain
    first_mean = jnp.mean(grad_unit, axis=-1, keepdims=True)
    second_mean = jnp.mean(grad_unit * unit, axis=-1, keepdims=True)
    return inverse * (grad_unit - first_mean - unit * second_mean)


def gelu_parts(values):
    cumulative = 0.5 + 0.5 * lax.erf(values * 0.7071067811865476)
    density = jnp.exp(values * values * -0.5) * 0.3989422804014327
    return values * cumulative, cumulative + values * density


def lanes_of(width=256):
    return lax.broadcasted_iota(jnp.int32, (1, width), 1)


def head_mask(head):
    lane = lanes_of()
    return jnp.where((lane >= head * HDIM) & (lane < (head + 1) * HDIM), 1.0, 0.0)


def lane_is(index):
    return jnp.where(lanes_of() == index, 1.0, 0.0)


def split_three(column):
    high = column.astype(BF).astype(F32)
    rest = column - high
    middle = rest.astype(BF).astype(F32)
    return high, middle, rest - middle


def attend_forward(normed, weight, bias, lengths, q_ref, k_ref, v_ref, mixed_ref, exact_ref, lse_ref):
    whole = lengths[:, 0:1] == SLOT
    total = jnp.sum(lengths, axis=1, keepdims=True)
    onlane = lanes_of()
    aux_k = jnp.where((onlane >= 196) & (onlane < 199), 1.0, 0.0)
    aux_v = jnp.where((onlane >= 192) & (onlane < 199) & (onlane != 195), 1.0, 0.0)
    for block in range(4):
        rows = pl.ds(block * 256, 256)
        projected = nn(normed[rows, :], weight[...]) + bias
        projected = projected.astype(BF).astype(F32)
        q_ref[rows, :] = (projected[:, :256] * 0.125 + lane_is(192 + block)).astype(BF)
        other = jnp.where((onlane >= 192) & (onlane < 196) & (onlane != 192 + block), 1.0, 0.0)
        far = other * jnp.where(whole, 0.0, FAR)
        k_ref[rows, :] = (projected[:, 256:512] + (aux_k + far)).astype(BF)
        v_ref[rows, :] = (projected[:, 512:] + aux_v).astype(BF)
    on_aux = jnp.where(onlane >= 192, 1.0, 0.0)

    def block_step(block, carry):
        rows = pl.ds(pl.multiple_of(block * 256, 256), 256)
        queries = q_ref[rows, :]
        mixed = jnp.zeros((256, 256), F32)
        tops = []
        for head in range(3):
            scores = nt(queries * (head_mask(head) + on_aux).astype(BF), k_ref[...])
            top = jnp.max(scores, axis=1, keepdims=True)
            weights = jnp.exp(scores - top).astype(BF)
            mixed += nn(weights, v_ref[...] * (head_mask(head) + lane_is(192 + head)).astype(BF))
            tops.append(top)
        lse = jnp.zeros((256, 128), F32)
        scale = jnp.zeros((256, 256), F32)
        small = lax.broadcasted_iota(jnp.int32, (1, 128), 1)
        for head in range(3):
            row_sum = jnp.sum(mixed * lane_is(192 + head), axis=1, keepdims=True)
            lse += (tops[head] + jnp.log(row_sum)) * jnp.where(small == head, 1.0, 0.0)
            scale += (1.0 / row_sum) * head_mask(head)
        mixed = mixed * scale
        position = block * 256 + lax.broadcasted_iota(jnp.int32, (256, 1), 0)
        on_heads = jnp.where(onlane < 192, 1.0, 0.0)
        mixed = jnp.where(position < total, mixed, v_ref[rows, :].astype(F32) * on_heads)
        exact_ref[rows, :] = mixed
        mixed_ref[rows, :] = mixed[:, :192].astype(BF)
        lse_ref[rows, :] = lse
        return carry

    lax.fori_loop(0, 4, block_step, 0)


def attend_backward(q_ref, k_ref, v_ref, exact_ref, lse_ref, grad_mixed, q_aug, g_aug, scores_low, dq_acc, dk_acc, dv_acc):
    for head in range(3):
        mask = head_mask(head)

        def augment(block, carry):
            rows = pl.ds(pl.multiple_of(block * 256, 256), 256)
            grads = grad_mixed[rows, :].astype(F32) * mask
            inner = jnp.sum(grads * exact_ref[rows, :], axis=1, keepdims=True)
            lse = lse_ref[rows, :][:, head : head + 1]
            queries = q_ref[rows, :].astype(F32) * (mask + jnp.where(lanes_of() >= 192, 1.0, 0.0))
            for place, part in enumerate(split_three(-lse)):
                queries = queries + part * lane_is(196 + place)
            for place, part in enumerate(split_three(-inner)):
                grads = grads + part * lane_is(196 + place)
            q_aug[rows, :] = queries.astype(BF)
            g_aug[rows, :] = grads.astype(BF)
            return carry

        lax.fori_loop(0, 4, augment, 0)

        def block_step(block, carry):
            rows = pl.ds(pl.multiple_of(block * 256, 256), 256)
            probs = jnp.exp(nt(k_ref[rows, :], q_aug[...]))
            grad_probs = nt(v_ref[rows, :], g_aug[...])
            grad_scores = (probs * grad_probs).astype(BF)
            scores_low[rows, :] = grad_scores
            key_part = nn(grad_scores, q_aug[...]) * mask
            value_part = nn(probs.astype(BF), g_aug[...]) * mask
            if head == 0:
                dk_acc[rows, :] = key_part
                dv_acc[rows, :] = value_part
            else:
                dk_acc[rows, :] += key_part
                dv_acc[rows, :] += value_part
            return carry

        lax.fori_loop(0, 4, block_step, 0)
        query_part = tn(scores_low[...], k_ref[...] * mask.astype(BF)) * 0.125
        if head == 0:
            dq_acc[...] = query_part
        else:
            dq_acc[...] += query_part


def forward_kernel(normed, weight, bias, lengths, q_ref, k_ref, v_ref, mixed_ref, exact_ref, lse_ref):
    attend_forward(normed, weight, bias[...], lengths[...], q_ref, k_ref, v_ref, mixed_ref, exact_ref, lse_ref)


def middle_kernel(
    mixed_in, x_in, d_low, w_out, w_up, w_down, gains, shifts, biases, up_bias,
    block_ref, second_ref, hid_ref, low_ref, sums_ref, mixed_rows, act_ref,
):
    rows = x_in.shape[0]
    for group in range(4):
        mixed_rows[:, group * 192 : (group + 1) * 192] = mixed_in[group]
    hidden = x_in[...].astype(F32) + nn(mixed_rows[...], w_out[...]) + biases[0:1, :]
    unit, inverse, normed = norm_parts(hidden, gains[1:2, :], shifts[1:2, :])
    second = normed.astype(BF)
    second_ref[...] = second
    grad_low = d_low[...]
    down = jnp.zeros((rows, D), F32)
    back = jnp.zeros((rows, D), F32)
    step = 768
    for tile in range(FF // step):
        cut = slice(tile * step, (tile + 1) * step)
        up = nn(second, w_up[:, cut]) + up_bias[:, cut]
        value, slope = gelu_parts(up)
        down += nn(value.astype(BF), w_down[cut, :])
        grad_up = nt(grad_low, w_down[cut, :]) * slope
        back += nt(grad_up.astype(BF), w_up[:, cut])
    block_ref[...] = (hidden + down + biases[1:2, :]).astype(BF)
    grad_block = grad_low.astype(F32)
    grad_hidden = grad_block + norm_back(back, unit, inverse, gains[1:2, :])
    hid_ref[...] = grad_hidden
    low_ref[...] = grad_hidden.astype(BF)
    sums_ref[...] = jnp.zeros_like(sums_ref)
    sums_ref[0:1, :] = jnp.sum(back * unit, axis=0, keepdims=True)
    sums_ref[1:2, :] = jnp.sum(back, axis=0, keepdims=True)
    sums_ref[2:3, :] = jnp.sum(grad_hidden, axis=0, keepdims=True)
    sums_ref[3:4, :] = jnp.sum(grad_block, axis=0, keepdims=True)


def feed_kernel(second, d_low, w_up, w_down, up_bias, up_grad, down_grad, bias_grad, act_ref, grad_ref):
    width = w_up.shape[1]
    bias_grad[...] = jnp.zeros_like(bias_grad)

    def step(block, carry):
        rows = pl.ds(pl.multiple_of(block * 256, 256), 256)
        up = nn(second[rows, :], w_up[...]) + up_bias[...]
        value, slope = gelu_parts(up)
        act_ref[rows, :] = value.astype(BF)
        grad_up = nt(d_low[rows, :], w_down[...]) * slope
        bias_grad[0:1, :] += jnp.sum(grad_up, axis=0, keepdims=True)
        grad_ref[rows, :] = grad_up.astype(BF)
        return carry

    lax.fori_loop(0, 4, step, 0)
    down_grad[...] = tn(d_low[...], act_ref[...]).astype(BF)
    up_grad[...] = tn(grad_ref[...], second[...]).astype(BF)


def backward_kernel(
    grad_low, w_out, normed, mixed, q_ref, k_ref, v_ref, exact_ref, lse_ref,
    grad_ref, out_grad, qkv_grad, bias_grad,
    grad_mixed, q_aug, g_aug, scores_low, dq_acc, dk_acc, dv_acc,
):
    padded = jnp.zeros((64, D), BF)
    weight = jnp.concatenate([w_out[...], padded], axis=0)
    grad_mixed[...] = nt(grad_low[...], weight).astype(BF)
    out_grad[...] = tn(grad_low[...], mixed[...]).astype(BF)
    attend_backward(q_ref, k_ref, v_ref, exact_ref, lse_ref, grad_mixed, q_aug, g_aug, scores_low, dq_acc, dk_acc, dv_acc)
    for place, part in enumerate((dq_acc, dk_acc, dv_acc)):
        grad_ref[:, place * 192 : (place + 1) * 192] = part[:, :192].astype(BF)
    bias_grad[...] = jnp.zeros_like(bias_grad)
    bias_grad[0:1, :] = jnp.sum(grad_ref[...].astype(F32), axis=0, keepdims=True)
    qkv_grad[...] = tn(grad_ref[...], normed[...]).astype(BF)


def last_kernel(grad_in, w_qkv, x_in, hid, gains, shifts, out_ref, sums_ref, grad_rows):
    for part in range(3):
        for group in range(4):
            place = part * D + group * 192
            grad_rows[:, place : place + 192] = grad_in[group][:, part * 192 : (part + 1) * 192]
    grad_first = nt(grad_rows[...], w_qkv[...])
    unit, inverse, _ = norm_parts(x_in[...].astype(F32), gains[0:1, :], shifts[0:1, :])
    out_ref[...] = hid[...] + norm_back(grad_first, unit, inverse, gains[0:1, :])
    sums_ref[...] = jnp.zeros_like(sums_ref)
    sums_ref[0:1, :] = jnp.sum(grad_first * unit, axis=0, keepdims=True)
    sums_ref[1:2, :] = jnp.sum(grad_first, axis=0, keepdims=True)


def whole_call(kernel, outs, scratch=(), name=None):
    return pl.pallas_call(
        kernel,
        out_shape=[jax.ShapeDtypeStruct(*out) for out in outs],
        scratch_shapes=[pltpu.VMEM(*item) for item in scratch],
        compiler_params=pltpu.CompilerParams(vmem_limit_bytes=VMEM_LIMIT),
        name=name,
    )


def general_device(x, norm_gains, norm_shifts, w_qkv, qv_bias, w_out, out_biases, w_up, up_bias, w_down, lengths, d_out):
    groups = lax.axis_size("head")
    shards = lax.axis_size("dp")
    group = lax.axis_index("head")
    rows = x.shape[1]
    own = D // groups
    x = x[0]
    gains = norm_gains.astype(F32)
    shifts = norm_shifts.astype(F32)
    biases = out_biases.astype(F32)
    up_shift = up_bias.astype(F32)
    full_bias = jnp.stack([qv_bias[0], jnp.zeros_like(qv_bias[0]), qv_bias[1]]).astype(F32)

    weight_own = lax.dynamic_index_in_dim(w_qkv.reshape(D, 3, groups, own), group, 2, False)
    weight_own = jnp.pad(weight_own, ((0, 0), (0, 0), (0, 256 - own))).reshape(D, 768)
    bias_own = lax.dynamic_index_in_dim(full_bias.reshape(3, groups, own), group, 1, False)
    bias_own = jnp.pad(bias_own, ((0, 0), (0, 256 - own))).reshape(1, 768)
    out_own = lax.dynamic_slice_in_dim(w_out, group * own, own, 0)
    unit_ff = FF // (shards * groups)
    up_own = lax.dynamic_index_in_dim(w_up.reshape(D, shards, groups, unit_ff), group, 2, False).reshape(D, D)
    down_own = lax.dynamic_index_in_dim(w_down.reshape(shards, groups, unit_ff, D), group, 1, False).reshape(D, D)
    ub_own = lax.dynamic_index_in_dim(up_shift.reshape(shards, groups, unit_ff), group, 1, False).reshape(1, D)

    normed = norm_parts(x.astype(F32), gains[0], shifts[0])[2].astype(BF)
    normed_all = lax.all_gather(normed, "head", axis=0, tiled=True)
    total = jnp.sum(lengths[0])
    position = group * rows + jnp.arange(rows, dtype=jnp.int32)
    d_low = jnp.where((position < total)[:, None], d_out[0], jnp.zeros_like(d_out[0]))
    d_all = lax.all_gather(d_low, "head", axis=0, tiled=True)

    q, k, v, mixed, exact, lse = whole_call(
        forward_kernel,
        [((SLOT, 256), BF)] * 3 + [((SLOT, own), BF), ((SLOT, 256), F32), ((SLOT, 128), F32)],
        name="attend_forward",
    )(normed_all, weight_own, bias_own, lengths)
    mixed_in = lax.all_to_all(mixed.reshape(groups, rows, own), "head", 0, 0, tiled=True)
    block_out, second, hid, hid_low, sums_mid = whole_call(
        middle_kernel,
        [((rows, D), BF), ((rows, D), BF), ((rows, D), F32), ((rows, D), BF), ((8, D), F32)],
        [((rows, D), BF), ((rows, FF), BF)],
        name="middle",
    )(mixed_in, x, d_low, w_out, w_up, w_down, gains, shifts, biases, up_shift.reshape(1, FF))
    second_all = lax.all_gather(second, "head", axis=0, tiled=True)
    low_all = lax.all_gather(hid_low, "head", axis=0, tiled=True)
    up_grad, down_grad, ub_grad = whole_call(
        feed_kernel,
        [((D, D), BF), ((D, D), BF), ((8, D), F32)],
        [((SLOT, D), BF), ((SLOT, D), BF)],
        name="feed",
    )(second_all, d_all, up_own, down_own, ub_own)
    grad_own, out_grad, qkv_grad, qkv_sum = whole_call(
        backward_kernel,
        [((SLOT, 3 * own), BF), ((D, own), BF), ((3 * own, D), BF), ((8, 3 * own), F32)],
        [((SLOT, 256), BF)] * 3 + [((SLOT, SLOT), BF)] + [((SLOT, 256), F32)] * 3,
        name="attend_backward",
    )(low_all, out_own, normed_all, mixed, q, k, v, exact, lse)
    grad_in = lax.all_to_all(grad_own.reshape(groups, rows, 3 * own), "head", 0, 0, tiled=True)
    grad_inputs, sums_last = whole_call(
        last_kernel,
        [((rows, D), F32), ((8, D), F32)],
        [((rows, 3 * D), BF)],
        name="last",
    )(grad_in, w_qkv, x, hid, gains, shifts)

    def scatter(values):
        return lax.psum_scatter(values, "dp", scatter_dimension=0, tiled=True)

    up_part = lax.all_gather(scatter(up_grad), "head", axis=0, tiled=True)
    down_part = lax.all_gather(scatter(down_grad), "head", axis=1, tiled=True)
    out_part = lax.all_gather(scatter(out_grad), "head", axis=1, tiled=True)
    down_out = down_part.astype(F32).T.reshape(groups, shards, unit_ff, D // shards)
    down_out = down_out.transpose(1, 0, 2, 3).reshape(FF, D // shards)
    spread = jnp.zeros((3, groups, own, D), BF)
    spread = lax.dynamic_update_slice(spread, qkv_grad.reshape(3, 1, own, D), (0, group, 0, 0))
    qkv_part = lax.psum(scatter(spread.reshape(3 * D, D)), "head")

    def place_rows(values):
        parts = values.reshape(3, own)
        empty = jnp.zeros((3, groups, own), F32)
        return lax.dynamic_update_slice(empty, parts[:, None], (0, group, 0)).reshape(3, D)

    bias_rows = place_rows(qkv_sum[0])
    ub_rows = lax.dynamic_update_slice(
        jnp.zeros((shards, groups, unit_ff), F32), ub_grad[0].reshape(shards, 1, unit_ff), (0, group, 0)
    ).reshape(4, D)
    small = jnp.concatenate([sums_last[0:2], sums_mid[0:4], bias_rows[0:1], bias_rows[2:3], ub_rows], axis=0)
    small = lax.psum(small, ("dp", "head"))
    shard = lax.axis_index("dp")

    def cut(values):
        width = D // shards
        return lax.dynamic_slice_in_dim(values, shard * width, width, 1)

    ub_out = lax.dynamic_slice_in_dim(small[8:12].reshape(FF), shard * (FF // shards), FF // shards, 0)
    return (
        block_out[None],
        grad_inputs[None],
        cut(jnp.stack([small[0], small[2]])),
        cut(jnp.stack([small[1], small[3]])),
        qkv_part.astype(F32).T,
        cut(small[6:8]),
        out_part.astype(F32).T,
        cut(small[4:6]),
        up_part.astype(F32).T,
        ub_out,
        down_out,
    )


MESH = pl.DeviceIdType.MESH
BLOCK = 256

BUFFERS = (
    ("xv", (256, D), BF),
    ("dv", (256, D), BF),
    ("wqkv", (D, 3 * D), BF),
    ("wout", (D, D), BF),
    ("wup", (D, FF), BF),
    ("big", (3 * SLOT, SLOT), BF),
    ("wqo", (D, D), BF),
    ("wuo", (D, D), BF),
    ("wdo", (D, D), BF),
    ("woo", (256, D), BF),
    ("nall", (SLOT, D), BF),
    ("dall", (SLOT, D), BF),
    ("sall", (SLOT, D), BF),
    ("lall", (SLOT, D), BF),
    ("qb", (SLOT, 256), BF),
    ("kb", (SLOT, 256), BF),
    ("vb", (SLOT, 256), BF),
    ("mix", (SLOT, 256), BF),
    ("exact", (SLOT, 256), F32),
    ("lse", (SLOT, 128), F32),
    ("mixs", (4, 384, 128), BF),
    ("mixin", (4, 384, 128), BF),
    ("gh", (256, D), F32),
    ("act", (SLOT, D), BF),
    ("gup", (SLOT, D), BF),
    ("kvin", (4, 256, 384), BF),
    ("qs_", (4, 384, 128), BF),
    ("qin", (4, 384, 128), BF),
    ("pdy", (8, 96, 256), BF),
    ("pdz", (8, 96, 512), BF),
    ("pup", (6, D, 128), BF),
    ("pou", (8, 144, 128), BF),
    ("pqk", (12, 48, D), BF),
    ("ydy", (4, 96, 256), BF),
    ("ydz", (1, 96, 512), BF),
    ("yup", (6, D, 128), BF),
    ("you", (4, 144, 128), BF),
    ("yqk", (12, 48, D), BF),
    ("zdy", (4, 96, 256), BF),
    ("zdz", (4, 2, 96, 512), BF),
    ("zup", (12, D, 128), BF),
    ("zou", (4, 144, 128), BF),
    ("zqk", (24, 48, D), BF),
    ("vec", (8, D), F32),
    ("bias_rows", (24, 128), F32),
    ("small", (2, 4, 16, 128), F32),
    ("ysm", (4, 16, 128), F32),
    ("zsm", (4, 16, 128), F32),
    ("fsm", (4, 16, 128), F32),
)
SEMAPHORES = (
    ("load", 22), ("give", 8),
    ("ns", 5), ("nr", 5), ("ds", 5), ("dr", 5), ("ss", 5), ("sr", 5), ("ls", 5), ("lr", 5),
    ("ms", 3), ("mr", 3), ("kvs", 3), ("kvr", 3), ("qs", 3), ("qr", 3),
    ("ydys", 4), ("ydyr", 4), ("zdys", 4), ("zdyr", 4), ("fdys", 3), ("fdyr", 3),
    ("ydzs", 1), ("ydzr", 1), ("zdzs", 4), ("zdzr", 4), ("fdzs", 3), ("fdzr", 3),
    ("yous", 4), ("your", 4), ("zous", 4), ("zour", 4), ("fous", 3), ("four", 3),
    ("yups", 6), ("yupr", 6), ("zups", 6), ("zupr", 12), ("fups", 9), ("fupr", 9),
    ("yqks", 12), ("yqkr", 12), ("zqks", 12), ("zqkr", 24), ("fqks", 18), ("fqkr", 18),
    ("ysms", 1), ("ysmr", 1), ("zsms", 4), ("zsmr", 4), ("fsms", 3), ("fsmr", 3),
)
INPUTS = ("x", "gains", "shifts", "w_qkv", "qv_bias", "w_out", "biases", "w_up", "up_bias", "w_down", "lengths", "d_out")
IN_PLACE = ("x", "w_qkv", "w_out", "w_up", "w_down", "d_out")
OUTPUTS = (
    ("block_out", (256, D), BF),
    ("grad_inputs", (256, D), F32),
    ("fup", (3, D, 128), BF),
    ("fqk", (6, 48, D), BF),
    ("fdy", (4, 96, 256), BF),
    ("fdz", (4, 96, 512), BF),
    ("fou", (4, 144, 128), BF),
    ("fsum", (16, 128), F32),
)


class Refs:
    pass


def block_rows(block, size=BLOCK, offset=0):
    return pl.ds(pl.multiple_of(block * BLOCK + offset, 128), size)


def one_kernel(*args):
    r = Refs()
    names = [*INPUTS] + ["to_" + o[0] for o in OUTPUTS] + [b[0] for b in OUTPUTS + BUFFERS] + [s[0] for s in SEMAPHORES]
    for name, ref in zip(names, args, strict=True):
        setattr(r, name, ref)
    dp, head = lax.axis_index("dp"), lax.axis_index("head")
    z, y = lax.div(dp, 2), lax.rem(dp, 2)
    px, pc = lax.div(head, 2), lax.rem(head, 2)

    def peer(code):
        return lax.rem(px + (code // 2 if isinstance(code, int) else lax.div(code, 2)), 2) * 2 + lax.rem(
            pc + (code % 2 if isinstance(code, int) else lax.rem(code, 2)), 2
        )

    sib, far, diag = peer(1), peer(2), peer(3)
    other_y = z * 2 + (1 - y)

    def z_shard(k):
        return lax.rem(z + k, 4)

    half = lax.div(z, 2)
    inner = (z == 1) | (z == 2)
    outer = (z == 0) | (z == 3)
    beside = half * 2 + 1 - lax.rem(z, 2)
    z_order = (3 * (1 - half), 2 - half, beside, z)

    sent = []

    def push(src, dst, send, recv, to):
        return pltpu.make_async_remote_copy(
            src_ref=src, dst_ref=dst, send_sem=send, recv_sem=recv, device_id=to, device_id_type=MESH
        )

    def when(cond, body):
        if cond is None:
            body()
        else:
            pl.when(cond)(body)

    given = []

    def give(name):
        copy = pltpu.make_async_copy(getattr(r, name), getattr(r, "to_" + name), r.give.at[len(given)])
        copy.start()
        given.append(copy)

    def start(make, cond=None):
        when(cond, lambda: make().start())
        sent.append((make, cond))

    loads = {}

    def load(name, src, dst):
        loads.setdefault(name, []).append(pltpu.make_async_copy(src, dst, r.load.at[sum(map(len, loads.values()))]))

    load("x", r.x, r.xv)
    load("d", r.d_out, r.dv)
    load("wqkv", r.w_qkv, r.wqkv)
    load("wout", r.w_out, r.wout)
    load("wup", r.w_up, r.wup)
    load("wdown", r.w_down, r.big.at[:, 0:D])
    load("woo", r.w_out.at[pl.ds(pl.multiple_of(head * 192, 64), 192), :], r.woo.at[0:192, :])
    for j in range(6):
        unit = pl.ds(pl.multiple_of((4 * j + head) * 128, 128), 128)
        load("wuo", r.w_up.at[:, unit], r.wuo.at[:, j * 128 : (j + 1) * 128])
        load("wdo", r.w_down.at[unit, :], r.wdo.at[j * 128 : (j + 1) * 128, :])
    for copies in loads.values():
        for copy in copies:
            copy.start()

    def loaded(name):
        for copy in loads[name]:
            copy.wait()

    barrier = pltpu.get_barrier_semaphore()
    for to in [(dp, sib), (dp, far), (dp, diag), (other_y, head)] + [(z_shard(k) * 2 + y, head) for k in (1, 2, 3)]:
        pl.semaphore_signal(barrier, inc=1, device_id=to, device_id_type=MESH)

    gains = r.gains[...].astype(F32)
    shifts = r.shifts[...].astype(F32)
    biases = r.biases[...].astype(F32)
    onlane = lanes_of()
    lengths = r.lengths[...]
    whole = lengths[:, 0:1] == SLOT
    total = jnp.sum(lengths, axis=1, keepdims=True)

    def gather(buf, send, recv):
        def copy_of(index):
            if index == 0:
                rows, to = block_rows(head), sib
            elif index < 3:
                rows, to = block_rows(head, 128, (index - 1) * 128), far
            else:
                rows, to = block_rows(far, 128, (index - 3) * 128), sib
            return push(buf.at[rows, :], buf.at[rows, :], send.at[index], recv.at[index], (dp, to))

        def begin(these=(1, 2, 0)):
            for index in these:
                copy_of(index).start()

        def wait(index):
            copy_of(index).wait_recv()

        def relay(these=(1, 2)):
            for index in these:
                wait(index)
                copy_of(index + 2).start()

        def rest():
            for index in (3, 4):
                wait(index)

        def drain():
            for index in range(5):
                copy_of(index).wait_send()

        return begin, wait, relay, rest, drain

    n_begin, n_wait, n_relay, n_rest, n_drain = gather(r.nall, r.ns, r.nr)
    d_begin, d_wait, d_relay, d_rest, d_drain = gather(r.dall, r.ds, r.dr)
    s_begin, s_wait, s_relay, s_rest, s_drain = gather(r.sall, r.ss, r.sr)
    l_begin, l_wait, l_relay, l_rest, l_drain = gather(r.lall, r.ls, r.lr)

    loaded("x")
    first = norm_parts(r.xv[...].astype(F32), gains[0:1, :], shifts[0:1, :])[2]
    r.nall[block_rows(head), :] = first.astype(BF)
    pl.semaphore_wait(barrier, 7)
    n_begin()
    position = head * BLOCK + lax.broadcasted_iota(jnp.int32, (BLOCK, 1), 0)
    loaded("d")
    r.dall[block_rows(head), :] = (r.dv[...].astype(F32) * jnp.where(position < total, 1.0, 0.0)).astype(BF)
    d_begin((1, 0))
    loaded("wqkv")
    aligned = lax.div(3 * head, 2) * 128
    odd = jnp.where(lax.rem(head, 2) == 1, 1.0, 0.0)
    on_heads = jnp.where(onlane < 192, 1.0, 0.0)

    def own_window(values):
        moved = pltpu.roll(values, 192, 1)
        return (values * (1.0 - odd) + moved * odd) * on_heads

    r.vec[0:2, :] = r.qv_bias[...].astype(F32)
    pair_bias = own_window(r.vec[:, pl.ds(pl.multiple_of(aligned, 128), 256)])
    bias = jnp.concatenate([pair_bias[0:1], jnp.zeros((1, 256), F32), pair_bias[1:2]], axis=1)
    for part in range(3):
        window = pl.ds(pl.multiple_of(part * D + aligned, 128), 256)
        r.wqo[:, part * 256 : (part + 1) * 256] = own_window(r.wqkv[:, window].astype(F32)).astype(BF)

    aux_k = jnp.where((onlane >= 196) & (onlane < 199), 1.0, 0.0)
    aux_v = jnp.where((onlane >= 192) & (onlane < 199) & (onlane != 195), 1.0, 0.0)
    on_aux = jnp.where(onlane >= 192, 1.0, 0.0)

    def project(block):
        rows = block_rows(block)
        projected = (nn(r.nall[rows, :], r.wqo[...]) + bias).astype(BF).astype(F32)
        r.qb[rows, :] = (projected[:, :256] * 0.125 + lane_is(192 + block)).astype(BF)
        off = jnp.where((onlane >= 192) & (onlane < 196) & (onlane != 192 + block), 1.0, 0.0)
        r.kb[rows, :] = (projected[:, 256:512] + (aux_k + off * jnp.where(whole, 0.0, FAR))).astype(BF)
        r.vb[rows, :] = (projected[:, 512:] + aux_v).astype(BF)

    project(head)
    n_wait(0)
    project(sib)
    n_relay()
    project(far)
    n_rest()
    project(diag)

    def packed(values):
        third = values[:, 128:]
        return jnp.concatenate([values[:, :128], third[:128] + pltpu.roll(third[128:], 64, 1)], axis=0).astype(BF)

    def unpack(source, dst, base):
        for group in range(4):
            lane = group * 192
            dst[base : base + 256, lane : lane + 128] = source[group, 0:256, :]
            dst[base : base + 128, lane + 128 : lane + 192] = source[group, 256:384, 0:64]
            dst[base + 128 : base + 256, lane + 128 : lane + 192] = source[group, 256:384, 64:128]

    def mix_copy(code):
        return push(r.mixs.at[code], r.mixin.at[head], r.ms.at[code - 1], r.mr.at[code - 1], (dp, peer(code)))

    small_lane = lax.broadcasted_iota(jnp.int32, (1, 128), 1)

    def attend(step, carry):
        code = 3 - step
        block = peer(code)
        rows = block_rows(block)
        queries = r.qb[rows, :]
        mixed = jnp.zeros((BLOCK, 256), F32)
        tops = []
        for n in range(3):
            scores = nt(queries * (head_mask(n) + on_aux).astype(BF), r.kb[...])
            top = jnp.max(scores, axis=1, keepdims=True)
            weights = jnp.exp(scores - top).astype(BF)
            mixed += nn(weights, r.vb[...] * (head_mask(n) + lane_is(192 + n)).astype(BF))
            tops.append(top)
        lse = jnp.zeros((BLOCK, 128), F32)
        scale = jnp.zeros((BLOCK, 256), F32)
        for n in range(3):
            row_sum = jnp.sum(mixed * lane_is(192 + n), axis=1, keepdims=True)
            lse += (tops[n] + jnp.log(row_sum)) * jnp.where(small_lane == n, 1.0, 0.0)
            scale += (1.0 / row_sum) * head_mask(n)
        place = block * BLOCK + lax.broadcasted_iota(jnp.int32, (BLOCK, 1), 0)
        mixed = jnp.where(place < total, mixed * scale, r.vb[rows, :].astype(F32) * on_heads)
        r.exact[rows, :] = mixed
        r.lse[rows, :] = lse
        r.mix[rows, :] = mixed.astype(BF)
        r.mixs[code] = packed(mixed)

        @pl.when(step < 3)
        def _():
            mix_copy(code).start()

        @pl.when(step == 1)
        def _():
            d_begin((2,))

        return carry

    lax.fori_loop(0, 4, attend, 0)
    r.mixin[head] = r.mixs[0]
    d_relay((1,))

    loaded("wout")
    loaded("wup")
    loaded("wdown")
    for code in (3, 2, 1):
        mix_copy(code).wait_recv()
    unpack(r.mixin, r.wqo, 0)
    hidden = r.xv[...].astype(F32) + nn(r.wqo[0:256, :], r.wout[...]) + biases[0:1, :]
    unit, inverse, normed = norm_parts(hidden, gains[1:2, :], shifts[1:2, :])
    second = normed.astype(BF)
    r.sall[block_rows(head), :] = second
    s_begin()
    grad_low = r.dall[block_rows(head), :]
    up_bias = r.up_bias[...].astype(F32)
    r.bias_rows[...] = up_bias
    down = jnp.zeros((BLOCK, D), F32)
    back = jnp.zeros((BLOCK, D), F32)
    for tile in range(4):
        cut = slice(tile * D, (tile + 1) * D)
        up = nn(second, r.wup[:, cut]) + jnp.concatenate([up_bias[6 * tile + i : 6 * tile + i + 1] for i in range(6)], axis=1)
        value, slope = gelu_parts(up)
        w_down = r.big[cut, 0:D]
        down += nn(value.astype(BF), w_down)
        grad_up = nt(grad_low, w_down) * slope
        back += nt(grad_up.astype(BF), r.wup[:, cut])
    r.block_out[...] = (hidden + down + biases[1:2, :]).astype(BF)
    give("block_out")
    grad_block = grad_low.astype(F32)
    grad_hidden = grad_block + norm_back(back, unit, inverse, gains[1:2, :])
    r.gh[...] = grad_hidden
    r.lall[block_rows(head), :] = grad_hidden.astype(BF)
    l_begin()
    r.vec[...] = jnp.zeros_like(r.vec)
    r.vec[1:2, :] = jnp.sum(back * unit, axis=0, keepdims=True)
    r.vec[3:4, :] = jnp.sum(back, axis=0, keepdims=True)
    r.vec[6:7, :] = jnp.sum(grad_hidden, axis=0, keepdims=True)
    r.vec[7:8, :] = jnp.sum(grad_block, axis=0, keepdims=True)

    loaded("wuo")
    loaded("wdo")
    loaded("woo")
    own_bias = jnp.concatenate([r.bias_rows[pl.ds(4 * j + head, 1), :] for j in range(6)], axis=1)

    def feed(step, sums):
        @pl.when(step == 1)
        def _():
            d_wait(0)
            s_wait(0)

        @pl.when(step == 2)
        def _():
            d_relay((2,))
            s_relay()

        @pl.when(step == 3)
        def _():
            d_rest()
            s_rest()

        rows = block_rows(peer(step))
        up = nn(r.sall[rows, :], r.wuo[...]) + own_bias
        value, slope = gelu_parts(up)
        r.act[rows, :] = value.astype(BF)
        grad_up = nt(r.dall[rows, :], r.wdo[...]) * slope
        r.gup[rows, :] = grad_up.astype(BF)
        return sums + jnp.sum(grad_up, axis=0, keepdims=True)

    sums = lax.fori_loop(0, 4, feed, jnp.zeros((1, D), F32))
    def parts_of(name):
        refs = [getattr(r, part + name) for part in ("p", "y", "z", "f")]
        return refs + [getattr(r, part + name + end) for part in ("y", "z", "f") for end in ("s", "r")]

    def finals(fin, fs, fr):
        def f_copy(code):
            place = far if code == 3 else head
            to = far if code == 2 else sib
            return push(fin.at[place], fin.at[place], fs.at[code - 1], fr.at[code - 1], (dp, to))

        def begin():
            for code in (2, 1):
                start(lambda code=code: f_copy(code))

        def relay():
            f_copy(2).wait_recv()
            start(lambda: f_copy(3))

        def rest():
            f_copy(1).wait_recv()
            f_copy(3).wait_recv()

        return begin, relay, rest

    def add_to(ref, at, more):
        ref[at] = (ref[at].astype(F32) + more.astype(F32)).astype(BF)

    def y_first(name):
        own, ybuf, zbuf, fin, ys, yr, zs, zr, fs, fr = parts_of(name)
        f_begin, relay, rest = finals(fin, fs, fr)

        def y_copy(t):
            src = own.at[z_order[t] * 2 + (1 - y)]
            return push(src, ybuf.at[t], ys.at[t], yr.at[t], (other_y, head))

        def near_copy(t):
            return push(own.at[z_order[t] * 2 + y], zbuf.at[t], zs.at[t], zr.at[t], (beside * 2 + y, head))

        def across_copy(t):
            shard = z_order[t] * 2 + y
            return push(own.at[shard], zbuf.at[3], zs.at[t], zr.at[3], (shard, head))

        def begin():
            for t in range(4):
                start(lambda t=t: y_copy(t))

        def pair(t):
            y_copy(t).wait_recv()
            add_to(own, z_order[t] * 2 + y, ybuf[t])
            if t == 2:
                near_copy(t).start()
            elif t < 2:
                pl.when(outer)(lambda: near_copy(t).start())

        def fold(t):
            @pl.when(inner)
            def _():
                near_copy(t).wait_recv()
                add_to(own, z_order[t] * 2 + y, zbuf[t])
                across_copy(t).start()

        def total_up():
            near_copy(2).wait_recv()
            across_copy(0).wait_recv()
            fin[head] = (own[dp].astype(F32) + zbuf[2].astype(F32) + zbuf[3].astype(F32)).astype(BF)
            f_begin()
            sent.append((lambda: near_copy(2), None))
            for t in (0, 1):
                sent.append((lambda t=t: near_copy(t), outer))
                sent.append((lambda t=t: across_copy(t), inner))

        return begin, pair, fold, total_up, relay, rest

    def z_first(name):
        own, ybuf, zbuf, fin, ys, yr, zs, zr, fs, fr = parts_of(name)
        f_begin, relay, rest = finals(fin, fs, fr)

        def both(t):
            return pl.ds(z_order[t] * 2, 2)

        def near_copy(t):
            return push(own.at[both(t)], zbuf.at[t], zs.at[t], zr.at[t], (beside * 2 + y, head))

        def across_copy(t):
            return push(own.at[both(t)], zbuf.at[3], zs.at[t], zr.at[3], (z_order[t] * 2 + y, head))

        def y_copy():
            return push(own.at[z * 2 + (1 - y)], ybuf.at[0], ys.at[0], yr.at[0], (other_y, head))

        def begin():
            for t in (0, 1):
                start(lambda t=t: near_copy(t), outer)
            start(lambda: near_copy(2))

        def fold(t):
            @pl.when(inner)
            def _():
                near_copy(t).wait_recv()
                add_to(own, both(t), zbuf[t])
                across_copy(t).start()

        def pair():
            near_copy(2).wait_recv()
            across_copy(0).wait_recv()
            add_to(own, both(3), zbuf[2].astype(F32) + zbuf[3].astype(F32))
            y_copy().start()

        def total_up():
            y_copy().wait_recv()
            fin[head] = (own[dp].astype(F32) + ybuf[0].astype(F32)).astype(BF)
            f_begin()
            for t in (0, 1):
                sent.append((lambda t=t: across_copy(t), inner))
            sent.append((y_copy, None))

        return begin, fold, pair, total_up, relay, rest

    def irregular(name, count, per_shard, number_of, owner_of):
        own, ybuf, zbuf, fin, ys, yr, zs, zr, fs, fr = parts_of(name)

        def facts(j):
            number = number_of(j)
            shard = lax.div(number, per_shard)
            return shard, lax.div(shard, 2), lax.rem(shard, 2), lax.rem(number, per_shard)

        def y_copy(j):
            return push(own.at[j], ybuf.at[j], ys.at[j], yr.at[j], (other_y, head))

        def near_copy(j):
            slot = jnp.where(facts(j)[1] == beside, count + facts(j)[3], j)
            return push(own.at[j], zbuf.at[slot], zs.at[j], zr.at[slot], (beside * 2 + y, head))

        def near_arrival(j):
            return push(own.at[j], zbuf.at[j], zs.at[j], zr.at[j], (beside * 2 + y, head))

        def across_copy(j):
            shard, _, _, place = facts(j)
            return push(own.at[j], zbuf.at[count + per_shard + place], zs.at[j], zr.at[count + per_shard + place], (shard, head))

        def last_arrival(j, base):
            place = base + facts(j)[3]
            return push(own.at[j], zbuf.at[place], zs.at[j], zr.at[place], (dp, sib)), place

        def f_copy(code, place):
            index = (code - 1) * per_shard + place
            to = far if code == 2 else sib
            return push(fin.at[place], fin.at[place], fs.at[index], fr.at[index], (dp, to))

        def begin(these=range(count)):
            for j in these:
                start(lambda j=j: y_copy(j), facts(j)[2] != y)

        def mine(j):
            return facts(j)[2] == y

        def other_half(j):
            return lax.div(facts(j)[1], 2) != half

        def to_near(j):
            return mine(j) & ((facts(j)[1] == beside) | (other_half(j) & outer))

        def to_across(j):
            return mine(j) & other_half(j) & inner

        def fold(j):
            @pl.when(to_across(j))
            def _():
                near_arrival(j).wait_recv()
                add_to(own, j, zbuf[j])
                across_copy(j).start()

        def pair(j):
            @pl.when(mine(j))
            def _():
                y_copy(j).wait_recv()
                add_to(own, j, ybuf[j])

            pl.when(to_near(j))(lambda: near_copy(j).start())

        def total_up(these=range(count)):
            for j in these:
                sent.append((lambda j=j: near_copy(j), to_near(j)))
                sent.append((lambda j=j: across_copy(j), to_across(j)))
                shard, _, _, place = facts(j)

                def body(j=j, place=place):
                    value = own[j].astype(F32)
                    for base in (count, count + per_shard):
                        copy, slot = last_arrival(j, base)
                        copy.wait_recv()
                        value += zbuf[slot].astype(F32)
                    fin[place] = value.astype(BF)
                    f_copy(2, place).start()
                    f_copy(1, place).start()

                pl.when(shard == dp)(body)

        def relay():
            for place in range(per_shard):
                owner = owner_of(per_shard * dp + place)
                for code in (1, 2):
                    sent.append((lambda code=code, place=place: f_copy(code, place), owner == head))

                def body(place=place):
                    f_copy(2, place).wait_recv()
                    f_copy(3, place).start()

                pl.when(owner == far)(body)
                sent.append((lambda place=place: f_copy(3, place), owner == far))

        def rest():
            for place in range(per_shard):
                owner = owner_of(per_shard * dp + place)
                for code, source in ((1, sib), (3, diag)):
                    pl.when(owner == source)(lambda code=code, place=place: f_copy(code, place).wait_recv())

        return begin, pair, fold, total_up, relay, rest

    dy_begin, dy_pair, dy_fold, dy_total, dy_relay, dy_rest = y_first("dy")
    dz_begin, dz_fold, dz_pair, dz_total, dz_relay, dz_rest = z_first("dz")
    ou_begin, ou_pair, ou_fold, ou_total, ou_relay, ou_rest = y_first("ou")
    up_begin, up_pair, up_fold, up_total, up_relay, up_rest = irregular(
        "up", 6, 3, lambda j: 4 * j + head, lambda number: lax.rem(number, 4)
    )
    qk_begin, qk_pair, qk_fold, qk_total, qk_relay, qk_rest = irregular(
        "qk",
        12,
        6,
        lambda j: ((j // 4) * 8 + 2 * head + j // 2 % 2) * 2 + j % 2,
        lambda number: lax.div(lax.rem(lax.div(number, 2), 8), 2),
    )

    r.pdz[...] = tn(r.dall[...], r.act[:, 256:]).astype(BF).reshape(8, 96, 512)
    dz_begin()
    r.pdy[...] = tn(r.dall[...], r.act[:, :256]).astype(BF).reshape(8, 96, 256)
    dy_begin()
    up_grad = tn(r.sall[...], r.gup[...]).astype(BF)
    for j in range(6):
        r.pup[j] = up_grad[:, j * 128 : (j + 1) * 128]
    up_begin()

    r.small[...] = jnp.zeros_like(r.small)
    for j in range(6):
        number = 4 * j + head
        shard = lax.div(number, 3)
        r.small[lax.rem(shard, 2), lax.div(shard, 2), pl.ds(8 + lax.rem(number, 3), 1), :] = sums[
            :, j * 128 : (j + 1) * 128
        ]

    q_aug, g_aug = r.act, r.gup
    tile_lane = lanes_of(128)
    spot_row, spot_lane = (lax.broadcasted_iota(jnp.int32, (128, 128), axis) for axis in (0, 1))
    spots = [
        jnp.where((spot_lane == 68 + lax.div(spot_row, 3)) & (lax.rem(spot_row, 3) == n) & (spot_row < 9), 1.0, 0.0)
        for n in range(3)
    ]
    spots = [spot.astype(BF) for spot in spots]

    def aux_of(columns):
        high, middle, low = split_three(columns)
        return (high + pltpu.roll(middle, 3, 1) + pltpu.roll(low, 6, 1)).astype(BF)

    def write_aug(dst, rows, source, aux, keep):
        left = source[:, :128]
        right = source[:, 128:].astype(F32)
        for n in range(3):
            if n < 2:
                part = left * jnp.where(lax.div(tile_lane, 64) == n, 1.0, 0.0).astype(BF)
            else:
                part = jnp.zeros((256, 128), BF)
            dst[rows, n * 256 : n * 256 + 128] = part
            mask = jnp.where(tile_lane < 64, 1.0 if n == 2 else 0.0, keep)
            dst[rows, n * 256 + 128 : (n + 1) * 256] = (right * mask + nn(aux, spots[n])).astype(BF)

    def augment_q(block, carry):
        rows = pl.ds(pl.multiple_of(block * 256, 256), 256)
        write_aug(q_aug, rows, r.qb[rows, :], aux_of(-r.lse[rows, :]), 1.0)
        return carry

    lax.fori_loop(0, 4, augment_q, 0)
    sum_row, sum_lane = (lax.broadcasted_iota(jnp.int32, (256, 128), axis) for axis in (0, 1))
    head_sums = jnp.where((lax.div(sum_row, 64) == sum_lane) & (sum_row < 192), 1.0, 0.0).astype(BF)
    r.woo[192:256, :] = jnp.zeros((64, D), BF)
    for t in range(4):
        dy_pair(t)
    dz_fold(0)
    s_drain()
    d_drain()
    dkv, dq, gm = r.sall.at[:, 0:384], r.sall.at[:, 384:640], r.dall.at[:, 0:256]
    l_wait(0)
    l_relay()
    l_rest()
    gm[...] = nt(r.lall[...], r.woo[...]).astype(BF)

    out_grad = tn(r.lall[...], r.mix[...]).reshape(8, 96, 256)
    r.pou[:, 0:96, :] = out_grad[:, :, :128].astype(BF)
    third = out_grad[:, :, 128:].reshape(8, 2, 48, 128)
    moved = pltpu.roll(third[:, 1].reshape(384, 128), 64, 1).reshape(8, 48, 128)
    r.pou[:, 96:144, :] = (third[:, 0] + moved).astype(BF)
    ou_begin()

    def augment_g(block, carry):
        rows = pl.ds(pl.multiple_of(block * 256, 256), 256)
        grads = gm[rows, :]
        product = grads.astype(F32) * r.exact[rows, :]
        inner = jnp.zeros((256, 128), F32)
        for part in split_three(product):
            inner += nn(part.astype(BF), head_sums)
        write_aug(g_aug, rows, grads, aux_of(-inner), 0.0)
        return carry

    lax.fori_loop(0, 4, augment_g, 0)
    dz_fold(1)

    def kv_copy(code):
        rows = block_rows(peer(code))
        return push(r.sall.at[rows, 0:384], r.kvin.at[head], r.kvs.at[code - 1], r.kvr.at[code - 1], (dp, peer(code)))

    def q_copy(code):
        return push(r.qs_.at[code], r.qin.at[head], r.qs.at[code - 1], r.qr.at[code - 1], (dp, peer(code)))

    def attend_back(step, carry):
        code = 3 - step
        block = peer(code)
        rows = block_rows(block)
        key_grad = jnp.zeros((BLOCK, 256), F32)
        value_grad = jnp.zeros((BLOCK, 256), F32)
        for n in range(3):
            mask = head_mask(n)
            lanes = slice(n * 256, (n + 1) * 256)
            probs = jnp.exp(nt(r.kb[rows, :], q_aug[:, lanes]))
            grad_scores = (probs * nt(r.vb[rows, :], g_aug[:, lanes])).astype(BF)
            r.big[pl.ds(pl.multiple_of(n * SLOT + block * BLOCK, 256), BLOCK), :] = grad_scores
            key_grad += nn(grad_scores, q_aug[:, lanes]) * mask
            value_grad += nn(probs.astype(BF), g_aug[:, lanes]) * mask
        dkv[rows, 0:192] = key_grad[:, :192].astype(BF)
        dkv[rows, 192:384] = value_grad[:, :192].astype(BF)

        @pl.when(step < 3)
        def _():
            kv_copy(code).start()

        @pl.when(step == 1)
        def _():
            dz_pair()
            dy_fold(0)
            for j in (0, 1, 2):
                up_pair(j)

        @pl.when(step == 2)
        def _():
            dy_fold(1)
            up_pair(3)

        @pl.when(step == 3)
        def _():
            up_pair(4)
            up_pair(5)

        return carry

    lax.fori_loop(0, 4, attend_back, 0)
    r.kvin[head] = dkv[block_rows(head), :]
    r.pqk[4:12] = tn(dkv[...], r.nall[...]).astype(BF).reshape(8, 48, D)
    qk_begin(range(4, 12))

    def query_back(step, carry):
        code = 3 - step
        block = peer(code)
        rows = block_rows(block)
        query_grad = jnp.zeros((BLOCK, 256), F32)
        for n in range(3):
            part = r.big[n * SLOT : (n + 1) * SLOT, pl.ds(pl.multiple_of(block * BLOCK, 256), BLOCK)]
            query_grad += tn(part, r.kb[...] * head_mask(n).astype(BF))
        query_grad = query_grad * 0.125
        dq[rows, :] = query_grad.astype(BF)
        r.qs_[code] = packed(query_grad)

        @pl.when(step < 3)
        def _():
            q_copy(code).start()

        return carry

    lax.fori_loop(0, 4, query_back, 0)
    r.qin[head] = r.qs_[0]
    r.pqk[0:4] = tn(dq[...], r.nall[...])[:192].astype(BF).reshape(4, 48, D)
    qk_begin(range(4))
    for t in range(4):
        ou_pair(t)
    for j in (0, 1, 2):
        up_fold(j)
    dy_total()
    dz_total()
    for j in range(4, 8):
        qk_pair(j)
    for j in (3, 4, 5):
        up_fold(j)
    for j in range(8, 12):
        qk_pair(j)

    for code in (3, 2, 1):
        kv_copy(code).wait_recv()
        q_copy(code).wait_recv()
    unpack(r.qin, r.wuo, 0)
    for group in range(4):
        lanes = slice(group * 192, (group + 1) * 192)
        r.wuo[256:512, lanes] = r.kvin[group][:, :192]
        r.wuo[512:768, lanes] = r.kvin[group][:, 192:]
    grad_first = nt(r.wuo[0:256, :], r.wqkv[:, 0:D])
    grad_first += nt(r.wuo[256:512, :], r.wqkv[:, D : 2 * D])
    grad_first += nt(r.wuo[512:768, :], r.wqkv[:, 2 * D :])
    unit, inverse, _ = norm_parts(r.xv[...].astype(F32), gains[0:1, :], shifts[0:1, :])
    r.grad_inputs[...] = r.gh[...] + norm_back(grad_first, unit, inverse, gains[0:1, :])
    give("grad_inputs")
    r.vec[0:1, :] = jnp.sum(grad_first * unit, axis=0, keepdims=True)
    r.vec[2:3, :] = jnp.sum(grad_first, axis=0, keepdims=True)
    query_sum = jnp.sum(dq[...].astype(F32), axis=0, keepdims=True)
    value_sum = jnp.sum(dkv[:, 128:384].astype(F32), axis=0, keepdims=True)
    for group in range(4):
        mine = jnp.where(head == group, 1.0, 0.0)
        r.vec[4:5, group * 192 : (group + 1) * 192] = query_sum[:, :192] * mine
        r.vec[5:6, group * 192 : (group + 1) * 192] = value_sum[:, 64:] * mine
    for shard in range(8):
        r.small[shard % 2, shard // 2, 0:8, 0:96] = r.vec[:, shard * 96 : (shard + 1) * 96]

    def small_y():
        return push(r.small.at[1 - y], r.ysm, r.ysms.at[0], r.ysmr.at[0], (other_y, head))

    def small_z(k):
        return push(
            r.small.at[y, z_shard(k)], r.zsm.at[k], r.zsms.at[k], r.zsmr.at[k], (z_shard(k) * 2 + y, head)
        )

    def small_f(code):
        return push(r.fsm.at[head], r.fsm.at[head], r.fsms.at[code - 1], r.fsmr.at[code - 1], (dp, peer(code)))

    start(small_y)
    for j in range(4):
        qk_pair(j)
    ou_fold(0)
    ou_fold(1)
    for j in range(4, 12):
        qk_fold(j)
    up_total()
    for j in range(4):
        qk_fold(j)
    ou_total()
    dy_relay()
    dz_relay()
    small_y().wait_recv()
    r.small[y] = r.small[y] + r.ysm[...]
    for k in (1, 2, 3):
        start(lambda k=k: small_z(k))
    up_relay()
    qk_total(range(4, 12))
    ou_relay()
    qk_total(range(4))
    for k in (1, 2, 3):
        small_z(k).wait_recv()
    r.fsm[head] = r.small[y, z] + r.zsm[1] + r.zsm[2] + r.zsm[3]
    for code in (2, 3, 1):
        start(lambda code=code: small_f(code))
    dy_rest()
    give("fdy")
    dz_rest()
    give("fdz")
    qk_relay()
    up_rest()
    give("fup")
    ou_rest()
    give("fou")
    qk_rest()
    give("fqk")
    for code in (2, 3, 1):
        small_f(code).wait_recv()
    r.fsum[...] = r.fsm[0] + r.fsm[1] + r.fsm[2] + r.fsm[3]
    give("fsum")
    n_drain()
    l_drain()
    for make, cond in sent:
        when(cond, lambda make=make: make().wait_send())
    for code in (1, 2, 3):
        mix_copy(code).wait_send()
        kv_copy(code).wait_send()
        q_copy(code).wait_send()
    for copy in given:
        copy.wait()


def emit_kernel(
    block_in, inputs_in, fup, fqk, fdy, fdz, fou, fsum,
    block_out, grad_inputs, gains, shifts, qkv, qv_bias, out, out_biases, up, up_bias, down,
    block_v, inputs_v, fup_v, fqk_v, fdy_v, fdz_v, fou_v, fsum_v, up_v, qkv_v, down_v, out_v, sems,
):
    count = []

    def begin(src, dst):
        count.append(pltpu.make_async_copy(src, dst, sems.at[len(count)]))
        count[-1].start()
        return count[-1]

    pairs = (
        (fdy, fdy_v), (fdz, fdz_v), (fup, fup_v), (inputs_in, inputs_v), (block_in, block_v), (fqk, fqk_v), (fou, fou_v),
        (fsum, fsum_v),
    )
    arrivals = [begin(src, dst) for src, dst in pairs]
    results = []
    arrivals[0].wait()
    arrivals[1].wait()
    for group in range(4):
        for j in range(6):
            place = (4 * j + group) * 128
            source, at = (fdy_v, j * 128) if j < 2 else (fdz_v, j * 128 - 256)
            down_v[:, place : place + 128] = source[group, :, at : at + 128].astype(F32)
    results.append(begin(down_v, down))
    arrivals[2].wait()
    for i in range(3):
        up_v[:, i * 128 : (i + 1) * 128] = fup_v[i].astype(F32)
    results.append(begin(up_v, up))
    for arrival, src, dst in ((3, inputs_v, grad_inputs), (4, block_v, block_out)):
        arrivals[arrival].wait()
        results.append(begin(src, dst))
    arrivals[5].wait()
    qkv_v[...] = fqk_v[...].reshape(288, D).astype(F32)
    results.append(begin(qkv_v, qkv))
    arrivals[6].wait()
    for group in range(4):
        piece, lane = fou_v[group].astype(F32), group * 192
        out_v[:, lane : lane + 128] = piece[0:96]
        out_v[0:48, lane + 128 : lane + 192] = piece[96:144, 0:64]
        out_v[48:96, lane + 128 : lane + 192] = piece[96:144, 64:128]
    results.append(begin(out_v, out))
    arrivals[7].wait()
    for index, ref in enumerate((gains, shifts, qv_bias, out_biases)):
        ref[...] = fsum_v[2 * index : 2 * index + 2, 0:96]
    up_bias[...] = fsum_v[8:11, :]
    for copy in results:
        copy.wait()


def per_device(x, norm_gains, norm_shifts, w_qkv, qv_bias, w_out, out_biases, w_up, up_bias, w_down, lengths, d_out):
    values = dict(
        x=x[0], gains=norm_gains, shifts=norm_shifts, w_qkv=w_qkv, qv_bias=qv_bias, w_out=w_out, biases=out_biases,
        w_up=w_up, up_bias=up_bias.reshape(24, 128), w_down=w_down, lengths=lengths, d_out=d_out[0],
    )
    place = {True: pl.BlockSpec(memory_space=pl.ANY), False: pl.BlockSpec(memory_space=pltpu.VMEM)}
    block_out, grad_inputs, fup, fqk, fdy, fdz, fou, fsum = pl.pallas_call(
        one_kernel,
        out_shape=[jax.ShapeDtypeStruct(shape, kind) for _, shape, kind in OUTPUTS],
        in_specs=[place[name in IN_PLACE] for name in INPUTS],
        out_specs=[place[True]] * len(OUTPUTS),
        scratch_shapes=[pltpu.VMEM(shape, kind) for _, shape, kind in OUTPUTS + BUFFERS]
        + [pltpu.SemaphoreType.DMA((count,)) for _, count in SEMAPHORES],
        compiler_params=pltpu.CompilerParams(
            collective_id=0, has_side_effects=True, vmem_limit_bytes=VMEM_LIMIT
        ),
        name="block",
    )(*(values[name] for name in INPUTS))
    anywhere = pl.BlockSpec(memory_space=pl.ANY)
    shapes = [(256, D), (256, D), (2, 96), (2, 96), (288, D), (2, 96), (96, D), (2, 96), (D, 384), (3, 128), (96, FF)]
    outs = pl.pallas_call(
        emit_kernel,
        out_shape=[jax.ShapeDtypeStruct(shape, F32 if n else BF) for n, shape in enumerate(shapes)],
        in_specs=[anywhere] * 8,
        out_specs=[anywhere] * 2 + [anywhere if shape[0] > 16 else place[False] for shape in shapes[2:]],
        scratch_shapes=[pltpu.VMEM(shape, kind) for _, shape, kind in OUTPUTS]
        + [pltpu.VMEM(shape, F32) for shape in ((D, 384), (288, D), (96, FF), (96, D))]
        + [pltpu.SemaphoreType.DMA((14,))],
        compiler_params=pltpu.CompilerParams(vmem_limit_bytes=VMEM_LIMIT),
        name="emit",
    )(block_out, grad_inputs, fup, fqk, fdy, fdz, fou, fsum)
    return (
        outs[0][None], outs[1][None], outs[2], outs[3], outs[4].T, outs[5], outs[6].T, outs[7], outs[8],
        outs[9].reshape(384), outs[10].T,
    )


def solution(mesh):
    split = P("dp", "head", None)
    placed = (split,) + (P(),) * 9 + (P("dp", None), split)
    return jax.shard_map(
        per_device if dict(mesh.shape) == {"dp": 8, "head": 4} else general_device,
        mesh=mesh,
        in_specs=placed,
        out_specs=(split, split) + (P(None, "dp"),) * 7 + (P("dp"), P(None, "dp")),
        check_vma=False,
    )
```

```python
import functools

import jax
import jax.numpy as jnp
from jax import lax
from jax.experimental import pallas as pl
from jax.experimental.pallas import tpu as pltpu
from jax.sharding import PartitionSpec as P

D = 768
HEADS = 12
HDIM = 64
FF = 3072
SLOT = 1024
EPSILON = 1e-06
BF = jnp.bfloat16
F32 = jnp.float32
FAR = -1e30
VMEM_LIMIT = 63 * 1024 * 1024


def nn(a, b):
    return lax.dot_general(a, b, (((1,), (0,)), ((), ())), preferred_element_type=F32)


def nt(a, b):
    return lax.dot_general(a, b, (((1,), (1,)), ((), ())), preferred_element_type=F32)


def tn(a, b):
    return lax.dot_general(a, b, (((0,), (0,)), ((), ())), preferred_element_type=F32)


def norm_parts(values, norm_gain, norm_shift):
    average = jnp.mean(values, axis=-1, keepdims=True)
    centered = values - average
    variance = jnp.mean(centered * centered, axis=-1, keepdims=True)
    inverse = lax.rsqrt(variance + EPSILON)
    unit = centered * inverse
    return unit, inverse, unit * norm_gain + norm_shift


def norm_back(grad_normed, unit, inverse, norm_gain):
    grad_unit = grad_normed * norm_gain
    first_mean = jnp.mean(grad_unit, axis=-1, keepdims=True)
    second_mean = jnp.mean(grad_unit * unit, axis=-1, keepdims=True)
    return inverse * (grad_unit - first_mean - unit * second_mean)


def gelu_parts(values):
    cumulative = 0.5 + 0.5 * lax.erf(values * 0.7071067811865476)
    density = jnp.exp(values * values * -0.5) * 0.3989422804014327
    return values * cumulative, cumulative + values * density


def lanes_of(width=256):
    return lax.broadcasted_iota(jnp.int32, (1, width), 1)


def head_mask(head):
    lane = lanes_of()
    return jnp.where((lane >= head * HDIM) & (lane < (head + 1) * HDIM), 1.0, 0.0)


def lane_is(index):
    return jnp.where(lanes_of() == index, 1.0, 0.0)


def split_three(column):
    high = column.astype(BF).astype(F32)
    rest = column - high
    middle = rest.astype(BF).astype(F32)
    return high, middle, rest - middle


def attend_forward(normed, weight, bias, lengths, q_ref, k_ref, v_ref, mixed_ref, exact_ref, lse_ref):
    whole = lengths[:, 0:1] == SLOT
    total = jnp.sum(lengths, axis=1, keepdims=True)
    onlane = lanes_of()
    aux_k = jnp.where((onlane >= 196) & (onlane < 199), 1.0, 0.0)
    aux_v = jnp.where((onlane >= 192) & (onlane < 199) & (onlane != 195), 1.0, 0.0)
    for block in range(4):
        rows = pl.ds(block * 256, 256)
        projected = nn(normed[rows, :], weight[...]) + bias
        projected = projected.astype(BF).astype(F32)
        q_ref[rows, :] = (projected[:, :256] * 0.125 + lane_is(192 + block)).astype(BF)
        other = jnp.where((onlane >= 192) & (onlane < 196) & (onlane != 192 + block), 1.0, 0.0)
        far = other * jnp.where(whole, 0.0, FAR)
        k_ref[rows, :] = (projected[:, 256:512] + (aux_k + far)).astype(BF)
        v_ref[rows, :] = (projected[:, 512:] + aux_v).astype(BF)
    on_aux = jnp.where(onlane >= 192, 1.0, 0.0)

    def block_step(block, carry):
        rows = pl.ds(pl.multiple_of(block * 256, 256), 256)
        queries = q_ref[rows, :]
        mixed = jnp.zeros((256, 256), F32)
        tops = []
        for head in range(3):
            scores = nt(queries * (head_mask(head) + on_aux).astype(BF), k_ref[...])
            top = jnp.max(scores, axis=1, keepdims=True)
            weights = jnp.exp(scores - top).astype(BF)
            mixed += nn(weights, v_ref[...] * (head_mask(head) + lane_is(192 + head)).astype(BF))
            tops.append(top)
        lse = jnp.zeros((256, 128), F32)
        scale = jnp.zeros((256, 256), F32)
        small = lax.broadcasted_iota(jnp.int32, (1, 128), 1)
        for head in range(3):
            row_sum = jnp.sum(mixed * lane_is(192 + head), axis=1, keepdims=True)
            lse += (tops[head] + jnp.log(row_sum)) * jnp.where(small == head, 1.0, 0.0)
            scale += (1.0 / row_sum) * head_mask(head)
        mixed = mixed * scale
        position = block * 256 + lax.broadcasted_iota(jnp.int32, (256, 1), 0)
        on_heads = jnp.where(onlane < 192, 1.0, 0.0)
        mixed = jnp.where(position < total, mixed, v_ref[rows, :].astype(F32) * on_heads)
        exact_ref[rows, :] = mixed
        mixed_ref[rows, :] = mixed[:, :192].astype(BF)
        lse_ref[rows, :] = lse
        return carry

    lax.fori_loop(0, 4, block_step, 0)


def attend_backward(q_ref, k_ref, v_ref, exact_ref, lse_ref, grad_mixed, q_aug, g_aug, scores_low, dq_acc, dk_acc, dv_acc):
    for head in range(3):
        mask = head_mask(head)

        def augment(block, carry):
            rows = pl.ds(pl.multiple_of(block * 256, 256), 256)
            grads = grad_mixed[rows, :].astype(F32) * mask
            inner = jnp.sum(grads * exact_ref[rows, :], axis=1, keepdims=True)
            lse = lse_ref[rows, :][:, head : head + 1]
            queries = q_ref[rows, :].astype(F32) * (mask + jnp.where(lanes_of() >= 192, 1.0, 0.0))
            for place, part in enumerate(split_three(-lse)):
                queries = queries + part * lane_is(196 + place)
            for place, part in enumerate(split_three(-inner)):
                grads = grads + part * lane_is(196 + place)
            q_aug[rows, :] = queries.astype(BF)
            g_aug[rows, :] = grads.astype(BF)
            return carry

        lax.fori_loop(0, 4, augment, 0)

        def block_step(block, carry):
            rows = pl.ds(pl.multiple_of(block * 256, 256), 256)
            probs = jnp.exp(nt(k_ref[rows, :], q_aug[...]))
            grad_probs = nt(v_ref[rows, :], g_aug[...])
            grad_scores = (probs * grad_probs).astype(BF)
            scores_low[rows, :] = grad_scores
            key_part = nn(grad_scores, q_aug[...]) * mask
            value_part = nn(probs.astype(BF), g_aug[...]) * mask
            if head == 0:
                dk_acc[rows, :] = key_part
                dv_acc[rows, :] = value_part
            else:
                dk_acc[rows, :] += key_part
                dv_acc[rows, :] += value_part
            return carry

        lax.fori_loop(0, 4, block_step, 0)
        query_part = tn(scores_low[...], k_ref[...] * mask.astype(BF)) * 0.125
        if head == 0:
            dq_acc[...] = query_part
        else:
            dq_acc[...] += query_part


def forward_kernel(normed, weight, bias, lengths, q_ref, k_ref, v_ref, mixed_ref, exact_ref, lse_ref):
    attend_forward(normed, weight, bias[...], lengths[...], q_ref, k_ref, v_ref, mixed_ref, exact_ref, lse_ref)


def middle_kernel(
    mixed_in, x_in, d_low, w_out, w_up, w_down, gains, shifts, biases, up_bias,
    block_ref, second_ref, hid_ref, low_ref, sums_ref, mixed_rows, act_ref,
):
    rows = x_in.shape[0]
    for group in range(4):
        mixed_rows[:, group * 192 : (group + 1) * 192] = mixed_in[group]
    hidden = x_in[...].astype(F32) + nn(mixed_rows[...], w_out[...]) + biases[0:1, :]
    unit, inverse, normed = norm_parts(hidden, gains[1:2, :], shifts[1:2, :])
    second = normed.astype(BF)
    second_ref[...] = second
    grad_low = d_low[...]
    down = jnp.zeros((rows, D), F32)
    back = jnp.zeros((rows, D), F32)
    step = 768
    for tile in range(FF // step):
        cut = slice(tile * step, (tile + 1) * step)
        up = nn(second, w_up[:, cut]) + up_bias[:, cut]
        value, slope = gelu_parts(up)
        down += nn(value.astype(BF), w_down[cut, :])
        grad_up = nt(grad_low, w_down[cut, :]) * slope
        back += nt(grad_up.astype(BF), w_up[:, cut])
    block_ref[...] = (hidden + down + biases[1:2, :]).astype(BF)
    grad_block = grad_low.astype(F32)
    grad_hidden = grad_block + norm_back(back, unit, inverse, gains[1:2, :])
    hid_ref[...] = grad_hidden
    low_ref[...] = grad_hidden.astype(BF)
    sums_ref[...] = jnp.zeros_like(sums_ref)
    sums_ref[0:1, :] = jnp.sum(back * unit, axis=0, keepdims=True)
    sums_ref[1:2, :] = jnp.sum(back, axis=0, keepdims=True)
    sums_ref[2:3, :] = jnp.sum(grad_hidden, axis=0, keepdims=True)
    sums_ref[3:4, :] = jnp.sum(grad_block, axis=0, keepdims=True)


def feed_kernel(second, d_low, w_up, w_down, up_bias, up_grad, down_grad, bias_grad, act_ref, grad_ref):
    width = w_up.shape[1]
    bias_grad[...] = jnp.zeros_like(bias_grad)

    def step(block, carry):
        rows = pl.ds(pl.multiple_of(block * 256, 256), 256)
        up = nn(second[rows, :], w_up[...]) + up_bias[...]
        value, slope = gelu_parts(up)
        act_ref[rows, :] = value.astype(BF)
        grad_up = nt(d_low[rows, :], w_down[...]) * slope
        bias_grad[0:1, :] += jnp.sum(grad_up, axis=0, keepdims=True)
        grad_ref[rows, :] = grad_up.astype(BF)
        return carry

    lax.fori_loop(0, 4, step, 0)
    down_grad[...] = tn(d_low[...], act_ref[...]).astype(BF)
    up_grad[...] = tn(grad_ref[...], second[...]).astype(BF)


def backward_kernel(
    grad_low, w_out, normed, mixed, q_ref, k_ref, v_ref, exact_ref, lse_ref,
    grad_ref, out_grad, qkv_grad, bias_grad,
    grad_mixed, q_aug, g_aug, scores_low, dq_acc, dk_acc, dv_acc,
):
    padded = jnp.zeros((64, D), BF)
    weight = jnp.concatenate([w_out[...], padded], axis=0)
    grad_mixed[...] = nt(grad_low[...], weight).astype(BF)
    out_grad[...] = tn(grad_low[...], mixed[...]).astype(BF)
    attend_backward(q_ref, k_ref, v_ref, exact_ref, lse_ref, grad_mixed, q_aug, g_aug, scores_low, dq_acc, dk_acc, dv_acc)
    for place, part in enumerate((dq_acc, dk_acc, dv_acc)):
        grad_ref[:, place * 192 : (place + 1) * 192] = part[:, :192].astype(BF)
    bias_grad[...] = jnp.zeros_like(bias_grad)
    bias_grad[0:1, :] = jnp.sum(grad_ref[...].astype(F32), axis=0, keepdims=True)
    qkv_grad[...] = tn(grad_ref[...], normed[...]).astype(BF)


def last_kernel(grad_in, w_qkv, x_in, hid, gains, shifts, out_ref, sums_ref, grad_rows):
    for part in range(3):
        for group in range(4):
            place = part * D + group * 192
            grad_rows[:, place : place + 192] = grad_in[group][:, part * 192 : (part + 1) * 192]
    grad_first = nt(grad_rows[...], w_qkv[...])
    unit, inverse, _ = norm_parts(x_in[...].astype(F32), gains[0:1, :], shifts[0:1, :])
    out_ref[...] = hid[...] + norm_back(grad_first, unit, inverse, gains[0:1, :])
    sums_ref[...] = jnp.zeros_like(sums_ref)
    sums_ref[0:1, :] = jnp.sum(grad_first * unit, axis=0, keepdims=True)
    sums_ref[1:2, :] = jnp.sum(grad_first, axis=0, keepdims=True)


def whole_call(kernel, outs, scratch=(), name=None):
    return pl.pallas_call(
        kernel,
        out_shape=[jax.ShapeDtypeStruct(*out) for out in outs],
        scratch_shapes=[pltpu.VMEM(*item) for item in scratch],
        compiler_params=pltpu.CompilerParams(vmem_limit_bytes=VMEM_LIMIT),
        name=name,
    )


def general_device(x, norm_gains, norm_shifts, w_qkv, qv_bias, w_out, out_biases, w_up, up_bias, w_down, lengths, d_out):
    groups = lax.axis_size("head")
    shards = lax.axis_size("dp")
    group = lax.axis_index("head")
    rows = x.shape[1]
    own = D // groups
    x = x[0]
    gains = norm_gains.astype(F32)
    shifts = norm_shifts.astype(F32)
    biases = out_biases.astype(F32)
    up_shift = up_bias.astype(F32)
    full_bias = jnp.stack([qv_bias[0], jnp.zeros_like(qv_bias[0]), qv_bias[1]]).astype(F32)

    weight_own = lax.dynamic_index_in_dim(w_qkv.reshape(D, 3, groups, own), group, 2, False)
    weight_own = jnp.pad(weight_own, ((0, 0), (0, 0), (0, 256 - own))).reshape(D, 768)
    bias_own = lax.dynamic_index_in_dim(full_bias.reshape(3, groups, own), group, 1, False)
    bias_own = jnp.pad(bias_own, ((0, 0), (0, 256 - own))).reshape(1, 768)
    out_own = lax.dynamic_slice_in_dim(w_out, group * own, own, 0)
    unit_ff = FF // (shards * groups)
    up_own = lax.dynamic_index_in_dim(w_up.reshape(D, shards, groups, unit_ff), group, 2, False).reshape(D, D)
    down_own = lax.dynamic_index_in_dim(w_down.reshape(shards, groups, unit_ff, D), group, 1, False).reshape(D, D)
    ub_own = lax.dynamic_index_in_dim(up_shift.reshape(shards, groups, unit_ff), group, 1, False).reshape(1, D)

    normed = norm_parts(x.astype(F32), gains[0], shifts[0])[2].astype(BF)
    normed_all = lax.all_gather(normed, "head", axis=0, tiled=True)
    total = jnp.sum(lengths[0])
    position = group * rows + jnp.arange(rows, dtype=jnp.int32)
    d_low = jnp.where((position < total)[:, None], d_out[0], jnp.zeros_like(d_out[0]))
    d_all = lax.all_gather(d_low, "head", axis=0, tiled=True)

    q, k, v, mixed, exact, lse = whole_call(
        forward_kernel,
        [((SLOT, 256), BF)] * 3 + [((SLOT, own), BF), ((SLOT, 256), F32), ((SLOT, 128), F32)],
        name="attend_forward",
    )(normed_all, weight_own, bias_own, lengths)
    mixed_in = lax.all_to_all(mixed.reshape(groups, rows, own), "head", 0, 0, tiled=True)
    block_out, second, hid, hid_low, sums_mid = whole_call(
        middle_kernel,
        [((rows, D), BF), ((rows, D), BF), ((rows, D), F32), ((rows, D), BF), ((8, D), F32)],
        [((rows, D), BF), ((rows, FF), BF)],
        name="middle",
    )(mixed_in, x, d_low, w_out, w_up, w_down, gains, shifts, biases, up_shift.reshape(1, FF))
    second_all = lax.all_gather(second, "head", axis=0, tiled=True)
    low_all = lax.all_gather(hid_low, "head", axis=0, tiled=True)
    up_grad, down_grad, ub_grad = whole_call(
        feed_kernel,
        [((D, D), BF), ((D, D), BF), ((8, D), F32)],
        [((SLOT, D), BF), ((SLOT, D), BF)],
        name="feed",
    )(second_all, d_all, up_own, down_own, ub_own)
    grad_own, out_grad, qkv_grad, qkv_sum = whole_call(
        backward_kernel,
        [((SLOT, 3 * own), BF), ((D, own), BF), ((3 * own, D), BF), ((8, 3 * own), F32)],
        [((SLOT, 256), BF)] * 3 + [((SLOT, SLOT), BF)] + [((SLOT, 256), F32)] * 3,
        name="attend_backward",
    )(low_all, out_own, normed_all, mixed, q, k, v, exact, lse)
    grad_in = lax.all_to_all(grad_own.reshape(groups, rows, 3 * own), "head", 0, 0, tiled=True)
    grad_inputs, sums_last = whole_call(
        last_kernel,
        [((rows, D), F32), ((8, D), F32)],
        [((rows, 3 * D), BF)],
        name="last",
    )(grad_in, w_qkv, x, hid, gains, shifts)

    def scatter(values):
        return lax.psum_scatter(values, "dp", scatter_dimension=0, tiled=True)

    up_part = lax.all_gather(scatter(up_grad), "head", axis=0, tiled=True)
    down_part = lax.all_gather(scatter(down_grad), "head", axis=1, tiled=True)
    out_part = lax.all_gather(scatter(out_grad), "head", axis=1, tiled=True)
    down_out = down_part.astype(F32).T.reshape(groups, shards, unit_ff, D // shards)
    down_out = down_out.transpose(1, 0, 2, 3).reshape(FF, D // shards)
    spread = jnp.zeros((3, groups, own, D), BF)
    spread = lax.dynamic_update_slice(spread, qkv_grad.reshape(3, 1, own, D), (0, group, 0, 0))
    qkv_part = lax.psum(scatter(spread.reshape(3 * D, D)), "head")

    def place_rows(values):
        parts = values.reshape(3, own)
        empty = jnp.zeros((3, groups, own), F32)
        return lax.dynamic_update_slice(empty, parts[:, None], (0, group, 0)).reshape(3, D)

    bias_rows = place_rows(qkv_sum[0])
    ub_rows = lax.dynamic_update_slice(
        jnp.zeros((shards, groups, unit_ff), F32), ub_grad[0].reshape(shards, 1, unit_ff), (0, group, 0)
    ).reshape(4, D)
    small = jnp.concatenate([sums_last[0:2], sums_mid[0:4], bias_rows[0:1], bias_rows[2:3], ub_rows], axis=0)
    small = lax.psum(small, ("dp", "head"))
    shard = lax.axis_index("dp")

    def cut(values):
        width = D // shards
        return lax.dynamic_slice_in_dim(values, shard * width, width, 1)

    ub_out = lax.dynamic_slice_in_dim(small[8:12].reshape(FF), shard * (FF // shards), FF // shards, 0)
    return (
        block_out[None],
        grad_inputs[None],
        cut(jnp.stack([small[0], small[2]])),
        cut(jnp.stack([small[1], small[3]])),
        qkv_part.astype(F32).T,
        cut(small[6:8]),
        out_part.astype(F32).T,
        cut(small[4:6]),
        up_part.astype(F32).T,
        ub_out,
        down_out,
    )


MESH = pl.DeviceIdType.MESH
BLOCK = 256

BUFFERS = (
    ("xv", (256, D), BF),
    ("dv", (256, D), BF),
    ("wqkv", (D, 3 * D), BF),
    ("wout", (D, D), BF),
    ("wup", (D, FF), BF),
    ("big", (3 * SLOT, SLOT), BF),
    ("wqo", (D, D), BF),
    ("wuo", (D, D), BF),
    ("wdo", (D, D), BF),
    ("woo", (256, D), BF),
    ("nall", (SLOT, D), BF),
    ("dall", (SLOT, D), BF),
    ("sall", (SLOT, D), BF),
    ("lall", (SLOT, D), BF),
    ("qb", (SLOT, 256), BF),
    ("kb", (SLOT, 256), BF),
    ("vb", (SLOT, 256), BF),
    ("mix", (SLOT, 256), BF),
    ("exact", (SLOT, 256), F32),
    ("lse", (SLOT, 128), F32),
    ("mixs", (4, 384, 128), BF),
    ("mixin", (4, 384, 128), BF),
    ("gh", (256, D), F32),
    ("act", (SLOT, D), BF),
    ("gup", (SLOT, D), BF),
    ("kin", (4, 384, 128), BF),
    ("vin", (4, 384, 128), BF),
    ("ks_", (4, 384, 128), BF),
    ("vs_", (4, 384, 128), BF),
    ("qs_", (4, 384, 128), BF),
    ("qin", (4, 384, 128), BF),
    ("pdy", (8, 96, 256), BF),
    ("pdz", (8, 96, 512), BF),
    ("pup", (6, D, 128), BF),
    ("pou", (8, 144, 128), BF),
    ("pqk", (12, 48, D), BF),
    ("ydy", (4, 96, 256), BF),
    ("ydz", (1, 96, 512), BF),
    ("yup", (6, D, 128), BF),
    ("you", (4, 144, 128), BF),
    ("yqk", (12, 48, D), BF),
    ("zdy", (4, 96, 256), BF),
    ("zdz", (4, 2, 96, 512), BF),
    ("zup", (12, D, 128), BF),
    ("zou", (4, 144, 128), BF),
    ("zqk", (24, 48, D), BF),
    ("vec", (8, D), F32),
    ("bias_rows", (24, 128), F32),
    ("small", (2, 4, 16, 128), F32),
    ("ysm", (4, 16, 128), F32),
    ("zsm", (4, 16, 128), F32),
    ("fsm", (4, 2, 4, 16, 128), F32),
    ("last", (4, 16, 128), F32),
    ("lasty", (2, 8, 128), F32),
    ("lastz", (5, 8, 128), F32),
    ("lastf", (8, 128), F32),
)
SEMAPHORES = (
    ("load", 22), ("give", 8),
    ("ns", 5), ("nr", 5), ("ds", 5), ("dr", 5), ("ss", 5), ("sr", 5), ("ls", 5), ("lr", 5),
    ("ms", 3), ("mr", 3), ("ks", 3), ("kr", 3), ("vs", 3), ("vr", 3), ("qs", 3), ("qr", 3),
    ("ydys", 4), ("ydyr", 4), ("zdys", 4), ("zdyr", 4), ("fdys", 3), ("fdyr", 3),
    ("ydzs", 1), ("ydzr", 1), ("zdzs", 4), ("zdzr", 4), ("fdzs", 3), ("fdzr", 3),
    ("yous", 4), ("your", 4), ("zous", 4), ("zour", 4), ("fous", 3), ("four", 3),
    ("yups", 6), ("yupr", 6), ("zups", 6), ("zupr", 12), ("fups", 9), ("fupr", 9),
    ("yqks", 12), ("yqkr", 12), ("zqks", 12), ("zqkr", 24), ("fqks", 18), ("fqkr", 18),
    ("ysms", 1), ("ysmr", 1), ("zsms", 4), ("zsmr", 4), ("fsms", 3), ("fsmr", 3),
    ("las", 3), ("lar", 3), ("lays", 1), ("layr", 1), ("lazs", 4), ("lazr", 4),
)
INPUTS = ("x", "gains", "shifts", "w_qkv", "qv_bias", "w_out", "biases", "w_up", "up_bias", "w_down", "lengths", "d_out")
IN_PLACE = ("x", "w_qkv", "w_out", "w_up", "w_down", "d_out")
OUTPUTS = (
    ("block_out", (256, D), BF),
    ("grad_inputs", (256, D), F32),
    ("fup", (3, D, 128), BF),
    ("fqk", (6, 48, D), BF),
    ("fdy", (4, 96, 256), BF),
    ("fdz", (4, 96, 512), BF),
    ("fou", (4, 144, 128), BF),
    ("fsum", (16, 128), F32),
)


class Refs:
    pass


def block_rows(block, size=BLOCK, offset=0):
    return pl.ds(pl.multiple_of(block * BLOCK + offset, 128), size)


def one_kernel(*args):
    r = Refs()
    names = [*INPUTS] + ["to_" + o[0] for o in OUTPUTS] + [b[0] for b in OUTPUTS + BUFFERS] + [s[0] for s in SEMAPHORES]
    for name, ref in zip(names, args, strict=True):
        setattr(r, name, ref)
    dp, head = lax.axis_index("dp"), lax.axis_index("head")
    z, y = lax.div(dp, 2), lax.rem(dp, 2)
    px, pc = lax.div(head, 2), lax.rem(head, 2)

    def peer(code):
        return lax.rem(px + (code // 2 if isinstance(code, int) else lax.div(code, 2)), 2) * 2 + lax.rem(
            pc + (code % 2 if isinstance(code, int) else lax.rem(code, 2)), 2
        )

    sib, far, diag = peer(1), peer(2), peer(3)
    other_y = z * 2 + (1 - y)

    def z_shard(k):
        return lax.rem(z + k, 4)

    half = lax.div(z, 2)
    inner = (z == 1) | (z == 2)
    outer = (z == 0) | (z == 3)
    beside = half * 2 + 1 - lax.rem(z, 2)
    z_order = (3 * (1 - half), 2 - half, beside, z)

    sent = []

    def push(src, dst, send, recv, to):
        return pltpu.make_async_remote_copy(
            src_ref=src, dst_ref=dst, send_sem=send, recv_sem=recv, device_id=to, device_id_type=MESH
        )

    def when(cond, body):
        if cond is None:
            body()
        else:
            pl.when(cond)(body)

    given = []

    def give(name):
        copy = pltpu.make_async_copy(getattr(r, name), getattr(r, "to_" + name), r.give.at[len(given)])
        copy.start()
        given.append(copy)

    def start(make, cond=None):
        when(cond, lambda: make().start())
        sent.append((make, cond))

    loads = {}

    def load(name, src, dst):
        loads.setdefault(name, []).append(pltpu.make_async_copy(src, dst, r.load.at[sum(map(len, loads.values()))]))

    load("x", r.x, r.xv)
    load("d", r.d_out, r.dv)
    load("wqkv", r.w_qkv, r.wqkv)
    load("wout", r.w_out, r.wout)
    load("wup", r.w_up, r.wup)
    load("wdown", r.w_down, r.big.at[:, 0:D])
    load("woo", r.w_out.at[pl.ds(pl.multiple_of(head * 192, 64), 192), :], r.woo.at[0:192, :])
    for j in range(6):
        unit = pl.ds(pl.multiple_of((4 * j + head) * 128, 128), 128)
        load("wuo", r.w_up.at[:, unit], r.wuo.at[:, j * 128 : (j + 1) * 128])
        load("wdo", r.w_down.at[unit, :], r.wdo.at[j * 128 : (j + 1) * 128, :])
    for copies in loads.values():
        for copy in copies:
            copy.start()

    def loaded(name):
        for copy in loads[name]:
            copy.wait()

    barrier = pltpu.get_barrier_semaphore()
    for to in [(dp, sib), (dp, far), (dp, diag), (other_y, head)] + [(z_shard(k) * 2 + y, head) for k in (1, 2, 3)]:
        pl.semaphore_signal(barrier, inc=1, device_id=to, device_id_type=MESH)

    gains = r.gains[...].astype(F32)
    shifts = r.shifts[...].astype(F32)
    biases = r.biases[...].astype(F32)
    onlane = lanes_of()
    lengths = r.lengths[...]
    whole = lengths[:, 0:1] == SLOT
    total = jnp.sum(lengths, axis=1, keepdims=True)

    def piece_rows(block, offset, size):
        return pl.ds(pl.multiple_of(block * BLOCK + offset, 32), size)

    def gather(buf, send, recv, cut=128):
        pieces = ((0, cut), (cut, BLOCK - cut))

        def copy_of(index):
            if index == 0:
                rows, to = block_rows(head), sib
            elif index < 3:
                rows, to = piece_rows(head, *pieces[index - 1]), far
            else:
                rows, to = piece_rows(far, *pieces[index - 3]), sib
            return push(buf.at[rows, :], buf.at[rows, :], send.at[index], recv.at[index], (dp, to))

        def begin(these=(1, 2, 0)):
            for index in these:
                copy_of(index).start()

        def wait(index):
            copy_of(index).wait_recv()

        def relay(these=(1, 2)):
            for index in these:
                wait(index)
                copy_of(index + 2).start()

        def rest():
            for index in (3, 4):
                wait(index)

        def drain():
            for index in range(5):
                copy_of(index).wait_send()

        return begin, wait, relay, rest, drain

    n_begin, n_wait, n_relay, n_rest, n_drain = gather(r.nall, r.ns, r.nr)
    d_begin, d_wait, d_relay, d_rest, d_drain = gather(r.dall, r.ds, r.dr, 160)
    s_begin, s_wait, s_relay, s_rest, s_drain = gather(r.sall, r.ss, r.sr)
    l_begin, l_wait, l_relay, l_rest, l_drain = gather(r.lall, r.ls, r.lr)

    loaded("x")
    first = norm_parts(r.xv[...].astype(F32), gains[0:1, :], shifts[0:1, :])[2]
    r.nall[block_rows(head), :] = first.astype(BF)
    pl.semaphore_wait(barrier, 7)
    n_begin()
    position = head * BLOCK + lax.broadcasted_iota(jnp.int32, (BLOCK, 1), 0)
    loaded("d")
    r.dall[block_rows(head), :] = (r.dv[...].astype(F32) * jnp.where(position < total, 1.0, 0.0)).astype(BF)
    d_begin((1, 0))
    loaded("wqkv")
    aligned = lax.div(3 * head, 2) * 128
    odd = jnp.where(lax.rem(head, 2) == 1, 1.0, 0.0)
    on_heads = jnp.where(onlane < 192, 1.0, 0.0)

    def own_window(values):
        moved = pltpu.roll(values, 192, 1)
        return (values * (1.0 - odd) + moved * odd) * on_heads

    r.vec[0:2, :] = r.qv_bias[...].astype(F32)
    pair_bias = own_window(r.vec[:, pl.ds(pl.multiple_of(aligned, 128), 256)])
    bias = jnp.concatenate([pair_bias[0:1], jnp.zeros((1, 256), F32), pair_bias[1:2]], axis=1)
    for part in range(3):
        window = pl.ds(pl.multiple_of(part * D + aligned, 128), 256)
        r.wqo[:, part * 256 : (part + 1) * 256] = own_window(r.wqkv[:, window].astype(F32)).astype(BF)

    aux_k = jnp.where((onlane >= 196) & (onlane < 199), 1.0, 0.0)
    aux_v = jnp.where((onlane >= 192) & (onlane < 199) & (onlane != 195), 1.0, 0.0)
    on_aux = jnp.where(onlane >= 192, 1.0, 0.0)

    def project(block):
        rows = block_rows(block)
        projected = (nn(r.nall[rows, :], r.wqo[...]) + bias).astype(BF).astype(F32)
        r.qb[rows, :] = (projected[:, :256] * 0.125 + lane_is(192 + block)).astype(BF)
        off = jnp.where((onlane >= 192) & (onlane < 196) & (onlane != 192 + block), 1.0, 0.0)
        r.kb[rows, :] = (projected[:, 256:512] + (aux_k + off * jnp.where(whole, 0.0, FAR))).astype(BF)
        r.vb[rows, :] = (projected[:, 512:] + aux_v).astype(BF)

    project(head)
    n_wait(0)
    project(sib)
    n_relay()
    project(far)
    n_rest()
    project(diag)

    def packed(values):
        third = values[:, 128:]
        return jnp.concatenate([values[:, :128], third[:128] + pltpu.roll(third[128:], 64, 1)], axis=0).astype(BF)

    def unpack(source, dst, base):
        for group in range(4):
            lane = group * 192
            dst[base : base + 256, lane : lane + 128] = source[group, 0:256, :]
            dst[base : base + 128, lane + 128 : lane + 192] = source[group, 256:384, 0:64]
            dst[base + 128 : base + 256, lane + 128 : lane + 192] = source[group, 256:384, 64:128]

    def mix_copy(code):
        return push(r.mixs.at[code], r.mixin.at[head], r.ms.at[code - 1], r.mr.at[code - 1], (dp, peer(code)))

    small_lane = lax.broadcasted_iota(jnp.int32, (1, 128), 1)

    def attend(step, carry):
        code = 3 - step
        block = peer(code)
        rows = block_rows(block)
        queries = r.qb[rows, :]
        mixed = jnp.zeros((BLOCK, 256), F32)
        tops = []
        for n in range(3):
            scores = nt(queries * (head_mask(n) + on_aux).astype(BF), r.kb[...])
            top = jnp.max(scores, axis=1, keepdims=True)
            weights = jnp.exp(scores - top).astype(BF)
            mixed += nn(weights, r.vb[...] * (head_mask(n) + lane_is(192 + n)).astype(BF))
            tops.append(top)
        lse = jnp.zeros((BLOCK, 128), F32)
        scale = jnp.zeros((BLOCK, 256), F32)
        for n in range(3):
            row_sum = jnp.sum(mixed * lane_is(192 + n), axis=1, keepdims=True)
            lse += (tops[n] + jnp.log(row_sum)) * jnp.where(small_lane == n, 1.0, 0.0)
            scale += (1.0 / row_sum) * head_mask(n)
        place = block * BLOCK + lax.broadcasted_iota(jnp.int32, (BLOCK, 1), 0)
        mixed = jnp.where(place < total, mixed * scale, r.vb[rows, :].astype(F32) * on_heads)
        r.exact[rows, :] = mixed
        r.lse[rows, :] = lse
        r.mix[rows, :] = mixed.astype(BF)
        r.mixs[code] = packed(mixed)

        @pl.when(step < 3)
        def _():
            mix_copy(code).start()

        @pl.when(step == 1)
        def _():
            d_begin((2,))

        return carry

    lax.fori_loop(0, 4, attend, 0)
    r.mixin[head] = r.mixs[0]
    d_relay((1,))

    loaded("wout")
    loaded("wup")
    loaded("wdown")
    for code in (3, 2, 1):
        mix_copy(code).wait_recv()
    unpack(r.mixin, r.wqo, 0)
    hidden = r.xv[...].astype(F32) + nn(r.wqo[0:256, :], r.wout[...]) + biases[0:1, :]
    unit, inverse, normed = norm_parts(hidden, gains[1:2, :], shifts[1:2, :])
    second = normed.astype(BF)
    r.sall[block_rows(head), :] = second
    s_begin()
    grad_low = r.dall[block_rows(head), :]
    up_bias = r.up_bias[...].astype(F32)
    r.bias_rows[...] = up_bias
    down = jnp.zeros((BLOCK, D), F32)
    back = jnp.zeros((BLOCK, D), F32)
    for tile in range(4):
        cut = slice(tile * D, (tile + 1) * D)
        up = nn(second, r.wup[:, cut]) + jnp.concatenate([up_bias[6 * tile + i : 6 * tile + i + 1] for i in range(6)], axis=1)
        value, slope = gelu_parts(up)
        w_down = r.big[cut, 0:D]
        down += nn(value.astype(BF), w_down)
        grad_up = nt(grad_low, w_down) * slope
        back += nt(grad_up.astype(BF), r.wup[:, cut])
    r.block_out[...] = (hidden + down + biases[1:2, :]).astype(BF)
    give("block_out")
    grad_block = grad_low.astype(F32)
    grad_hidden = grad_block + norm_back(back, unit, inverse, gains[1:2, :])
    r.gh[...] = grad_hidden
    r.lall[block_rows(head), :] = grad_hidden.astype(BF)
    l_begin()
    r.vec[...] = jnp.zeros_like(r.vec)
    r.vec[1:2, :] = jnp.sum(back * unit, axis=0, keepdims=True)
    r.vec[3:4, :] = jnp.sum(back, axis=0, keepdims=True)
    r.vec[6:7, :] = jnp.sum(grad_hidden, axis=0, keepdims=True)
    r.vec[7:8, :] = jnp.sum(grad_block, axis=0, keepdims=True)

    loaded("wuo")
    loaded("wdo")
    loaded("woo")
    own_bias = jnp.concatenate([r.bias_rows[pl.ds(4 * j + head, 1), :] for j in range(6)], axis=1)

    def feed(step, sums):
        @pl.when(step == 1)
        def _():
            d_wait(0)
            s_wait(0)

        @pl.when(step == 2)
        def _():
            d_relay((2,))
            s_relay()

        @pl.when(step == 3)
        def _():
            d_rest()
            s_rest()

        rows = block_rows(peer(step))
        up = nn(r.sall[rows, :], r.wuo[...]) + own_bias
        value, slope = gelu_parts(up)
        r.act[rows, :] = value.astype(BF)
        grad_up = nt(r.dall[rows, :], r.wdo[...]) * slope
        r.gup[rows, :] = grad_up.astype(BF)
        return sums + jnp.sum(grad_up, axis=0, keepdims=True)

    sums = lax.fori_loop(0, 4, feed, jnp.zeros((1, D), F32))
    def parts_of(name):
        refs = [getattr(r, part + name) for part in ("p", "y", "z", "f")]
        return refs + [getattr(r, part + name + end) for part in ("y", "z", "f") for end in ("s", "r")]

    def finals(fin, fs, fr):
        def f_copy(code):
            place = far if code == 3 else head
            to = far if code == 2 else sib
            return push(fin.at[place], fin.at[place], fs.at[code - 1], fr.at[code - 1], (dp, to))

        def begin():
            for code in (2, 1):
                start(lambda code=code: f_copy(code))

        def relay():
            f_copy(2).wait_recv()
            start(lambda: f_copy(3))

        def rest():
            f_copy(1).wait_recv()
            f_copy(3).wait_recv()

        return begin, relay, rest

    def add_to(ref, at, more):
        ref[at] = (ref[at].astype(F32) + more.astype(F32)).astype(BF)

    def y_first(name):
        own, ybuf, zbuf, fin, ys, yr, zs, zr, fs, fr = parts_of(name)
        f_begin, relay, rest = finals(fin, fs, fr)

        def y_copy(t):
            src = own.at[z_order[t] * 2 + (1 - y)]
            return push(src, ybuf.at[t], ys.at[t], yr.at[t], (other_y, head))

        def near_copy(t):
            return push(own.at[z_order[t] * 2 + y], zbuf.at[t], zs.at[t], zr.at[t], (beside * 2 + y, head))

        def across_copy(t):
            shard = z_order[t] * 2 + y
            return push(own.at[shard], zbuf.at[3], zs.at[t], zr.at[3], (shard, head))

        def begin():
            for t in range(4):
                start(lambda t=t: y_copy(t))

        def pair(t):
            y_copy(t).wait_recv()
            add_to(own, z_order[t] * 2 + y, ybuf[t])
            if t == 2:
                near_copy(t).start()
            elif t < 2:
                pl.when(outer)(lambda: near_copy(t).start())

        def fold(t):
            @pl.when(inner)
            def _():
                near_copy(t).wait_recv()
                add_to(own, z_order[t] * 2 + y, zbuf[t])
                across_copy(t).start()

        def total_up():
            near_copy(2).wait_recv()
            across_copy(0).wait_recv()
            fin[head] = (own[dp].astype(F32) + zbuf[2].astype(F32) + zbuf[3].astype(F32)).astype(BF)
            f_begin()
            sent.append((lambda: near_copy(2), None))
            for t in (0, 1):
                sent.append((lambda t=t: near_copy(t), outer))
                sent.append((lambda t=t: across_copy(t), inner))

        return begin, pair, fold, total_up, relay, rest

    def z_first(name):
        own, ybuf, zbuf, fin, ys, yr, zs, zr, fs, fr = parts_of(name)
        f_begin, relay, rest = finals(fin, fs, fr)

        def both(t):
            return pl.ds(z_order[t] * 2, 2)

        def near_copy(t):
            return push(own.at[both(t)], zbuf.at[t], zs.at[t], zr.at[t], (beside * 2 + y, head))

        def across_copy(t):
            return push(own.at[both(t)], zbuf.at[3], zs.at[t], zr.at[3], (z_order[t] * 2 + y, head))

        def y_copy():
            return push(own.at[z * 2 + (1 - y)], ybuf.at[0], ys.at[0], yr.at[0], (other_y, head))

        def begin():
            for t in (0, 1):
                start(lambda t=t: near_copy(t), outer)
            start(lambda: near_copy(2))

        def fold(t):
            @pl.when(inner)
            def _():
                near_copy(t).wait_recv()
                add_to(own, both(t), zbuf[t])
                across_copy(t).start()

        def pair():
            near_copy(2).wait_recv()
            across_copy(0).wait_recv()
            add_to(own, both(3), zbuf[2].astype(F32) + zbuf[3].astype(F32))
            y_copy().start()

        def total_up():
            y_copy().wait_recv()
            fin[head] = (own[dp].astype(F32) + ybuf[0].astype(F32)).astype(BF)
            f_begin()
            for t in (0, 1):
                sent.append((lambda t=t: across_copy(t), inner))
            sent.append((y_copy, None))

        return begin, fold, pair, total_up, relay, rest

    def irregular(name, count, per_shard, number_of, owner_of):
        own, ybuf, zbuf, fin, ys, yr, zs, zr, fs, fr = parts_of(name)

        def facts(j):
            number = number_of(j)
            shard = lax.div(number, per_shard)
            return shard, lax.div(shard, 2), lax.rem(shard, 2), lax.rem(number, per_shard)

        def y_copy(j):
            return push(own.at[j], ybuf.at[j], ys.at[j], yr.at[j], (other_y, head))

        def near_copy(j):
            slot = jnp.where(facts(j)[1] == beside, count + facts(j)[3], j)
            return push(own.at[j], zbuf.at[slot], zs.at[j], zr.at[slot], (beside * 2 + y, head))

        def near_arrival(j):
            return push(own.at[j], zbuf.at[j], zs.at[j], zr.at[j], (beside * 2 + y, head))

        def across_copy(j):
            shard, _, _, place = facts(j)
            return push(own.at[j], zbuf.at[count + per_shard + place], zs.at[j], zr.at[count + per_shard + place], (shard, head))

        def last_arrival(j, base):
            place = base + facts(j)[3]
            return push(own.at[j], zbuf.at[place], zs.at[j], zr.at[place], (dp, sib)), place

        def f_copy(code, place):
            index = (code - 1) * per_shard + place
            to = far if code == 2 else sib
            return push(fin.at[place], fin.at[place], fs.at[index], fr.at[index], (dp, to))

        def begin(these=range(count)):
            for j in these:
                start(lambda j=j: y_copy(j), facts(j)[2] != y)

        def mine(j):
            return facts(j)[2] == y

        def other_half(j):
            return lax.div(facts(j)[1], 2) != half

        def to_near(j):
            return mine(j) & ((facts(j)[1] == beside) | (other_half(j) & outer))

        def to_across(j):
            return mine(j) & other_half(j) & inner

        def fold(j):
            @pl.when(to_across(j))
            def _():
                near_arrival(j).wait_recv()
                add_to(own, j, zbuf[j])
                across_copy(j).start()

        def pair(j):
            @pl.when(mine(j))
            def _():
                y_copy(j).wait_recv()
                add_to(own, j, ybuf[j])

            pl.when(to_near(j))(lambda: near_copy(j).start())

        def total_up(these=range(count)):
            for j in these:
                sent.append((lambda j=j: near_copy(j), to_near(j)))
                sent.append((lambda j=j: across_copy(j), to_across(j)))
                shard, _, _, place = facts(j)

                def body(j=j, place=place):
                    value = own[j].astype(F32)
                    for base in (count, count + per_shard):
                        copy, slot = last_arrival(j, base)
                        copy.wait_recv()
                        value += zbuf[slot].astype(F32)
                    fin[place] = value.astype(BF)
                    f_copy(2, place).start()
                    f_copy(1, place).start()

                pl.when(shard == dp)(body)

        def relay():
            for place in range(per_shard):
                owner = owner_of(per_shard * dp + place)
                for code in (1, 2):
                    sent.append((lambda code=code, place=place: f_copy(code, place), owner == head))

                def body(place=place):
                    f_copy(2, place).wait_recv()
                    f_copy(3, place).start()

                pl.when(owner == far)(body)
                sent.append((lambda place=place: f_copy(3, place), owner == far))

        def rest():
            for place in range(per_shard):
                owner = owner_of(per_shard * dp + place)
                for code, source in ((1, sib), (3, diag)):
                    pl.when(owner == source)(lambda code=code, place=place: f_copy(code, place).wait_recv())

        return begin, pair, fold, total_up, relay, rest

    dy_begin, dy_pair, dy_fold, dy_total, dy_relay, dy_rest = y_first("dy")
    dz_begin, dz_fold, dz_pair, dz_total, dz_relay, dz_rest = z_first("dz")
    ou_begin, ou_pair, ou_fold, ou_total, ou_relay, ou_rest = y_first("ou")
    up_begin, up_pair, up_fold, up_total, up_relay, up_rest = irregular(
        "up", 6, 3, lambda j: 4 * j + head, lambda number: lax.rem(number, 4)
    )
    qk_begin, qk_pair, qk_fold, qk_total, qk_relay, qk_rest = irregular(
        "qk",
        12,
        6,
        lambda j: ((j // 4) * 8 + 2 * head + j // 2 % 2) * 2 + j % 2,
        lambda number: lax.div(lax.rem(lax.div(number, 2), 8), 2),
    )

    r.pdz[...] = tn(r.dall[...], r.act[:, 256:]).astype(BF).reshape(8, 96, 512)
    dz_begin()
    r.pdy[...] = tn(r.dall[...], r.act[:, :256]).astype(BF).reshape(8, 96, 256)
    dy_begin()
    up_grad = tn(r.sall[...], r.gup[...]).astype(BF)
    for j in range(6):
        r.pup[j] = up_grad[:, j * 128 : (j + 1) * 128]
    up_begin()

    r.fsm[head] = jnp.zeros((2, 4, 16, 128), F32)
    for j in range(6):
        number = 4 * j + head
        shard = lax.div(number, 3)
        r.fsm[head, lax.rem(shard, 2), lax.div(shard, 2), pl.ds(8 + lax.rem(number, 3), 1), :] = sums[
            :, j * 128 : (j + 1) * 128
        ]

    q_aug, g_aug = r.act, r.gup
    tile_lane = lanes_of(128)
    spot_row, spot_lane = (lax.broadcasted_iota(jnp.int32, (128, 128), axis) for axis in (0, 1))
    spots = [
        jnp.where((spot_lane == 68 + lax.div(spot_row, 3)) & (lax.rem(spot_row, 3) == n) & (spot_row < 9), 1.0, 0.0)
        for n in range(3)
    ]
    spots = [spot.astype(BF) for spot in spots]

    def aux_of(columns):
        high, middle, low = split_three(columns)
        return (high + pltpu.roll(middle, 3, 1) + pltpu.roll(low, 6, 1)).astype(BF)

    def write_aug(dst, rows, source, aux, keep):
        left = source[:, :128]
        right = source[:, 128:].astype(F32)
        for n in range(3):
            if n < 2:
                part = left * jnp.where(lax.div(tile_lane, 64) == n, 1.0, 0.0).astype(BF)
            else:
                part = jnp.zeros((256, 128), BF)
            dst[rows, n * 256 : n * 256 + 128] = part
            mask = jnp.where(tile_lane < 64, 1.0 if n == 2 else 0.0, keep)
            dst[rows, n * 256 + 128 : (n + 1) * 256] = (right * mask + nn(aux, spots[n])).astype(BF)

    def augment_q(block, carry):
        rows = pl.ds(pl.multiple_of(block * 256, 256), 256)
        write_aug(q_aug, rows, r.qb[rows, :], aux_of(-r.lse[rows, :]), 1.0)
        return carry

    lax.fori_loop(0, 4, augment_q, 0)
    sum_row, sum_lane = (lax.broadcasted_iota(jnp.int32, (256, 128), axis) for axis in (0, 1))
    head_sums = jnp.where((lax.div(sum_row, 64) == sum_lane) & (sum_row < 192), 1.0, 0.0).astype(BF)
    r.woo[192:256, :] = jnp.zeros((64, D), BF)
    l_relay((1,))
    dy_pair(0)
    dy_pair(1)
    s_drain()
    d_drain()
    dv, dq, dk = (r.sall.at[:, part * 256 : (part + 1) * 256] for part in range(3))
    gm = r.dall.at[:, 0:256]
    l_wait(0)
    l_relay((2,))
    dz_fold(0)
    dy_pair(2)
    dy_pair(3)
    l_rest()
    gm[...] = nt(r.lall[...], r.woo[...]).astype(BF)

    out_grad = tn(r.lall[...], r.mix[...]).reshape(8, 96, 256)
    r.pou[:, 0:96, :] = out_grad[:, :, :128].astype(BF)
    third = out_grad[:, :, 128:].reshape(8, 2, 48, 128)
    moved = pltpu.roll(third[:, 1].reshape(384, 128), 64, 1).reshape(8, 48, 128)
    r.pou[:, 96:144, :] = (third[:, 0] + moved).astype(BF)
    ou_begin()

    def augment_g(block, carry):
        rows = pl.ds(pl.multiple_of(block * 256, 256), 256)
        grads = gm[rows, :]
        product = grads.astype(F32) * r.exact[rows, :]
        inner = jnp.zeros((256, 128), F32)
        for part in split_three(product):
            inner += nn(part.astype(BF), head_sums)
        write_aug(g_aug, rows, grads, aux_of(-inner), 0.0)
        return carry

    lax.fori_loop(0, 4, augment_g, 0)
    dz_fold(1)

    def k_copy(code):
        return push(r.ks_.at[code], r.kin.at[head], r.ks.at[code - 1], r.kr.at[code - 1], (dp, peer(code)))

    def v_copy(code):
        return push(r.vs_.at[code], r.vin.at[head], r.vs.at[code - 1], r.vr.at[code - 1], (dp, peer(code)))

    def q_copy(code):
        return push(r.qs_.at[code], r.qin.at[head], r.qs.at[code - 1], r.qr.at[code - 1], (dp, peer(code)))

    def attend_back(step, carry):
        code = 3 - step
        block = peer(code)
        rows = block_rows(block)
        value_grad = jnp.zeros((BLOCK, 256), F32)
        for n in range(3):
            mask = head_mask(n)
            lanes = slice(n * 256, (n + 1) * 256)
            probs = jnp.exp(nt(r.kb[rows, :], q_aug[:, lanes]))
            grad_scores = (probs * nt(r.vb[rows, :], g_aug[:, lanes])).astype(BF)
            r.big[pl.ds(pl.multiple_of(n * SLOT + block * BLOCK, 256), BLOCK), :] = grad_scores
            value_grad += nn(probs.astype(BF), g_aug[:, lanes]) * mask
        dv[rows, :] = value_grad.astype(BF)
        r.vs_[code] = packed(value_grad)

        @pl.when(step < 3)
        def _():
            v_copy(code).start()

        @pl.when(step == 2)
        def _():
            dz_pair()
            dy_fold(0)
            up_pair(0)
            up_pair(1)

        @pl.when(step == 3)
        def _():
            dy_fold(1)
            up_pair(2)

        return carry

    lax.fori_loop(0, 4, attend_back, 0)
    r.vin[head] = r.vs_[0]
    r.pqk[8:12] = tn(dv[...], r.nall[...])[:192].astype(BF).reshape(4, 48, D)
    qk_begin(range(8, 12))
    up_pair(3)

    def query_back(step, carry):
        code = 3 - step
        block = peer(code)
        rows = block_rows(block)
        query_grad = jnp.zeros((BLOCK, 256), F32)
        for n in range(3):
            part = r.big[n * SLOT : (n + 1) * SLOT, pl.ds(pl.multiple_of(block * BLOCK, 256), BLOCK)]
            query_grad += tn(part, r.kb[...] * head_mask(n).astype(BF))
        query_grad = query_grad * 0.125
        dq[rows, :] = query_grad.astype(BF)
        r.qs_[code] = packed(query_grad)

        @pl.when(step < 3)
        def _():
            q_copy(code).start()

        return carry

    lax.fori_loop(0, 4, query_back, 0)
    r.qin[head] = r.qs_[0]
    r.pqk[0:4] = tn(dq[...], r.nall[...])[:192].astype(BF).reshape(4, 48, D)
    qk_begin(range(4))
    up_pair(4)
    up_pair(5)

    def key_back(step, carry):
        code = 3 - step
        block = peer(code)
        rows = block_rows(block)
        key_grad = jnp.zeros((BLOCK, 256), F32)
        for n in range(3):
            part = r.big[pl.ds(pl.multiple_of(n * SLOT + block * BLOCK, 256), BLOCK), :]
            key_grad += nn(part, q_aug[:, n * 256 : (n + 1) * 256]) * head_mask(n)
        dk[rows, :] = key_grad.astype(BF)
        r.ks_[code] = packed(key_grad)

        @pl.when(step < 3)
        def _():
            k_copy(code).start()

        return carry

    lax.fori_loop(0, 4, key_back, 0)
    r.kin[head] = r.ks_[0]
    r.pqk[4:8] = tn(dk[...], r.nall[...])[:192].astype(BF).reshape(4, 48, D)
    qk_begin(range(4, 8))
    query_sum = jnp.sum(dq[...].astype(F32), axis=0, keepdims=True)
    value_sum = jnp.sum(dv[...].astype(F32), axis=0, keepdims=True)
    for group in range(4):
        mine = jnp.where(head == group, 1.0, 0.0)
        r.vec[4:5, group * 192 : (group + 1) * 192] = query_sum[:, :192] * mine
        r.vec[5:6, group * 192 : (group + 1) * 192] = value_sum[:, :192] * mine
    for shard in range(8):
        r.fsm[head, shard % 2, shard // 2, 0:8, 0:96] = r.vec[:, shard * 96 : (shard + 1) * 96]

    def small_y():
        return push(r.small.at[1 - y], r.ysm, r.ysms.at[0], r.ysmr.at[0], (other_y, head))

    def small_z(k):
        return push(
            r.small.at[y, z_shard(k)], r.zsm.at[k], r.zsms.at[k], r.zsmr.at[k], (z_shard(k) * 2 + y, head)
        )

    def small_f(code):
        return push(r.fsm.at[head], r.fsm.at[head], r.fsms.at[code - 1], r.fsmr.at[code - 1], (dp, peer(code)))

    for code in (2, 3, 1):
        start(lambda code=code: small_f(code))
    for t in range(4):
        ou_pair(t)
    for j in (0, 1, 2):
        up_fold(j)
    dy_total()
    dz_total()
    for j in range(8, 12):
        qk_pair(j)
    for j in (3, 4, 5):
        up_fold(j)
    for j in range(4):
        qk_pair(j)

    for code in (3, 2, 1):
        k_copy(code).wait_recv()
        v_copy(code).wait_recv()
        q_copy(code).wait_recv()
    unpack(r.qin, r.wuo, 0)
    unpack(r.kin, r.wuo, 256)
    unpack(r.vin, r.wuo, 512)
    grad_first = nt(r.wuo[0:256, :], r.wqkv[:, 0:D])
    grad_first += nt(r.wuo[256:512, :], r.wqkv[:, D : 2 * D])
    grad_first += nt(r.wuo[512:768, :], r.wqkv[:, 2 * D :])
    ou_fold(0)
    ou_fold(1)
    for code in (1, 2, 3):
        small_f(code).wait_recv()
    r.small[...] = r.fsm[0] + r.fsm[1] + r.fsm[2] + r.fsm[3]
    start(small_y)
    for j in range(8, 12):
        qk_fold(j)
    unit, inverse, _ = norm_parts(r.xv[...].astype(F32), gains[0:1, :], shifts[0:1, :])
    r.grad_inputs[...] = r.gh[...] + norm_back(grad_first, unit, inverse, gains[0:1, :])
    give("grad_inputs")
    pair = jnp.concatenate(
        [jnp.sum(grad_first * unit, axis=0, keepdims=True), jnp.sum(grad_first, axis=0, keepdims=True)], axis=0
    )
    r.last[head] = jnp.zeros((16, 128), F32)
    for shard in range(8):
        at = shard % 2 * 8 + shard // 2 * 2
        r.last[head, at : at + 2, 0:96] = pair[:, shard * 96 : (shard + 1) * 96]

    def last_head(code):
        return push(r.last.at[head], r.last.at[head], r.las.at[code - 1], r.lar.at[code - 1], (dp, peer(code)))

    def last_y():
        return push(r.lasty.at[1 - y], r.lastz.at[4], r.lays.at[0], r.layr.at[0], (other_y, head))

    def last_z(k):
        return push(r.lastz.at[0], r.lastz.at[k], r.lazs.at[k], r.lazr.at[k], (z_shard(k) * 2 + y, head))

    for code in (2, 3, 1):
        start(lambda code=code: last_head(code))
    for j in range(4, 8):
        qk_pair(j)
    up_total()
    for j in range(4):
        qk_fold(j)
    small_y().wait_recv()
    r.small[y] = r.small[y] + r.ysm[...]
    for k in (1, 2, 3):
        start(lambda k=k: small_z(k))
    for code in (1, 2, 3):
        last_head(code).wait_recv()
    over_head = r.last[0] + r.last[1] + r.last[2] + r.last[3]
    r.lasty[0] = over_head[0:8]
    r.lasty[1] = over_head[8:16]
    start(last_y)
    dy_relay()
    dz_relay()
    ou_total()
    qk_total(range(8, 12))
    for j in range(4, 8):
        qk_fold(j)
    last_y().wait_recv()
    r.lastz[0] = r.lasty[y] + r.lastz[4]
    for k in (1, 2, 3):
        start(lambda k=k: last_z(k))
    qk_total(range(4))
    up_relay()
    ou_relay()
    qk_total(range(4, 8))
    for k in (1, 2, 3):
        last_z(k).wait_recv()
    dy_rest()
    give("fdy")
    dz_rest()
    give("fdz")
    qk_relay()
    up_rest()
    give("fup")
    ou_rest()
    give("fou")
    qk_rest()
    give("fqk")
    for k in (1, 2, 3):
        small_z(k).wait_recv()
    r.fsum[...] = r.small[y, z] + r.zsm[1] + r.zsm[2] + r.zsm[3]
    r.lastf[...] = r.lastz[0] + r.lastz[1] + r.lastz[2] + r.lastz[3]
    r.fsum[0:1, :] = r.lastf[pl.ds(2 * z, 1), :]
    r.fsum[2:3, :] = r.lastf[pl.ds(2 * z + 1, 1), :]
    give("fsum")
    n_drain()
    l_drain()
    for make, cond in sent:
        when(cond, lambda make=make: make().wait_send())
    for code in (1, 2, 3):
        mix_copy(code).wait_send()
        k_copy(code).wait_send()
        v_copy(code).wait_send()
        q_copy(code).wait_send()
    for copy in given:
        copy.wait()


def emit_kernel(
    block_in, inputs_in, fup, fqk, fdy, fdz, fou, fsum,
    block_out, grad_inputs, gains, shifts, qkv, qv_bias, out, out_biases, up, up_bias, down,
    block_v, inputs_v, fup_v, fqk_v, fdy_v, fdz_v, fou_v, fsum_v, up_v, qkv_v, down_v, out_v, sems,
):
    count = []

    def begin(src, dst):
        count.append(pltpu.make_async_copy(src, dst, sems.at[len(count)]))
        count[-1].start()
        return count[-1]

    pairs = (
        (fdy, fdy_v), (fdz, fdz_v), (fup, fup_v), (inputs_in, inputs_v), (block_in, block_v), (fqk, fqk_v), (fou, fou_v),
        (fsum, fsum_v),
    )
    arrivals = [begin(src, dst) for src, dst in pairs]
    results = []
    arrivals[0].wait()
    arrivals[1].wait()
    for group in range(4):
        for j in range(6):
            place = (4 * j + group) * 128
            source, at = (fdy_v, j * 128) if j < 2 else (fdz_v, j * 128 - 256)
            down_v[:, place : place + 128] = source[group, :, at : at + 128].astype(F32)
    results.append(begin(down_v, down))
    arrivals[2].wait()
    for i in range(3):
        up_v[:, i * 128 : (i + 1) * 128] = fup_v[i].astype(F32)
    results.append(begin(up_v, up))
    for arrival, src, dst in ((3, inputs_v, grad_inputs), (4, block_v, block_out)):
        arrivals[arrival].wait()
        results.append(begin(src, dst))
    arrivals[5].wait()
    qkv_v[...] = fqk_v[...].reshape(288, D).astype(F32)
    results.append(begin(qkv_v, qkv))
    arrivals[6].wait()
    for group in range(4):
        piece, lane = fou_v[group].astype(F32), group * 192
        out_v[:, lane : lane + 128] = piece[0:96]
        out_v[0:48, lane + 128 : lane + 192] = piece[96:144, 0:64]
        out_v[48:96, lane + 128 : lane + 192] = piece[96:144, 64:128]
    results.append(begin(out_v, out))
    arrivals[7].wait()
    for index, ref in enumerate((gains, shifts, qv_bias, out_biases)):
        ref[...] = fsum_v[2 * index : 2 * index + 2, 0:96]
    up_bias[...] = fsum_v[8:11, :]
    for copy in results:
        copy.wait()


def per_device(x, norm_gains, norm_shifts, w_qkv, qv_bias, w_out, out_biases, w_up, up_bias, w_down, lengths, d_out):
    values = dict(
        x=x[0], gains=norm_gains, shifts=norm_shifts, w_qkv=w_qkv, qv_bias=qv_bias, w_out=w_out, biases=out_biases,
        w_up=w_up, up_bias=up_bias.reshape(24, 128), w_down=w_down, lengths=lengths, d_out=d_out[0],
    )
    place = {True: pl.BlockSpec(memory_space=pl.ANY), False: pl.BlockSpec(memory_space=pltpu.VMEM)}
    block_out, grad_inputs, fup, fqk, fdy, fdz, fou, fsum = pl.pallas_call(
        one_kernel,
        out_shape=[jax.ShapeDtypeStruct(shape, kind) for _, shape, kind in OUTPUTS],
        in_specs=[place[name in IN_PLACE] for name in INPUTS],
        out_specs=[place[True]] * len(OUTPUTS),
        scratch_shapes=[pltpu.VMEM(shape, kind) for _, shape, kind in OUTPUTS + BUFFERS]
        + [pltpu.SemaphoreType.DMA((count,)) for _, count in SEMAPHORES],
        compiler_params=pltpu.CompilerParams(
            collective_id=0, has_side_effects=True, vmem_limit_bytes=VMEM_LIMIT
        ),
        name="block",
    )(*(values[name] for name in INPUTS))
    anywhere = pl.BlockSpec(memory_space=pl.ANY)
    shapes = [(256, D), (256, D), (2, 96), (2, 96), (288, D), (2, 96), (96, D), (2, 96), (D, 384), (3, 128), (96, FF)]
    outs = pl.pallas_call(
        emit_kernel,
        out_shape=[jax.ShapeDtypeStruct(shape, F32 if n else BF) for n, shape in enumerate(shapes)],
        in_specs=[anywhere] * 8,
        out_specs=[anywhere] * 2 + [anywhere if shape[0] > 16 else place[False] for shape in shapes[2:]],
        scratch_shapes=[pltpu.VMEM(shape, kind) for _, shape, kind in OUTPUTS]
        + [pltpu.VMEM(shape, F32) for shape in ((D, 384), (288, D), (96, FF), (96, D))]
        + [pltpu.SemaphoreType.DMA((14,))],
        compiler_params=pltpu.CompilerParams(vmem_limit_bytes=VMEM_LIMIT),
        name="emit",
    )(block_out, grad_inputs, fup, fqk, fdy, fdz, fou, fsum)
    return (
        outs[0][None], outs[1][None], outs[2], outs[3], outs[4].T, outs[5], outs[6].T, outs[7], outs[8],
        outs[9].reshape(384), outs[10].T,
    )


def solution(mesh):
    split = P("dp", "head", None)
    placed = (split,) + (P(),) * 9 + (P("dp", None), split)
    return jax.shard_map(
        per_device if dict(mesh.shape) == {"dp": 8, "head": 4} else general_device,
        mesh=mesh,
        in_specs=placed,
        out_specs=(split, split) + (P(None, "dp"),) * 7 + (P("dp"), P(None, "dp")),
        check_vma=False,
    )
```

```python
import functools

import jax
import jax.numpy as jnp
from jax import lax
from jax.experimental import pallas as pl
from jax.experimental.pallas import tpu as pltpu
from jax.sharding import PartitionSpec as P

D = 768
HEADS = 12
HDIM = 64
FF = 3072
SLOT = 1024
EPSILON = 1e-06
BF = jnp.bfloat16
F32 = jnp.float32
FAR = -1e30
VMEM_LIMIT = 63 * 1024 * 1024


def nn(a, b):
    return lax.dot_general(a, b, (((1,), (0,)), ((), ())), preferred_element_type=F32)


def nt(a, b):
    return lax.dot_general(a, b, (((1,), (1,)), ((), ())), preferred_element_type=F32)


def tn(a, b):
    return lax.dot_general(a, b, (((0,), (0,)), ((), ())), preferred_element_type=F32)


def norm_parts(values, norm_gain, norm_shift):
    average = jnp.mean(values, axis=-1, keepdims=True)
    centered = values - average
    variance = jnp.mean(centered * centered, axis=-1, keepdims=True)
    inverse = lax.rsqrt(variance + EPSILON)
    unit = centered * inverse
    return unit, inverse, unit * norm_gain + norm_shift


def norm_back(grad_normed, unit, inverse, norm_gain):
    grad_unit = grad_normed * norm_gain
    first_mean = jnp.mean(grad_unit, axis=-1, keepdims=True)
    second_mean = jnp.mean(grad_unit * unit, axis=-1, keepdims=True)
    return inverse * (grad_unit - first_mean - unit * second_mean)


def gelu_parts(values):
    cumulative = 0.5 + 0.5 * lax.erf(values * 0.7071067811865476)
    density = jnp.exp(values * values * -0.5) * 0.3989422804014327
    return values * cumulative, cumulative + values * density


def lanes_of(width=256):
    return lax.broadcasted_iota(jnp.int32, (1, width), 1)


def head_mask(head):
    lane = lanes_of()
    return jnp.where((lane >= head * HDIM) & (lane < (head + 1) * HDIM), 1.0, 0.0)


def lane_is(index):
    return jnp.where(lanes_of() == index, 1.0, 0.0)


def split_three(column):
    high = column.astype(BF).astype(F32)
    rest = column - high
    middle = rest.astype(BF).astype(F32)
    return high, middle, rest - middle


def attend_forward(normed, weight, bias, lengths, q_ref, k_ref, v_ref, mixed_ref, exact_ref, lse_ref):
    whole = lengths[:, 0:1] == SLOT
    total = jnp.sum(lengths, axis=1, keepdims=True)
    onlane = lanes_of()
    aux_k = jnp.where((onlane >= 196) & (onlane < 199), 1.0, 0.0)
    aux_v = jnp.where((onlane >= 192) & (onlane < 199) & (onlane != 195), 1.0, 0.0)
    for block in range(4):
        rows = pl.ds(block * 256, 256)
        projected = nn(normed[rows, :], weight[...]) + bias
        projected = projected.astype(BF).astype(F32)
        q_ref[rows, :] = (projected[:, :256] * 0.125 + lane_is(192 + block)).astype(BF)
        other = jnp.where((onlane >= 192) & (onlane < 196) & (onlane != 192 + block), 1.0, 0.0)
        far = other * jnp.where(whole, 0.0, FAR)
        k_ref[rows, :] = (projected[:, 256:512] + (aux_k + far)).astype(BF)
        v_ref[rows, :] = (projected[:, 512:] + aux_v).astype(BF)
    on_aux = jnp.where(onlane >= 192, 1.0, 0.0)

    def block_step(block, carry):
        rows = pl.ds(pl.multiple_of(block * 256, 256), 256)
        queries = q_ref[rows, :]
        mixed = jnp.zeros((256, 256), F32)
        tops = []
        for head in range(3):
            scores = nt(queries * (head_mask(head) + on_aux).astype(BF), k_ref[...])
            top = jnp.max(scores, axis=1, keepdims=True)
            weights = jnp.exp(scores - top).astype(BF)
            mixed += nn(weights, v_ref[...] * (head_mask(head) + lane_is(192 + head)).astype(BF))
            tops.append(top)
        lse = jnp.zeros((256, 128), F32)
        scale = jnp.zeros((256, 256), F32)
        small = lax.broadcasted_iota(jnp.int32, (1, 128), 1)
        for head in range(3):
            row_sum = jnp.sum(mixed * lane_is(192 + head), axis=1, keepdims=True)
            lse += (tops[head] + jnp.log(row_sum)) * jnp.where(small == head, 1.0, 0.0)
            scale += (1.0 / row_sum) * head_mask(head)
        mixed = mixed * scale
        position = block * 256 + lax.broadcasted_iota(jnp.int32, (256, 1), 0)
        on_heads = jnp.where(onlane < 192, 1.0, 0.0)
        mixed = jnp.where(position < total, mixed, v_ref[rows, :].astype(F32) * on_heads)
        exact_ref[rows, :] = mixed
        mixed_ref[rows, :] = mixed[:, :192].astype(BF)
        lse_ref[rows, :] = lse
        return carry

    lax.fori_loop(0, 4, block_step, 0)


def attend_backward(q_ref, k_ref, v_ref, exact_ref, lse_ref, grad_mixed, q_aug, g_aug, scores_low, dq_acc, dk_acc, dv_acc):
    for head in range(3):
        mask = head_mask(head)

        def augment(block, carry):
            rows = pl.ds(pl.multiple_of(block * 256, 256), 256)
            grads = grad_mixed[rows, :].astype(F32) * mask
            inner = jnp.sum(grads * exact_ref[rows, :], axis=1, keepdims=True)
            lse = lse_ref[rows, :][:, head : head + 1]
            queries = q_ref[rows, :].astype(F32) * (mask + jnp.where(lanes_of() >= 192, 1.0, 0.0))
            for place, part in enumerate(split_three(-lse)):
                queries = queries + part * lane_is(196 + place)
            for place, part in enumerate(split_three(-inner)):
                grads = grads + part * lane_is(196 + place)
            q_aug[rows, :] = queries.astype(BF)
            g_aug[rows, :] = grads.astype(BF)
            return carry

        lax.fori_loop(0, 4, augment, 0)

        def block_step(block, carry):
            rows = pl.ds(pl.multiple_of(block * 256, 256), 256)
            probs = jnp.exp(nt(k_ref[rows, :], q_aug[...]))
            grad_probs = nt(v_ref[rows, :], g_aug[...])
            grad_scores = (probs * grad_probs).astype(BF)
            scores_low[rows, :] = grad_scores
            key_part = nn(grad_scores, q_aug[...]) * mask
            value_part = nn(probs.astype(BF), g_aug[...]) * mask
            if head == 0:
                dk_acc[rows, :] = key_part
                dv_acc[rows, :] = value_part
            else:
                dk_acc[rows, :] += key_part
                dv_acc[rows, :] += value_part
            return carry

        lax.fori_loop(0, 4, block_step, 0)
        query_part = tn(scores_low[...], k_ref[...] * mask.astype(BF)) * 0.125
        if head == 0:
            dq_acc[...] = query_part
        else:
            dq_acc[...] += query_part


def forward_kernel(normed, weight, bias, lengths, q_ref, k_ref, v_ref, mixed_ref, exact_ref, lse_ref):
    attend_forward(normed, weight, bias[...], lengths[...], q_ref, k_ref, v_ref, mixed_ref, exact_ref, lse_ref)


def middle_kernel(
    mixed_in, x_in, d_low, w_out, w_up, w_down, gains, shifts, biases, up_bias,
    block_ref, second_ref, hid_ref, low_ref, sums_ref, mixed_rows, act_ref,
):
    rows = x_in.shape[0]
    for group in range(4):
        mixed_rows[:, group * 192 : (group + 1) * 192] = mixed_in[group]
    hidden = x_in[...].astype(F32) + nn(mixed_rows[...], w_out[...]) + biases[0:1, :]
    unit, inverse, normed = norm_parts(hidden, gains[1:2, :], shifts[1:2, :])
    second = normed.astype(BF)
    second_ref[...] = second
    grad_low = d_low[...]
    down = jnp.zeros((rows, D), F32)
    back = jnp.zeros((rows, D), F32)
    step = 768
    for tile in range(FF // step):
        cut = slice(tile * step, (tile + 1) * step)
        up = nn(second, w_up[:, cut]) + up_bias[:, cut]
        value, slope = gelu_parts(up)
        down += nn(value.astype(BF), w_down[cut, :])
        grad_up = nt(grad_low, w_down[cut, :]) * slope
        back += nt(grad_up.astype(BF), w_up[:, cut])
    block_ref[...] = (hidden + down + biases[1:2, :]).astype(BF)
    grad_block = grad_low.astype(F32)
    grad_hidden = grad_block + norm_back(back, unit, inverse, gains[1:2, :])
    hid_ref[...] = grad_hidden
    low_ref[...] = grad_hidden.astype(BF)
    sums_ref[...] = jnp.zeros_like(sums_ref)
    sums_ref[0:1, :] = jnp.sum(back * unit, axis=0, keepdims=True)
    sums_ref[1:2, :] = jnp.sum(back, axis=0, keepdims=True)
    sums_ref[2:3, :] = jnp.sum(grad_hidden, axis=0, keepdims=True)
    sums_ref[3:4, :] = jnp.sum(grad_block, axis=0, keepdims=True)


def feed_kernel(second, d_low, w_up, w_down, up_bias, up_grad, down_grad, bias_grad, act_ref, grad_ref):
    width = w_up.shape[1]
    bias_grad[...] = jnp.zeros_like(bias_grad)

    def step(block, carry):
        rows = pl.ds(pl.multiple_of(block * 256, 256), 256)
        up = nn(second[rows, :], w_up[...]) + up_bias[...]
        value, slope = gelu_parts(up)
        act_ref[rows, :] = value.astype(BF)
        grad_up = nt(d_low[rows, :], w_down[...]) * slope
        bias_grad[0:1, :] += jnp.sum(grad_up, axis=0, keepdims=True)
        grad_ref[rows, :] = grad_up.astype(BF)
        return carry

    lax.fori_loop(0, 4, step, 0)
    down_grad[...] = tn(d_low[...], act_ref[...]).astype(BF)
    up_grad[...] = tn(grad_ref[...], second[...]).astype(BF)


def backward_kernel(
    grad_low, w_out, normed, mixed, q_ref, k_ref, v_ref, exact_ref, lse_ref,
    grad_ref, out_grad, qkv_grad, bias_grad,
    grad_mixed, q_aug, g_aug, scores_low, dq_acc, dk_acc, dv_acc,
):
    padded = jnp.zeros((64, D), BF)
    weight = jnp.concatenate([w_out[...], padded], axis=0)
    grad_mixed[...] = nt(grad_low[...], weight).astype(BF)
    out_grad[...] = tn(grad_low[...], mixed[...]).astype(BF)
    attend_backward(q_ref, k_ref, v_ref, exact_ref, lse_ref, grad_mixed, q_aug, g_aug, scores_low, dq_acc, dk_acc, dv_acc)
    for place, part in enumerate((dq_acc, dk_acc, dv_acc)):
        grad_ref[:, place * 192 : (place + 1) * 192] = part[:, :192].astype(BF)
    bias_grad[...] = jnp.zeros_like(bias_grad)
    bias_grad[0:1, :] = jnp.sum(grad_ref[...].astype(F32), axis=0, keepdims=True)
    qkv_grad[...] = tn(grad_ref[...], normed[...]).astype(BF)


def last_kernel(grad_in, w_qkv, x_in, hid, gains, shifts, out_ref, sums_ref, grad_rows):
    for part in range(3):
        for group in range(4):
            place = part * D + group * 192
            grad_rows[:, place : place + 192] = grad_in[group][:, part * 192 : (part + 1) * 192]
    grad_first = nt(grad_rows[...], w_qkv[...])
    unit, inverse, _ = norm_parts(x_in[...].astype(F32), gains[0:1, :], shifts[0:1, :])
    out_ref[...] = hid[...] + norm_back(grad_first, unit, inverse, gains[0:1, :])
    sums_ref[...] = jnp.zeros_like(sums_ref)
    sums_ref[0:1, :] = jnp.sum(grad_first * unit, axis=0, keepdims=True)
    sums_ref[1:2, :] = jnp.sum(grad_first, axis=0, keepdims=True)


def whole_call(kernel, outs, scratch=(), name=None):
    return pl.pallas_call(
        kernel,
        out_shape=[jax.ShapeDtypeStruct(*out) for out in outs],
        scratch_shapes=[pltpu.VMEM(*item) for item in scratch],
        compiler_params=pltpu.CompilerParams(vmem_limit_bytes=VMEM_LIMIT),
        name=name,
    )


def general_device(x, norm_gains, norm_shifts, w_qkv, qv_bias, w_out, out_biases, w_up, up_bias, w_down, lengths, d_out):
    groups = lax.axis_size("head")
    shards = lax.axis_size("dp")
    group = lax.axis_index("head")
    rows = x.shape[1]
    own = D // groups
    x = x[0]
    gains = norm_gains.astype(F32)
    shifts = norm_shifts.astype(F32)
    biases = out_biases.astype(F32)
    up_shift = up_bias.astype(F32)
    full_bias = jnp.stack([qv_bias[0], jnp.zeros_like(qv_bias[0]), qv_bias[1]]).astype(F32)

    weight_own = lax.dynamic_index_in_dim(w_qkv.reshape(D, 3, groups, own), group, 2, False)
    weight_own = jnp.pad(weight_own, ((0, 0), (0, 0), (0, 256 - own))).reshape(D, 768)
    bias_own = lax.dynamic_index_in_dim(full_bias.reshape(3, groups, own), group, 1, False)
    bias_own = jnp.pad(bias_own, ((0, 0), (0, 256 - own))).reshape(1, 768)
    out_own = lax.dynamic_slice_in_dim(w_out, group * own, own, 0)
    unit_ff = FF // (shards * groups)
    up_own = lax.dynamic_index_in_dim(w_up.reshape(D, shards, groups, unit_ff), group, 2, False).reshape(D, D)
    down_own = lax.dynamic_index_in_dim(w_down.reshape(shards, groups, unit_ff, D), group, 1, False).reshape(D, D)
    ub_own = lax.dynamic_index_in_dim(up_shift.reshape(shards, groups, unit_ff), group, 1, False).reshape(1, D)

    normed = norm_parts(x.astype(F32), gains[0], shifts[0])[2].astype(BF)
    normed_all = lax.all_gather(normed, "head", axis=0, tiled=True)
    total = jnp.sum(lengths[0])
    position = group * rows + jnp.arange(rows, dtype=jnp.int32)
    d_low = jnp.where((position < total)[:, None], d_out[0], jnp.zeros_like(d_out[0]))
    d_all = lax.all_gather(d_low, "head", axis=0, tiled=True)

    q, k, v, mixed, exact, lse = whole_call(
        forward_kernel,
        [((SLOT, 256), BF)] * 3 + [((SLOT, own), BF), ((SLOT, 256), F32), ((SLOT, 128), F32)],
        name="attend_forward",
    )(normed_all, weight_own, bias_own, lengths)
    mixed_in = lax.all_to_all(mixed.reshape(groups, rows, own), "head", 0, 0, tiled=True)
    block_out, second, hid, hid_low, sums_mid = whole_call(
        middle_kernel,
        [((rows, D), BF), ((rows, D), BF), ((rows, D), F32), ((rows, D), BF), ((8, D), F32)],
        [((rows, D), BF), ((rows, FF), BF)],
        name="middle",
    )(mixed_in, x, d_low, w_out, w_up, w_down, gains, shifts, biases, up_shift.reshape(1, FF))
    second_all = lax.all_gather(second, "head", axis=0, tiled=True)
    low_all = lax.all_gather(hid_low, "head", axis=0, tiled=True)
    up_grad, down_grad, ub_grad = whole_call(
        feed_kernel,
        [((D, D), BF), ((D, D), BF), ((8, D), F32)],
        [((SLOT, D), BF), ((SLOT, D), BF)],
        name="feed",
    )(second_all, d_all, up_own, down_own, ub_own)
    grad_own, out_grad, qkv_grad, qkv_sum = whole_call(
        backward_kernel,
        [((SLOT, 3 * own), BF), ((D, own), BF), ((3 * own, D), BF), ((8, 3 * own), F32)],
        [((SLOT, 256), BF)] * 3 + [((SLOT, SLOT), BF)] + [((SLOT, 256), F32)] * 3,
        name="attend_backward",
    )(low_all, out_own, normed_all, mixed, q, k, v, exact, lse)
    grad_in = lax.all_to_all(grad_own.reshape(groups, rows, 3 * own), "head", 0, 0, tiled=True)
    grad_inputs, sums_last = whole_call(
        last_kernel,
        [((rows, D), F32), ((8, D), F32)],
        [((rows, 3 * D), BF)],
        name="last",
    )(grad_in, w_qkv, x, hid, gains, shifts)

    def scatter(values):
        return lax.psum_scatter(values, "dp", scatter_dimension=0, tiled=True)

    up_part = lax.all_gather(scatter(up_grad), "head", axis=0, tiled=True)
    down_part = lax.all_gather(scatter(down_grad), "head", axis=1, tiled=True)
    out_part = lax.all_gather(scatter(out_grad), "head", axis=1, tiled=True)
    down_out = down_part.astype(F32).T.reshape(groups, shards, unit_ff, D // shards)
    down_out = down_out.transpose(1, 0, 2, 3).reshape(FF, D // shards)
    spread = jnp.zeros((3, groups, own, D), BF)
    spread = lax.dynamic_update_slice(spread, qkv_grad.reshape(3, 1, own, D), (0, group, 0, 0))
    qkv_part = lax.psum(scatter(spread.reshape(3 * D, D)), "head")

    def place_rows(values):
        parts = values.reshape(3, own)
        empty = jnp.zeros((3, groups, own), F32)
        return lax.dynamic_update_slice(empty, parts[:, None], (0, group, 0)).reshape(3, D)

    bias_rows = place_rows(qkv_sum[0])
    ub_rows = lax.dynamic_update_slice(
        jnp.zeros((shards, groups, unit_ff), F32), ub_grad[0].reshape(shards, 1, unit_ff), (0, group, 0)
    ).reshape(4, D)
    small = jnp.concatenate([sums_last[0:2], sums_mid[0:4], bias_rows[0:1], bias_rows[2:3], ub_rows], axis=0)
    small = lax.psum(small, ("dp", "head"))
    shard = lax.axis_index("dp")

    def cut(values):
        width = D // shards
        return lax.dynamic_slice_in_dim(values, shard * width, width, 1)

    ub_out = lax.dynamic_slice_in_dim(small[8:12].reshape(FF), shard * (FF // shards), FF // shards, 0)
    return (
        block_out[None],
        grad_inputs[None],
        cut(jnp.stack([small[0], small[2]])),
        cut(jnp.stack([small[1], small[3]])),
        qkv_part.astype(F32).T,
        cut(small[6:8]),
        out_part.astype(F32).T,
        cut(small[4:6]),
        up_part.astype(F32).T,
        ub_out,
        down_out,
    )


MESH = pl.DeviceIdType.MESH
BLOCK = 256

BUFFERS = (
    ("xv", (256, D), BF),
    ("dv", (256, D), BF),
    ("wqkv", (D, 3 * D), BF),
    ("wout", (D, D), BF),
    ("wup", (D, FF), BF),
    ("big", (3 * SLOT, SLOT), BF),
    ("wqo", (D, D), BF),
    ("wuo", (D, D), BF),
    ("wdo", (D, D), BF),
    ("woo", (256, D), BF),
    ("nall", (SLOT, D), BF),
    ("dall", (SLOT, D), BF),
    ("sall", (SLOT, D), BF),
    ("lall", (SLOT, D), BF),
    ("qb", (SLOT, 256), BF),
    ("kb", (SLOT, 256), BF),
    ("vb", (SLOT, 256), BF),
    ("mix", (SLOT, 256), BF),
    ("exact", (SLOT, 256), F32),
    ("lse", (SLOT, 128), F32),
    ("mixs", (4, 384, 128), BF),
    ("mixin", (4, 384, 128), BF),
    ("gh", (256, D), F32),
    ("act", (SLOT, D), BF),
    ("gup", (SLOT, D), BF),
    ("kin", (4, 384, 128), BF),
    ("vin", (4, 384, 128), BF),
    ("ks_", (4, 384, 128), BF),
    ("vs_", (4, 384, 128), BF),
    ("qs_", (4, 384, 128), BF),
    ("qin", (4, 384, 128), BF),
    ("pdy", (8, 96, 256), BF),
    ("pdz", (8, 96, 512), BF),
    ("pup", (6, D, 128), BF),
    ("pou", (8, 144, 128), BF),
    ("pqk", (12, 48, D), BF),
    ("ydy", (4, 96, 256), BF),
    ("ydz", (1, 96, 512), BF),
    ("yup", (6, D, 128), BF),
    ("you", (4, 144, 128), BF),
    ("yqk", (12, 48, D), BF),
    ("zdy", (4, 96, 256), BF),
    ("zdz", (4, 2, 96, 512), BF),
    ("zup", (12, D, 128), BF),
    ("zou", (4, 144, 128), BF),
    ("zqk", (24, 48, D), BF),
    ("vec", (8, D), F32),
    ("bias_rows", (24, 128), F32),
    ("small", (2, 4, 16, 128), F32),
    ("ysm", (4, 16, 128), F32),
    ("zsm", (4, 16, 128), F32),
    ("fsm", (4, 2, 4, 16, 128), F32),
    ("last", (4, 16, 128), F32),
    ("lasty", (2, 8, 128), F32),
    ("lastz", (5, 8, 128), F32),
    ("lastf", (8, 128), F32),
)
SEMAPHORES = (
    ("load", 22), ("give", 8),
    ("ns", 5), ("nr", 5), ("ds", 5), ("dr", 5), ("ss", 5), ("sr", 5), ("ls", 5), ("lr", 5),
    ("ms", 3), ("mr", 3), ("ks", 3), ("kr", 3), ("vs", 3), ("vr", 3), ("qs", 3), ("qr", 3),
    ("ydys", 4), ("ydyr", 4), ("zdys", 4), ("zdyr", 4), ("fdys", 3), ("fdyr", 3),
    ("ydzs", 1), ("ydzr", 1), ("zdzs", 4), ("zdzr", 4), ("fdzs", 3), ("fdzr", 3),
    ("yous", 4), ("your", 4), ("zous", 4), ("zour", 4), ("fous", 3), ("four", 3),
    ("yups", 6), ("yupr", 6), ("zups", 6), ("zupr", 12), ("fups", 9), ("fupr", 9),
    ("yqks", 12), ("yqkr", 12), ("zqks", 12), ("zqkr", 24), ("fqks", 18), ("fqkr", 18),
    ("ysms", 1), ("ysmr", 1), ("zsms", 4), ("zsmr", 4), ("fsms", 3), ("fsmr", 3),
    ("las", 3), ("lar", 3), ("lays", 1), ("layr", 1), ("lazs", 4), ("lazr", 4),
)
INPUTS = ("x", "gains", "shifts", "w_qkv", "qv_bias", "w_out", "biases", "w_up", "up_bias", "w_down", "lengths", "d_out")
IN_PLACE = ("x", "w_qkv", "w_out", "w_up", "w_down", "d_out")
OUTPUTS = (
    ("block_out", (256, D), BF),
    ("grad_inputs", (256, D), F32),
    ("fup", (3, D, 128), BF),
    ("fqk", (6, 48, D), BF),
    ("fdy", (4, 96, 256), BF),
    ("fdz", (4, 96, 512), BF),
    ("fou", (4, 144, 128), BF),
    ("fsum", (16, 128), F32),
)


class Refs:
    pass


def block_rows(block, size=BLOCK, offset=0):
    return pl.ds(pl.multiple_of(block * BLOCK + offset, 128), size)


def one_kernel(*args):
    r = Refs()
    names = [*INPUTS] + ["to_" + o[0] for o in OUTPUTS] + [b[0] for b in OUTPUTS + BUFFERS] + [s[0] for s in SEMAPHORES]
    for name, ref in zip(names, args, strict=True):
        setattr(r, name, ref)
    dp, head = lax.axis_index("dp"), lax.axis_index("head")
    z, y = lax.div(dp, 2), lax.rem(dp, 2)
    px, pc = lax.div(head, 2), lax.rem(head, 2)

    def peer(code):
        return lax.rem(px + (code // 2 if isinstance(code, int) else lax.div(code, 2)), 2) * 2 + lax.rem(
            pc + (code % 2 if isinstance(code, int) else lax.rem(code, 2)), 2
        )

    sib, far, diag = peer(1), peer(2), peer(3)
    other_y = z * 2 + (1 - y)

    def z_shard(k):
        return lax.rem(z + k, 4)

    half = lax.div(z, 2)
    inner = (z == 1) | (z == 2)
    outer = (z == 0) | (z == 3)
    beside = half * 2 + 1 - lax.rem(z, 2)
    z_order = (3 * (1 - half), 2 - half, beside, z)

    sent = []

    def push(src, dst, send, recv, to):
        return pltpu.make_async_remote_copy(
            src_ref=src, dst_ref=dst, send_sem=send, recv_sem=recv, device_id=to, device_id_type=MESH
        )

    def when(cond, body):
        if cond is None:
            body()
        else:
            pl.when(cond)(body)

    given = []

    def give(name):
        copy = pltpu.make_async_copy(getattr(r, name), getattr(r, "to_" + name), r.give.at[len(given)])
        copy.start()
        given.append(copy)

    def start(make, cond=None):
        when(cond, lambda: make().start())
        sent.append((make, cond))

    loads = {}

    def load(name, src, dst):
        loads.setdefault(name, []).append(pltpu.make_async_copy(src, dst, r.load.at[sum(map(len, loads.values()))]))

    load("x", r.x, r.xv)
    load("d", r.d_out, r.dv)
    load("wqkv", r.w_qkv, r.wqkv)
    load("wout", r.w_out, r.wout)
    load("wup", r.w_up, r.wup)
    load("wdown", r.w_down, r.big.at[:, 0:D])
    load("woo", r.w_out.at[pl.ds(pl.multiple_of(head * 192, 64), 192), :], r.woo.at[0:192, :])
    for j in range(6):
        unit = pl.ds(pl.multiple_of((4 * j + head) * 128, 128), 128)
        load("wuo", r.w_up.at[:, unit], r.wuo.at[:, j * 128 : (j + 1) * 128])
        load("wdo", r.w_down.at[unit, :], r.wdo.at[j * 128 : (j + 1) * 128, :])
    for copies in loads.values():
        for copy in copies:
            copy.start()

    def loaded(name):
        for copy in loads[name]:
            copy.wait()

    barrier = pltpu.get_barrier_semaphore()
    for to in [(dp, sib), (dp, far), (dp, diag), (other_y, head)] + [(z_shard(k) * 2 + y, head) for k in (1, 2, 3)]:
        pl.semaphore_signal(barrier, inc=1, device_id=to, device_id_type=MESH)

    gains = r.gains[...].astype(F32)
    shifts = r.shifts[...].astype(F32)
    biases = r.biases[...].astype(F32)
    onlane = lanes_of()
    lengths = r.lengths[...]
    whole = lengths[:, 0:1] == SLOT
    total = jnp.sum(lengths, axis=1, keepdims=True)

    def piece_rows(block, offset, size):
        return pl.ds(pl.multiple_of(block * BLOCK + offset, 32), size)

    def gather(buf, send, recv, cut=128):
        pieces = ((0, cut), (cut, BLOCK - cut))

        def copy_of(index):
            if index == 0:
                rows, to = block_rows(head), sib
            elif index < 3:
                rows, to = piece_rows(head, *pieces[index - 1]), far
            else:
                rows, to = piece_rows(far, *pieces[index - 3]), sib
            return push(buf.at[rows, :], buf.at[rows, :], send.at[index], recv.at[index], (dp, to))

        def begin(these=(1, 2, 0)):
            for index in these:
                copy_of(index).start()

        def wait(index):
            copy_of(index).wait_recv()

        def relay(these=(1, 2)):
            for index in these:
                wait(index)
                copy_of(index + 2).start()

        def rest():
            for index in (3, 4):
                wait(index)

        def drain():
            for index in range(5):
                copy_of(index).wait_send()

        return begin, wait, relay, rest, drain

    n_begin, n_wait, n_relay, n_rest, n_drain = gather(r.nall, r.ns, r.nr)
    d_begin, d_wait, d_relay, d_rest, d_drain = gather(r.dall, r.ds, r.dr, 160)
    s_begin, s_wait, s_relay, s_rest, s_drain = gather(r.sall, r.ss, r.sr)
    l_begin, l_wait, l_relay, l_rest, l_drain = gather(r.lall, r.ls, r.lr)

    loaded("x")
    first = norm_parts(r.xv[...].astype(F32), gains[0:1, :], shifts[0:1, :])[2]
    r.nall[block_rows(head), :] = first.astype(BF)
    pl.semaphore_wait(barrier, 7)
    n_begin()
    position = head * BLOCK + lax.broadcasted_iota(jnp.int32, (BLOCK, 1), 0)
    loaded("d")
    r.dall[block_rows(head), :] = (r.dv[...].astype(F32) * jnp.where(position < total, 1.0, 0.0)).astype(BF)
    d_begin((1, 0))
    loaded("wqkv")
    aligned = lax.div(3 * head, 2) * 128
    odd = jnp.where(lax.rem(head, 2) == 1, 1.0, 0.0)
    on_heads = jnp.where(onlane < 192, 1.0, 0.0)

    def own_window(values):
        moved = pltpu.roll(values, 192, 1)
        return (values * (1.0 - odd) + moved * odd) * on_heads

    r.vec[0:2, :] = r.qv_bias[...].astype(F32)
    pair_bias = own_window(r.vec[:, pl.ds(pl.multiple_of(aligned, 128), 256)])
    bias = jnp.concatenate([pair_bias[0:1], jnp.zeros((1, 256), F32), pair_bias[1:2]], axis=1)
    for part in range(3):
        window = pl.ds(pl.multiple_of(part * D + aligned, 128), 256)
        r.wqo[:, part * 256 : (part + 1) * 256] = own_window(r.wqkv[:, window].astype(F32)).astype(BF)

    aux_k = jnp.where((onlane >= 196) & (onlane < 199), 1.0, 0.0)
    aux_v = jnp.where((onlane >= 192) & (onlane < 199) & (onlane != 195), 1.0, 0.0)
    on_aux = jnp.where(onlane >= 192, 1.0, 0.0)

    def project(block):
        rows = block_rows(block)
        projected = (nn(r.nall[rows, :], r.wqo[...]) + bias).astype(BF).astype(F32)
        r.qb[rows, :] = (projected[:, :256] * 0.125 + lane_is(192 + block)).astype(BF)
        off = jnp.where((onlane >= 192) & (onlane < 196) & (onlane != 192 + block), 1.0, 0.0)
        r.kb[rows, :] = (projected[:, 256:512] + (aux_k + off * jnp.where(whole, 0.0, FAR))).astype(BF)
        r.vb[rows, :] = (projected[:, 512:] + aux_v).astype(BF)

    project(head)
    n_wait(0)
    project(sib)
    n_relay()
    project(far)
    n_rest()
    project(diag)

    def packed(values):
        third = values[:, 128:]
        return jnp.concatenate([values[:, :128], third[:128] + pltpu.roll(third[128:], 64, 1)], axis=0).astype(BF)

    def unpack(source, dst, base):
        for group in range(4):
            lane = group * 192
            dst[base : base + 256, lane : lane + 128] = source[group, 0:256, :]
            dst[base : base + 128, lane + 128 : lane + 192] = source[group, 256:384, 0:64]
            dst[base + 128 : base + 256, lane + 128 : lane + 192] = source[group, 256:384, 64:128]

    def mix_copy(code):
        return push(r.mixs.at[code], r.mixin.at[head], r.ms.at[code - 1], r.mr.at[code - 1], (dp, peer(code)))

    small_lane = lax.broadcasted_iota(jnp.int32, (1, 128), 1)

    def attend(step, carry):
        code = 3 - step
        block = peer(code)
        rows = block_rows(block)
        queries = r.qb[rows, :]
        mixed = jnp.zeros((BLOCK, 256), F32)
        tops = []
        for n in range(3):
            scores = nt(queries * (head_mask(n) + on_aux).astype(BF), r.kb[...])
            top = jnp.max(scores, axis=1, keepdims=True)
            weights = jnp.exp(scores - top).astype(BF)
            mixed += nn(weights, r.vb[...] * (head_mask(n) + lane_is(192 + n)).astype(BF))
            tops.append(top)
        lse = jnp.zeros((BLOCK, 128), F32)
        scale = jnp.zeros((BLOCK, 256), F32)
        for n in range(3):
            row_sum = jnp.sum(mixed * lane_is(192 + n), axis=1, keepdims=True)
            lse += (tops[n] + jnp.log(row_sum)) * jnp.where(small_lane == n, 1.0, 0.0)
            scale += (1.0 / row_sum) * head_mask(n)
        place = block * BLOCK + lax.broadcasted_iota(jnp.int32, (BLOCK, 1), 0)
        mixed = jnp.where(place < total, mixed * scale, r.vb[rows, :].astype(F32) * on_heads)
        r.exact[rows, :] = mixed
        r.lse[rows, :] = lse
        r.mix[rows, :] = mixed.astype(BF)
        r.mixs[code] = packed(mixed)

        @pl.when(step < 3)
        def _():
            mix_copy(code).start()

        @pl.when(step == 1)
        def _():
            d_begin((2,))

        return carry

    lax.fori_loop(0, 4, attend, 0)
    r.mixin[head] = r.mixs[0]
    d_relay((1,))

    loaded("wout")
    loaded("wup")
    loaded("wdown")
    for code in (3, 2, 1):
        mix_copy(code).wait_recv()
    unpack(r.mixin, r.wqo, 0)
    hidden = r.xv[...].astype(F32) + nn(r.wqo[0:256, :], r.wout[...]) + biases[0:1, :]
    unit, inverse, normed = norm_parts(hidden, gains[1:2, :], shifts[1:2, :])
    second = normed.astype(BF)
    r.sall[block_rows(head), :] = second
    s_begin()
    grad_low = r.dall[block_rows(head), :]
    up_bias = r.up_bias[...].astype(F32)
    r.bias_rows[...] = up_bias
    down = jnp.zeros((BLOCK, D), F32)
    back = jnp.zeros((BLOCK, D), F32)
    for tile in range(4):
        cut = slice(tile * D, (tile + 1) * D)
        up = nn(second, r.wup[:, cut]) + jnp.concatenate([up_bias[6 * tile + i : 6 * tile + i + 1] for i in range(6)], axis=1)
        value, slope = gelu_parts(up)
        w_down = r.big[cut, 0:D]
        down += nn(value.astype(BF), w_down)
        grad_up = nt(grad_low, w_down) * slope
        back += nt(grad_up.astype(BF), r.wup[:, cut])
    r.block_out[...] = (hidden + down + biases[1:2, :]).astype(BF)
    give("block_out")
    grad_block = grad_low.astype(F32)
    grad_hidden = grad_block + norm_back(back, unit, inverse, gains[1:2, :])
    r.gh[...] = grad_hidden
    r.lall[block_rows(head), :] = grad_hidden.astype(BF)
    l_begin()
    r.vec[...] = jnp.zeros_like(r.vec)
    r.vec[1:2, :] = jnp.sum(back * unit, axis=0, keepdims=True)
    r.vec[3:4, :] = jnp.sum(back, axis=0, keepdims=True)
    r.vec[6:7, :] = jnp.sum(grad_hidden, axis=0, keepdims=True)
    r.vec[7:8, :] = jnp.sum(grad_block, axis=0, keepdims=True)

    loaded("wuo")
    loaded("wdo")
    loaded("woo")
    own_bias = jnp.concatenate([r.bias_rows[pl.ds(4 * j + head, 1), :] for j in range(6)], axis=1)

    def feed(step, sums):
        @pl.when(step == 1)
        def _():
            d_wait(0)
            s_wait(0)

        @pl.when(step == 2)
        def _():
            d_relay((2,))
            s_relay()

        @pl.when(step == 3)
        def _():
            d_rest()
            s_rest()

        rows = block_rows(peer(step))
        up = nn(r.sall[rows, :], r.wuo[...]) + own_bias
        value, slope = gelu_parts(up)
        r.act[rows, :] = value.astype(BF)
        grad_up = nt(r.dall[rows, :], r.wdo[...]) * slope
        r.gup[rows, :] = grad_up.astype(BF)
        return sums + jnp.sum(grad_up, axis=0, keepdims=True)

    sums = lax.fori_loop(0, 4, feed, jnp.zeros((1, D), F32))
    def parts_of(name):
        refs = [getattr(r, part + name) for part in ("p", "y", "z", "f")]
        return refs + [getattr(r, part + name + end) for part in ("y", "z", "f") for end in ("s", "r")]

    def finals(fin, fs, fr):
        def f_copy(code):
            place = far if code == 3 else head
            to = far if code == 2 else sib
            return push(fin.at[place], fin.at[place], fs.at[code - 1], fr.at[code - 1], (dp, to))

        def begin():
            for code in (2, 1):
                start(lambda code=code: f_copy(code))

        def relay():
            f_copy(2).wait_recv()
            start(lambda: f_copy(3))

        def rest():
            f_copy(1).wait_recv()
            f_copy(3).wait_recv()

        return begin, relay, rest

    def add_to(ref, at, more):
        ref[at] = (ref[at].astype(F32) + more.astype(F32)).astype(BF)

    def y_first(name):
        own, ybuf, zbuf, fin, ys, yr, zs, zr, fs, fr = parts_of(name)
        f_begin, relay, rest = finals(fin, fs, fr)

        def y_copy(t):
            src = own.at[z_order[t] * 2 + (1 - y)]
            return push(src, ybuf.at[t], ys.at[t], yr.at[t], (other_y, head))

        def near_copy(t):
            return push(own.at[z_order[t] * 2 + y], zbuf.at[t], zs.at[t], zr.at[t], (beside * 2 + y, head))

        def across_copy(t):
            shard = z_order[t] * 2 + y
            return push(own.at[shard], zbuf.at[3], zs.at[t], zr.at[3], (shard, head))

        def begin():
            for t in range(4):
                start(lambda t=t: y_copy(t))

        def pair(t):
            y_copy(t).wait_recv()
            add_to(own, z_order[t] * 2 + y, ybuf[t])
            if t == 2:
                near_copy(t).start()
            elif t < 2:
                pl.when(outer)(lambda: near_copy(t).start())

        def fold(t):
            @pl.when(inner)
            def _():
                near_copy(t).wait_recv()
                add_to(own, z_order[t] * 2 + y, zbuf[t])
                across_copy(t).start()

        def total_up():
            near_copy(2).wait_recv()
            across_copy(0).wait_recv()
            fin[head] = (own[dp].astype(F32) + zbuf[2].astype(F32) + zbuf[3].astype(F32)).astype(BF)
            f_begin()
            sent.append((lambda: near_copy(2), None))
            for t in (0, 1):
                sent.append((lambda t=t: near_copy(t), outer))
                sent.append((lambda t=t: across_copy(t), inner))

        return begin, pair, fold, total_up, relay, rest

    def z_first(name):
        own, ybuf, zbuf, fin, ys, yr, zs, zr, fs, fr = parts_of(name)
        f_begin, relay, rest = finals(fin, fs, fr)

        def both(t):
            return pl.ds(z_order[t] * 2, 2)

        def near_copy(t):
            return push(own.at[both(t)], zbuf.at[t], zs.at[t], zr.at[t], (beside * 2 + y, head))

        def across_copy(t):
            return push(own.at[both(t)], zbuf.at[3], zs.at[t], zr.at[3], (z_order[t] * 2 + y, head))

        def y_copy():
            return push(own.at[z * 2 + (1 - y)], ybuf.at[0], ys.at[0], yr.at[0], (other_y, head))

        def begin():
            for t in (0, 1):
                start(lambda t=t: near_copy(t), outer)
            start(lambda: near_copy(2))

        def fold(t):
            @pl.when(inner)
            def _():
                near_copy(t).wait_recv()
                add_to(own, both(t), zbuf[t])
                across_copy(t).start()

        def pair():
            near_copy(2).wait_recv()
            across_copy(0).wait_recv()
            add_to(own, both(3), zbuf[2].astype(F32) + zbuf[3].astype(F32))
            y_copy().start()

        def total_up():
            y_copy().wait_recv()
            fin[head] = (own[dp].astype(F32) + ybuf[0].astype(F32)).astype(BF)
            f_begin()
            for t in (0, 1):
                sent.append((lambda t=t: across_copy(t), inner))
            sent.append((y_copy, None))

        return begin, fold, pair, total_up, relay, rest

    def irregular(name, count, per_shard, number_of, owner_of):
        own, ybuf, zbuf, fin, ys, yr, zs, zr, fs, fr = parts_of(name)

        def facts(j):
            number = number_of(j)
            shard = lax.div(number, per_shard)
            return shard, lax.div(shard, 2), lax.rem(shard, 2), lax.rem(number, per_shard)

        def y_copy(j):
            return push(own.at[j], ybuf.at[j], ys.at[j], yr.at[j], (other_y, head))

        def near_copy(j):
            slot = jnp.where(facts(j)[1] == beside, count + facts(j)[3], j)
            return push(own.at[j], zbuf.at[slot], zs.at[j], zr.at[slot], (beside * 2 + y, head))

        def near_arrival(j):
            return push(own.at[j], zbuf.at[j], zs.at[j], zr.at[j], (beside * 2 + y, head))

        def across_copy(j):
            shard, _, _, place = facts(j)
            return push(own.at[j], zbuf.at[count + per_shard + place], zs.at[j], zr.at[count + per_shard + place], (shard, head))

        def last_arrival(j, base):
            place = base + facts(j)[3]
            return push(own.at[j], zbuf.at[place], zs.at[j], zr.at[place], (dp, sib)), place

        def f_copy(code, place):
            index = (code - 1) * per_shard + place
            to = far if code == 2 else sib
            return push(fin.at[place], fin.at[place], fs.at[index], fr.at[index], (dp, to))

        def begin(these=range(count)):
            for j in these:
                start(lambda j=j: y_copy(j), facts(j)[2] != y)

        def mine(j):
            return facts(j)[2] == y

        def other_half(j):
            return lax.div(facts(j)[1], 2) != half

        def to_near(j):
            return mine(j) & ((facts(j)[1] == beside) | (other_half(j) & outer))

        def to_across(j):
            return mine(j) & other_half(j) & inner

        def fold(j):
            @pl.when(to_across(j))
            def _():
                near_arrival(j).wait_recv()
                add_to(own, j, zbuf[j])
                across_copy(j).start()

        def pair(j):
            @pl.when(mine(j))
            def _():
                y_copy(j).wait_recv()
                add_to(own, j, ybuf[j])

            pl.when(to_near(j))(lambda: near_copy(j).start())

        def total_up(these=range(count)):
            for j in these:
                sent.append((lambda j=j: near_copy(j), to_near(j)))
                sent.append((lambda j=j: across_copy(j), to_across(j)))
                shard, _, _, place = facts(j)

                def body(j=j, place=place):
                    value = own[j].astype(F32)
                    for base in (count, count + per_shard):
                        copy, slot = last_arrival(j, base)
                        copy.wait_recv()
                        value += zbuf[slot].astype(F32)
                    fin[place] = value.astype(BF)
                    f_copy(2, place).start()
                    f_copy(1, place).start()

                pl.when(shard == dp)(body)

        def relay():
            for place in range(per_shard):
                owner = owner_of(per_shard * dp + place)
                for code in (1, 2):
                    sent.append((lambda code=code, place=place: f_copy(code, place), owner == head))

                def body(place=place):
                    f_copy(2, place).wait_recv()
                    f_copy(3, place).start()

                pl.when(owner == far)(body)
                sent.append((lambda place=place: f_copy(3, place), owner == far))

        def rest():
            for place in range(per_shard):
                owner = owner_of(per_shard * dp + place)
                for code, source in ((1, sib), (3, diag)):
                    pl.when(owner == source)(lambda code=code, place=place: f_copy(code, place).wait_recv())

        return begin, pair, fold, total_up, relay, rest

    dy_begin, dy_pair, dy_fold, dy_total, dy_relay, dy_rest = y_first("dy")
    dz_begin, dz_fold, dz_pair, dz_total, dz_relay, dz_rest = z_first("dz")
    ou_begin, ou_pair, ou_fold, ou_total, ou_relay, ou_rest = y_first("ou")
    up_begin, up_pair, up_fold, up_total, up_relay, up_rest = irregular(
        "up", 6, 3, lambda j: 4 * j + head, lambda number: lax.rem(number, 4)
    )
    qk_begin, qk_pair, qk_fold, qk_total, qk_relay, qk_rest = irregular(
        "qk",
        12,
        6,
        lambda j: ((j // 4) * 8 + 2 * head + j // 2 % 2) * 2 + j % 2,
        lambda number: lax.div(lax.rem(lax.div(number, 2), 8), 2),
    )

    r.pdz[...] = tn(r.dall[...], r.act[:, 256:]).astype(BF).reshape(8, 96, 512)
    dz_begin()
    r.pdy[...] = tn(r.dall[...], r.act[:, :256]).astype(BF).reshape(8, 96, 256)
    dy_begin()
    up_grad = tn(r.sall[...], r.gup[...]).astype(BF)
    for j in range(6):
        r.pup[j] = up_grad[:, j * 128 : (j + 1) * 128]
    up_begin()

    r.fsm[head] = jnp.zeros((2, 4, 16, 128), F32)
    for j in range(6):
        number = 4 * j + head
        shard = lax.div(number, 3)
        r.fsm[head, lax.rem(shard, 2), lax.div(shard, 2), pl.ds(8 + lax.rem(number, 3), 1), :] = sums[
            :, j * 128 : (j + 1) * 128
        ]

    q_aug, g_aug = r.act, r.gup
    tile_lane = lanes_of(128)
    spot_row, spot_lane = (lax.broadcasted_iota(jnp.int32, (128, 128), axis) for axis in (0, 1))
    spots = [
        jnp.where((spot_lane == 68 + lax.div(spot_row, 3)) & (lax.rem(spot_row, 3) == n) & (spot_row < 9), 1.0, 0.0)
        for n in range(3)
    ]
    spots = [spot.astype(BF) for spot in spots]

    def aux_of(columns):
        high, middle, low = split_three(columns)
        return (high + pltpu.roll(middle, 3, 1) + pltpu.roll(low, 6, 1)).astype(BF)

    def write_aug(dst, rows, source, aux, keep):
        left = source[:, :128]
        right = source[:, 128:].astype(F32)
        for n in range(3):
            if n < 2:
                part = left * jnp.where(lax.div(tile_lane, 64) == n, 1.0, 0.0).astype(BF)
            else:
                part = jnp.zeros((256, 128), BF)
            dst[rows, n * 256 : n * 256 + 128] = part
            mask = jnp.where(tile_lane < 64, 1.0 if n == 2 else 0.0, keep)
            dst[rows, n * 256 + 128 : (n + 1) * 256] = (right * mask + nn(aux, spots[n])).astype(BF)

    def augment_q(block, carry):
        rows = pl.ds(pl.multiple_of(block * 256, 256), 256)
        write_aug(q_aug, rows, r.qb[rows, :], aux_of(-r.lse[rows, :]), 1.0)
        return carry

    lax.fori_loop(0, 4, augment_q, 0)
    sum_row, sum_lane = (lax.broadcasted_iota(jnp.int32, (256, 128), axis) for axis in (0, 1))
    head_sums = jnp.where((lax.div(sum_row, 64) == sum_lane) & (sum_row < 192), 1.0, 0.0).astype(BF)
    r.woo[192:256, :] = jnp.zeros((64, D), BF)
    l_relay((1,))
    dy_pair(0)
    dy_pair(1)
    s_drain()
    d_drain()
    dv, dq, dk = (r.sall.at[:, part * 256 : (part + 1) * 256] for part in range(3))
    gm = r.dall.at[:, 0:256]
    l_wait(0)
    l_relay((2,))
    dz_fold(0)
    dy_pair(2)
    dy_pair(3)
    l_rest()
    gm[...] = nt(r.lall[...], r.woo[...]).astype(BF)

    out_grad = tn(r.lall[...], r.mix[...]).reshape(8, 96, 256)
    r.pou[:, 0:96, :] = out_grad[:, :, :128].astype(BF)
    third = out_grad[:, :, 128:].reshape(8, 2, 48, 128)
    moved = pltpu.roll(third[:, 1].reshape(384, 128), 64, 1).reshape(8, 48, 128)
    r.pou[:, 96:144, :] = (third[:, 0] + moved).astype(BF)
    ou_begin()

    def augment_g(block, carry):
        rows = pl.ds(pl.multiple_of(block * 256, 256), 256)
        grads = gm[rows, :]
        product = grads.astype(F32) * r.exact[rows, :]
        inner = jnp.zeros((256, 128), F32)
        for part in split_three(product):
            inner += nn(part.astype(BF), head_sums)
        write_aug(g_aug, rows, grads, aux_of(-inner), 0.0)
        return carry

    lax.fori_loop(0, 4, augment_g, 0)
    dz_fold(1)

    def k_copy(code):
        return push(r.ks_.at[code], r.kin.at[head], r.ks.at[code - 1], r.kr.at[code - 1], (dp, peer(code)))

    def v_copy(code):
        return push(r.vs_.at[code], r.vin.at[head], r.vs.at[code - 1], r.vr.at[code - 1], (dp, peer(code)))

    def q_copy(code):
        return push(r.qs_.at[code], r.qin.at[head], r.qs.at[code - 1], r.qr.at[code - 1], (dp, peer(code)))

    def attend_back(step, carry):
        code = 3 - step
        block = peer(code)
        rows = block_rows(block)
        value_grad = jnp.zeros((BLOCK, 256), F32)
        for n in range(3):
            mask = head_mask(n)
            lanes = slice(n * 256, (n + 1) * 256)
            probs = jnp.exp(nt(r.kb[rows, :], q_aug[:, lanes]))
            grad_scores = (probs * nt(r.vb[rows, :], g_aug[:, lanes])).astype(BF)
            r.big[pl.ds(pl.multiple_of(n * SLOT + block * BLOCK, 256), BLOCK), :] = grad_scores
            value_grad += nn(probs.astype(BF), g_aug[:, lanes]) * mask
        dv[rows, :] = value_grad.astype(BF)
        r.vs_[code] = packed(value_grad)

        @pl.when(step < 3)
        def _():
            v_copy(code).start()

        @pl.when(step == 2)
        def _():
            dz_pair()
            dy_fold(0)
            up_pair(0)
            up_pair(1)

        @pl.when(step == 3)
        def _():
            dy_fold(1)
            up_pair(2)

        return carry

    lax.fori_loop(0, 4, attend_back, 0)
    r.vin[head] = r.vs_[0]
    r.pqk[8:12] = tn(dv[...], r.nall[...])[:192].astype(BF).reshape(4, 48, D)
    qk_begin(range(8, 12))
    up_pair(3)

    def query_back(step, carry):
        code = 3 - step
        block = peer(code)
        rows = block_rows(block)
        query_grad = jnp.zeros((BLOCK, 256), F32)
        for n in range(3):
            part = r.big[n * SLOT : (n + 1) * SLOT, pl.ds(pl.multiple_of(block * BLOCK, 256), BLOCK)]
            query_grad += tn(part, r.kb[...] * head_mask(n).astype(BF))
        query_grad = query_grad * 0.125
        dq[rows, :] = query_grad.astype(BF)
        r.qs_[code] = packed(query_grad)

        @pl.when(step < 3)
        def _():
            q_copy(code).start()

        return carry

    lax.fori_loop(0, 4, query_back, 0)
    r.qin[head] = r.qs_[0]
    r.pqk[0:4] = tn(dq[...], r.nall[...])[:192].astype(BF).reshape(4, 48, D)
    qk_begin(range(4))
    up_pair(4)
    up_pair(5)

    def key_back(step, carry):
        code = 3 - step
        block = peer(code)
        rows = block_rows(block)
        key_grad = jnp.zeros((BLOCK, 256), F32)
        for n in range(3):
            part = r.big[pl.ds(pl.multiple_of(n * SLOT + block * BLOCK, 256), BLOCK), :]
            key_grad += nn(part, q_aug[:, n * 256 : (n + 1) * 256]) * head_mask(n)
        dk[rows, :] = key_grad.astype(BF)
        r.ks_[code] = packed(key_grad)

        @pl.when(step < 3)
        def _():
            k_copy(code).start()

        return carry

    lax.fori_loop(0, 4, key_back, 0)
    r.kin[head] = r.ks_[0]
    r.pqk[4:8] = tn(dk[...], r.nall[...])[:192].astype(BF).reshape(4, 48, D)
    qk_begin(range(4, 8))
    query_sum = jnp.sum(dq[...].astype(F32), axis=0, keepdims=True)
    value_sum = jnp.sum(dv[...].astype(F32), axis=0, keepdims=True)
    for group in range(4):
        mine = jnp.where(head == group, 1.0, 0.0)
        r.vec[4:5, group * 192 : (group + 1) * 192] = query_sum[:, :192] * mine
        r.vec[5:6, group * 192 : (group + 1) * 192] = value_sum[:, :192] * mine
    for shard in range(8):
        r.fsm[head, shard % 2, shard // 2, 0:8, 0:96] = r.vec[:, shard * 96 : (shard + 1) * 96]

    def small_y():
        return push(r.small.at[1 - y], r.ysm, r.ysms.at[0], r.ysmr.at[0], (other_y, head))

    def small_z(k):
        return push(
            r.small.at[y, z_shard(k)], r.zsm.at[k], r.zsms.at[k], r.zsmr.at[k], (z_shard(k) * 2 + y, head)
        )

    def small_f(code):
        return push(r.fsm.at[head], r.fsm.at[head], r.fsms.at[code - 1], r.fsmr.at[code - 1], (dp, peer(code)))

    for code in (2, 3, 1):
        start(lambda code=code: small_f(code))
    for t in range(4):
        ou_pair(t)
    for j in range(8, 12):
        qk_pair(j)
    for j in range(6):
        up_fold(j)
    dy_total()
    dz_total()
    for j in range(4):
        qk_pair(j)

    for code in (3, 2, 1):
        k_copy(code).wait_recv()
        v_copy(code).wait_recv()
        q_copy(code).wait_recv()
    unpack(r.qin, r.wuo, 0)
    unpack(r.kin, r.wuo, 256)
    unpack(r.vin, r.wuo, 512)
    grad_first = nt(r.wuo[0:256, :], r.wqkv[:, 0:D])
    grad_first += nt(r.wuo[256:512, :], r.wqkv[:, D : 2 * D])
    grad_first += nt(r.wuo[512:768, :], r.wqkv[:, 2 * D :])
    ou_fold(0)
    ou_fold(1)
    for code in (1, 2, 3):
        small_f(code).wait_recv()
    r.small[...] = r.fsm[0] + r.fsm[1] + r.fsm[2] + r.fsm[3]
    start(small_y)
    for j in range(8, 12):
        qk_fold(j)
    unit, inverse, _ = norm_parts(r.xv[...].astype(F32), gains[0:1, :], shifts[0:1, :])
    r.grad_inputs[...] = r.gh[...] + norm_back(grad_first, unit, inverse, gains[0:1, :])
    give("grad_inputs")
    pair = jnp.concatenate(
        [jnp.sum(grad_first * unit, axis=0, keepdims=True), jnp.sum(grad_first, axis=0, keepdims=True)], axis=0
    )
    r.last[head] = jnp.zeros((16, 128), F32)
    for shard in range(8):
        at = shard % 2 * 8 + shard // 2 * 2
        r.last[head, at : at + 2, 0:96] = pair[:, shard * 96 : (shard + 1) * 96]

    def last_head(code):
        return push(r.last.at[head], r.last.at[head], r.las.at[code - 1], r.lar.at[code - 1], (dp, peer(code)))

    def last_y():
        return push(r.lasty.at[1 - y], r.lastz.at[4], r.lays.at[0], r.layr.at[0], (other_y, head))

    def last_z(k):
        return push(r.lastz.at[0], r.lastz.at[k], r.lazs.at[k], r.lazr.at[k], (z_shard(k) * 2 + y, head))

    for code in (2, 3, 1):
        start(lambda code=code: last_head(code))
    for j in range(4, 8):
        qk_pair(j)
    up_total()
    for j in range(4):
        qk_fold(j)
    small_y().wait_recv()
    r.small[y] = r.small[y] + r.ysm[...]
    for k in (1, 2, 3):
        start(lambda k=k: small_z(k))
    for code in (1, 2, 3):
        last_head(code).wait_recv()
    over_head = r.last[0] + r.last[1] + r.last[2] + r.last[3]
    r.lasty[0] = over_head[0:8]
    r.lasty[1] = over_head[8:16]
    start(last_y)
    dy_relay()
    dz_relay()
    ou_total()
    qk_total(range(8, 12))
    for j in range(4, 8):
        qk_fold(j)
    last_y().wait_recv()
    r.lastz[0] = r.lasty[y] + r.lastz[4]
    for k in (1, 2, 3):
        start(lambda k=k: last_z(k))
    qk_total(range(4))
    up_relay()
    ou_relay()
    qk_total(range(4, 8))
    for k in (1, 2, 3):
        last_z(k).wait_recv()
    dy_rest()
    give("fdy")
    dz_rest()
    give("fdz")
    qk_relay()
    up_rest()
    give("fup")
    ou_rest()
    give("fou")
    qk_rest()
    give("fqk")
    for k in (1, 2, 3):
        small_z(k).wait_recv()
    r.fsum[...] = r.small[y, z] + r.zsm[1] + r.zsm[2] + r.zsm[3]
    r.lastf[...] = r.lastz[0] + r.lastz[1] + r.lastz[2] + r.lastz[3]
    r.fsum[0:1, :] = r.lastf[pl.ds(2 * z, 1), :]
    r.fsum[2:3, :] = r.lastf[pl.ds(2 * z + 1, 1), :]
    give("fsum")
    n_drain()
    l_drain()
    for make, cond in sent:
        when(cond, lambda make=make: make().wait_send())
    for code in (1, 2, 3):
        mix_copy(code).wait_send()
        k_copy(code).wait_send()
        v_copy(code).wait_send()
        q_copy(code).wait_send()
    for copy in given:
        copy.wait()


def emit_kernel(
    block_in, inputs_in, fup, fqk, fdy, fdz, fou, fsum,
    block_out, grad_inputs, gains, shifts, qkv, qv_bias, out, out_biases, up, up_bias, down,
    block_v, inputs_v, fup_v, fqk_v, fdy_v, fdz_v, fou_v, fsum_v, up_v, qkv_v, down_v, out_v, gains_v, shifts_v, qv_v, ob_v, ub_v, sems,
):
    count = []

    def begin(src, dst):
        count.append(pltpu.make_async_copy(src, dst, sems.at[len(count)]))
        count[-1].start()
        return count[-1]

    pairs = (
        (fdy, fdy_v), (fdz, fdz_v), (fup, fup_v), (inputs_in, inputs_v), (block_in, block_v), (fqk, fqk_v), (fou, fou_v),
        (fsum, fsum_v),
    )
    arrivals = [begin(src, dst) for src, dst in pairs]
    results = []
    arrivals[0].wait()
    arrivals[1].wait()
    for group in range(4):
        for j in range(6):
            place = (4 * j + group) * 128
            source, at = (fdy_v, j * 128) if j < 2 else (fdz_v, j * 128 - 256)
            down_v[:, place : place + 128] = source[group, :, at : at + 128].astype(F32)
    results.append(begin(down_v, down))
    arrivals[7].wait()
    for index, (ref, dst) in enumerate(((gains_v, gains), (shifts_v, shifts), (qv_v, qv_bias), (ob_v, out_biases))):
        ref[...] = fsum_v[2 * index : 2 * index + 2, 0:96]
        results.append(begin(ref, dst))
    ub_v[...] = fsum_v[8:11, :]
    results.append(begin(ub_v, up_bias))
    arrivals[2].wait()
    for i in range(3):
        up_v[:, i * 128 : (i + 1) * 128] = fup_v[i].astype(F32)
    results.append(begin(up_v, up))
    for arrival, src, dst in ((3, inputs_v, grad_inputs), (4, block_v, block_out)):
        arrivals[arrival].wait()
        results.append(begin(src, dst))
    arrivals[5].wait()
    qkv_v[...] = fqk_v[...].reshape(288, D).astype(F32)
    results.append(begin(qkv_v, qkv))
    arrivals[6].wait()
    for group in range(4):
        piece, lane = fou_v[group].astype(F32), group * 192
        out_v[:, lane : lane + 128] = piece[0:96]
        out_v[0:48, lane + 128 : lane + 192] = piece[96:144, 0:64]
        out_v[48:96, lane + 128 : lane + 192] = piece[96:144, 64:128]
    results.append(begin(out_v, out))
    for copy in results:
        copy.wait()


def per_device(x, norm_gains, norm_shifts, w_qkv, qv_bias, w_out, out_biases, w_up, up_bias, w_down, lengths, d_out):
    values = dict(
        x=x[0], gains=norm_gains, shifts=norm_shifts, w_qkv=w_qkv, qv_bias=qv_bias, w_out=w_out, biases=out_biases,
        w_up=w_up, up_bias=up_bias.reshape(24, 128), w_down=w_down, lengths=lengths, d_out=d_out[0],
    )
    place = {True: pl.BlockSpec(memory_space=pl.ANY), False: pl.BlockSpec(memory_space=pltpu.VMEM)}
    block_out, grad_inputs, fup, fqk, fdy, fdz, fou, fsum = pl.pallas_call(
        one_kernel,
        out_shape=[jax.ShapeDtypeStruct(shape, kind) for _, shape, kind in OUTPUTS],
        in_specs=[place[name in IN_PLACE] for name in INPUTS],
        out_specs=[place[True]] * len(OUTPUTS),
        scratch_shapes=[pltpu.VMEM(shape, kind) for _, shape, kind in OUTPUTS + BUFFERS]
        + [pltpu.SemaphoreType.DMA((count,)) for _, count in SEMAPHORES],
        compiler_params=pltpu.CompilerParams(
            collective_id=0, has_side_effects=True, vmem_limit_bytes=VMEM_LIMIT
        ),
        name="block",
    )(*(values[name] for name in INPUTS))
    anywhere = pl.BlockSpec(memory_space=pl.ANY)
    shapes = [(256, D), (256, D), (2, 96), (2, 96), (288, D), (2, 96), (96, D), (2, 96), (D, 384), (3, 128), (96, FF)]
    outs = pl.pallas_call(
        emit_kernel,
        out_shape=[jax.ShapeDtypeStruct(shape, F32 if n else BF) for n, shape in enumerate(shapes)],
        in_specs=[anywhere] * 8,
        out_specs=[anywhere] * len(shapes),
        scratch_shapes=[pltpu.VMEM(shape, kind) for _, shape, kind in OUTPUTS]
        + [pltpu.VMEM(shape, F32) for shape in ((D, 384), (288, D), (96, FF), (96, D))]
        + [pltpu.VMEM(shape, F32) for shape in ((2, 96),) * 4 + ((3, 128),)]
        + [pltpu.SemaphoreType.DMA((19,))],
        compiler_params=pltpu.CompilerParams(vmem_limit_bytes=VMEM_LIMIT),
        name="emit",
    )(block_out, grad_inputs, fup, fqk, fdy, fdz, fou, fsum)
    return (
        outs[0][None], outs[1][None], outs[2], outs[3], outs[4].T, outs[5], outs[6].T, outs[7], outs[8],
        outs[9].reshape(384), outs[10].T,
    )


def solution(mesh):
    split = P("dp", "head", None)
    placed = (split,) + (P(),) * 9 + (P("dp", None), split)
    return jax.shard_map(
        per_device if dict(mesh.shape) == {"dp": 8, "head": 4} else general_device,
        mesh=mesh,
        in_specs=placed,
        out_specs=(split, split) + (P(None, "dp"),) * 7 + (P("dp"), P(None, "dp")),
        check_vma=False,
    )
```

```python
import functools

import jax
import jax.numpy as jnp
from jax import lax
from jax.experimental import pallas as pl
from jax.experimental.pallas import tpu as pltpu
from jax.sharding import PartitionSpec as P

D = 768
HEADS = 12
HDIM = 64
FF = 3072
SLOT = 1024
EPSILON = 1e-06
BF = jnp.bfloat16
F32 = jnp.float32
FAR = -1e30
VMEM_LIMIT = 63 * 1024 * 1024


def nn(a, b):
    return lax.dot_general(a, b, (((1,), (0,)), ((), ())), preferred_element_type=F32)


def nt(a, b):
    return lax.dot_general(a, b, (((1,), (1,)), ((), ())), preferred_element_type=F32)


def tn(a, b):
    return lax.dot_general(a, b, (((0,), (0,)), ((), ())), preferred_element_type=F32)


def norm_parts(values, norm_gain, norm_shift):
    average = jnp.mean(values, axis=-1, keepdims=True)
    centered = values - average
    variance = jnp.mean(centered * centered, axis=-1, keepdims=True)
    inverse = lax.rsqrt(variance + EPSILON)
    unit = centered * inverse
    return unit, inverse, unit * norm_gain + norm_shift


def norm_back(grad_normed, unit, inverse, norm_gain):
    grad_unit = grad_normed * norm_gain
    first_mean = jnp.mean(grad_unit, axis=-1, keepdims=True)
    second_mean = jnp.mean(grad_unit * unit, axis=-1, keepdims=True)
    return inverse * (grad_unit - first_mean - unit * second_mean)


def gelu_parts(values):
    cumulative = 0.5 + 0.5 * lax.erf(values * 0.7071067811865476)
    density = jnp.exp(values * values * -0.5) * 0.3989422804014327
    return values * cumulative, cumulative + values * density


def lanes_of(width=256):
    return lax.broadcasted_iota(jnp.int32, (1, width), 1)


def head_mask(head):
    lane = lanes_of()
    return jnp.where((lane >= head * HDIM) & (lane < (head + 1) * HDIM), 1.0, 0.0)


def lane_is(index):
    return jnp.where(lanes_of() == index, 1.0, 0.0)


def split_three(column):
    high = column.astype(BF).astype(F32)
    rest = column - high
    middle = rest.astype(BF).astype(F32)
    return high, middle, rest - middle


def attend_forward(normed, weight, bias, lengths, q_ref, k_ref, v_ref, mixed_ref, exact_ref, lse_ref):
    whole = lengths[:, 0:1] == SLOT
    total = jnp.sum(lengths, axis=1, keepdims=True)
    onlane = lanes_of()
    aux_k = jnp.where((onlane >= 196) & (onlane < 199), 1.0, 0.0)
    aux_v = jnp.where((onlane >= 192) & (onlane < 199) & (onlane != 195), 1.0, 0.0)
    for block in range(4):
        rows = pl.ds(block * 256, 256)
        projected = nn(normed[rows, :], weight[...]) + bias
        projected = projected.astype(BF).astype(F32)
        q_ref[rows, :] = (projected[:, :256] * 0.125 + lane_is(192 + block)).astype(BF)
        other = jnp.where((onlane >= 192) & (onlane < 196) & (onlane != 192 + block), 1.0, 0.0)
        far = other * jnp.where(whole, 0.0, FAR)
        k_ref[rows, :] = (projected[:, 256:512] + (aux_k + far)).astype(BF)
        v_ref[rows, :] = (projected[:, 512:] + aux_v).astype(BF)
    on_aux = jnp.where(onlane >= 192, 1.0, 0.0)

    def block_step(block, carry):
        rows = pl.ds(pl.multiple_of(block * 256, 256), 256)
        queries = q_ref[rows, :]
        mixed = jnp.zeros((256, 256), F32)
        tops = []
        for head in range(3):
            scores = nt(queries * (head_mask(head) + on_aux).astype(BF), k_ref[...])
            top = jnp.max(scores, axis=1, keepdims=True)
            weights = jnp.exp(scores - top).astype(BF)
            mixed += nn(weights, v_ref[...] * (head_mask(head) + lane_is(192 + head)).astype(BF))
            tops.append(top)
        lse = jnp.zeros((256, 128), F32)
        scale = jnp.zeros((256, 256), F32)
        small = lax.broadcasted_iota(jnp.int32, (1, 128), 1)
        for head in range(3):
            row_sum = jnp.sum(mixed * lane_is(192 + head), axis=1, keepdims=True)
            lse += (tops[head] + jnp.log(row_sum)) * jnp.where(small == head, 1.0, 0.0)
            scale += (1.0 / row_sum) * head_mask(head)
        mixed = mixed * scale
        position = block * 256 + lax.broadcasted_iota(jnp.int32, (256, 1), 0)
        on_heads = jnp.where(onlane < 192, 1.0, 0.0)
        mixed = jnp.where(position < total, mixed, v_ref[rows, :].astype(F32) * on_heads)
        exact_ref[rows, :] = mixed
        mixed_ref[rows, :] = mixed[:, :192].astype(BF)
        lse_ref[rows, :] = lse
        return carry

    lax.fori_loop(0, 4, block_step, 0)


def attend_backward(q_ref, k_ref, v_ref, exact_ref, lse_ref, grad_mixed, q_aug, g_aug, scores_low, dq_acc, dk_acc, dv_acc):
    for head in range(3):
        mask = head_mask(head)

        def augment(block, carry):
            rows = pl.ds(pl.multiple_of(block * 256, 256), 256)
            grads = grad_mixed[rows, :].astype(F32) * mask
            inner = jnp.sum(grads * exact_ref[rows, :], axis=1, keepdims=True)
            lse = lse_ref[rows, :][:, head : head + 1]
            queries = q_ref[rows, :].astype(F32) * (mask + jnp.where(lanes_of() >= 192, 1.0, 0.0))
            for place, part in enumerate(split_three(-lse)):
                queries = queries + part * lane_is(196 + place)
            for place, part in enumerate(split_three(-inner)):
                grads = grads + part * lane_is(196 + place)
            q_aug[rows, :] = queries.astype(BF)
            g_aug[rows, :] = grads.astype(BF)
            return carry

        lax.fori_loop(0, 4, augment, 0)

        def block_step(block, carry):
            rows = pl.ds(pl.multiple_of(block * 256, 256), 256)
            probs = jnp.exp(nt(k_ref[rows, :], q_aug[...]))
            grad_probs = nt(v_ref[rows, :], g_aug[...])
            grad_scores = (probs * grad_probs).astype(BF)
            scores_low[rows, :] = grad_scores
            key_part = nn(grad_scores, q_aug[...]) * mask
            value_part = nn(probs.astype(BF), g_aug[...]) * mask
            if head == 0:
                dk_acc[rows, :] = key_part
                dv_acc[rows, :] = value_part
            else:
                dk_acc[rows, :] += key_part
                dv_acc[rows, :] += value_part
            return carry

        lax.fori_loop(0, 4, block_step, 0)
        query_part = tn(scores_low[...], k_ref[...] * mask.astype(BF)) * 0.125
        if head == 0:
            dq_acc[...] = query_part
        else:
            dq_acc[...] += query_part


def forward_kernel(normed, weight, bias, lengths, q_ref, k_ref, v_ref, mixed_ref, exact_ref, lse_ref):
    attend_forward(normed, weight, bias[...], lengths[...], q_ref, k_ref, v_ref, mixed_ref, exact_ref, lse_ref)


def middle_kernel(
    mixed_in, x_in, d_low, w_out, w_up, w_down, gains, shifts, biases, up_bias,
    block_ref, second_ref, hid_ref, low_ref, sums_ref, mixed_rows, act_ref,
):
    rows = x_in.shape[0]
    for group in range(4):
        mixed_rows[:, group * 192 : (group + 1) * 192] = mixed_in[group]
    hidden = x_in[...].astype(F32) + nn(mixed_rows[...], w_out[...]) + biases[0:1, :]
    unit, inverse, normed = norm_parts(hidden, gains[1:2, :], shifts[1:2, :])
    second = normed.astype(BF)
    second_ref[...] = second
    grad_low = d_low[...]
    down = jnp.zeros((rows, D), F32)
    back = jnp.zeros((rows, D), F32)
    step = 768
    for tile in range(FF // step):
        cut = slice(tile * step, (tile + 1) * step)
        up = nn(second, w_up[:, cut]) + up_bias[:, cut]
        value, slope = gelu_parts(up)
        down += nn(value.astype(BF), w_down[cut, :])
        grad_up = nt(grad_low, w_down[cut, :]) * slope
        back += nt(grad_up.astype(BF), w_up[:, cut])
    block_ref[...] = (hidden + down + biases[1:2, :]).astype(BF)
    grad_block = grad_low.astype(F32)
    grad_hidden = grad_block + norm_back(back, unit, inverse, gains[1:2, :])
    hid_ref[...] = grad_hidden
    low_ref[...] = grad_hidden.astype(BF)
    sums_ref[...] = jnp.zeros_like(sums_ref)
    sums_ref[0:1, :] = jnp.sum(back * unit, axis=0, keepdims=True)
    sums_ref[1:2, :] = jnp.sum(back, axis=0, keepdims=True)
    sums_ref[2:3, :] = jnp.sum(grad_hidden, axis=0, keepdims=True)
    sums_ref[3:4, :] = jnp.sum(grad_block, axis=0, keepdims=True)


def feed_kernel(second, d_low, w_up, w_down, up_bias, up_grad, down_grad, bias_grad, act_ref, grad_ref):
    width = w_up.shape[1]
    bias_grad[...] = jnp.zeros_like(bias_grad)

    def step(block, carry):
        rows = pl.ds(pl.multiple_of(block * 256, 256), 256)
        up = nn(second[rows, :], w_up[...]) + up_bias[...]
        value, slope = gelu_parts(up)
        act_ref[rows, :] = value.astype(BF)
        grad_up = nt(d_low[rows, :], w_down[...]) * slope
        bias_grad[0:1, :] += jnp.sum(grad_up, axis=0, keepdims=True)
        grad_ref[rows, :] = grad_up.astype(BF)
        return carry

    lax.fori_loop(0, 4, step, 0)
    down_grad[...] = tn(d_low[...], act_ref[...]).astype(BF)
    up_grad[...] = tn(grad_ref[...], second[...]).astype(BF)


def backward_kernel(
    grad_low, w_out, normed, mixed, q_ref, k_ref, v_ref, exact_ref, lse_ref,
    grad_ref, out_grad, qkv_grad, bias_grad,
    grad_mixed, q_aug, g_aug, scores_low, dq_acc, dk_acc, dv_acc,
):
    padded = jnp.zeros((64, D), BF)
    weight = jnp.concatenate([w_out[...], padded], axis=0)
    grad_mixed[...] = nt(grad_low[...], weight).astype(BF)
    out_grad[...] = tn(grad_low[...], mixed[...]).astype(BF)
    attend_backward(q_ref, k_ref, v_ref, exact_ref, lse_ref, grad_mixed, q_aug, g_aug, scores_low, dq_acc, dk_acc, dv_acc)
    for place, part in enumerate((dq_acc, dk_acc, dv_acc)):
        grad_ref[:, place * 192 : (place + 1) * 192] = part[:, :192].astype(BF)
    bias_grad[...] = jnp.zeros_like(bias_grad)
    bias_grad[0:1, :] = jnp.sum(grad_ref[...].astype(F32), axis=0, keepdims=True)
    qkv_grad[...] = tn(grad_ref[...], normed[...]).astype(BF)


def last_kernel(grad_in, w_qkv, x_in, hid, gains, shifts, out_ref, sums_ref, grad_rows):
    for part in range(3):
        for group in range(4):
            place = part * D + group * 192
            grad_rows[:, place : place + 192] = grad_in[group][:, part * 192 : (part + 1) * 192]
    grad_first = nt(grad_rows[...], w_qkv[...])
    unit, inverse, _ = norm_parts(x_in[...].astype(F32), gains[0:1, :], shifts[0:1, :])
    out_ref[...] = hid[...] + norm_back(grad_first, unit, inverse, gains[0:1, :])
    sums_ref[...] = jnp.zeros_like(sums_ref)
    sums_ref[0:1, :] = jnp.sum(grad_first * unit, axis=0, keepdims=True)
    sums_ref[1:2, :] = jnp.sum(grad_first, axis=0, keepdims=True)


def whole_call(kernel, outs, scratch=(), name=None):
    return pl.pallas_call(
        kernel,
        out_shape=[jax.ShapeDtypeStruct(*out) for out in outs],
        scratch_shapes=[pltpu.VMEM(*item) for item in scratch],
        compiler_params=pltpu.CompilerParams(vmem_limit_bytes=VMEM_LIMIT),
        name=name,
    )


def general_device(x, norm_gains, norm_shifts, w_qkv, qv_bias, w_out, out_biases, w_up, up_bias, w_down, lengths, d_out):
    groups = lax.axis_size("head")
    shards = lax.axis_size("dp")
    group = lax.axis_index("head")
    rows = x.shape[1]
    own = D // groups
    x = x[0]
    gains = norm_gains.astype(F32)
    shifts = norm_shifts.astype(F32)
    biases = out_biases.astype(F32)
    up_shift = up_bias.astype(F32)
    full_bias = jnp.stack([qv_bias[0], jnp.zeros_like(qv_bias[0]), qv_bias[1]]).astype(F32)

    weight_own = lax.dynamic_index_in_dim(w_qkv.reshape(D, 3, groups, own), group, 2, False)
    weight_own = jnp.pad(weight_own, ((0, 0), (0, 0), (0, 256 - own))).reshape(D, 768)
    bias_own = lax.dynamic_index_in_dim(full_bias.reshape(3, groups, own), group, 1, False)
    bias_own = jnp.pad(bias_own, ((0, 0), (0, 256 - own))).reshape(1, 768)
    out_own = lax.dynamic_slice_in_dim(w_out, group * own, own, 0)
    unit_ff = FF // (shards * groups)
    up_own = lax.dynamic_index_in_dim(w_up.reshape(D, shards, groups, unit_ff), group, 2, False).reshape(D, D)
    down_own = lax.dynamic_index_in_dim(w_down.reshape(shards, groups, unit_ff, D), group, 1, False).reshape(D, D)
    ub_own = lax.dynamic_index_in_dim(up_shift.reshape(shards, groups, unit_ff), group, 1, False).reshape(1, D)

    normed = norm_parts(x.astype(F32), gains[0], shifts[0])[2].astype(BF)
    normed_all = lax.all_gather(normed, "head", axis=0, tiled=True)
    total = jnp.sum(lengths[0])
    position = group * rows + jnp.arange(rows, dtype=jnp.int32)
    d_low = jnp.where((position < total)[:, None], d_out[0], jnp.zeros_like(d_out[0]))
    d_all = lax.all_gather(d_low, "head", axis=0, tiled=True)

    q, k, v, mixed, exact, lse = whole_call(
        forward_kernel,
        [((SLOT, 256), BF)] * 3 + [((SLOT, own), BF), ((SLOT, 256), F32), ((SLOT, 128), F32)],
        name="attend_forward",
    )(normed_all, weight_own, bias_own, lengths)
    mixed_in = lax.all_to_all(mixed.reshape(groups, rows, own), "head", 0, 0, tiled=True)
    block_out, second, hid, hid_low, sums_mid = whole_call(
        middle_kernel,
        [((rows, D), BF), ((rows, D), BF), ((rows, D), F32), ((rows, D), BF), ((8, D), F32)],
        [((rows, D), BF), ((rows, FF), BF)],
        name="middle",
    )(mixed_in, x, d_low, w_out, w_up, w_down, gains, shifts, biases, up_shift.reshape(1, FF))
    second_all = lax.all_gather(second, "head", axis=0, tiled=True)
    low_all = lax.all_gather(hid_low, "head", axis=0, tiled=True)
    up_grad, down_grad, ub_grad = whole_call(
        feed_kernel,
        [((D, D), BF), ((D, D), BF), ((8, D), F32)],
        [((SLOT, D), BF), ((SLOT, D), BF)],
        name="feed",
    )(second_all, d_all, up_own, down_own, ub_own)
    grad_own, out_grad, qkv_grad, qkv_sum = whole_call(
        backward_kernel,
        [((SLOT, 3 * own), BF), ((D, own), BF), ((3 * own, D), BF), ((8, 3 * own), F32)],
        [((SLOT, 256), BF)] * 3 + [((SLOT, SLOT), BF)] + [((SLOT, 256), F32)] * 3,
        name="attend_backward",
    )(low_all, out_own, normed_all, mixed, q, k, v, exact, lse)
    grad_in = lax.all_to_all(grad_own.reshape(groups, rows, 3 * own), "head", 0, 0, tiled=True)
    grad_inputs, sums_last = whole_call(
        last_kernel,
        [((rows, D), F32), ((8, D), F32)],
        [((rows, 3 * D), BF)],
        name="last",
    )(grad_in, w_qkv, x, hid, gains, shifts)

    def scatter(values):
        return lax.psum_scatter(values, "dp", scatter_dimension=0, tiled=True)

    up_part = lax.all_gather(scatter(up_grad), "head", axis=0, tiled=True)
    down_part = lax.all_gather(scatter(down_grad), "head", axis=1, tiled=True)
    out_part = lax.all_gather(scatter(out_grad), "head", axis=1, tiled=True)
    down_out = down_part.astype(F32).T.reshape(groups, shards, unit_ff, D // shards)
    down_out = down_out.transpose(1, 0, 2, 3).reshape(FF, D // shards)
    spread = jnp.zeros((3, groups, own, D), BF)
    spread = lax.dynamic_update_slice(spread, qkv_grad.reshape(3, 1, own, D), (0, group, 0, 0))
    qkv_part = lax.psum(scatter(spread.reshape(3 * D, D)), "head")

    def place_rows(values):
        parts = values.reshape(3, own)
        empty = jnp.zeros((3, groups, own), F32)
        return lax.dynamic_update_slice(empty, parts[:, None], (0, group, 0)).reshape(3, D)

    bias_rows = place_rows(qkv_sum[0])
    ub_rows = lax.dynamic_update_slice(
        jnp.zeros((shards, groups, unit_ff), F32), ub_grad[0].reshape(shards, 1, unit_ff), (0, group, 0)
    ).reshape(4, D)
    small = jnp.concatenate([sums_last[0:2], sums_mid[0:4], bias_rows[0:1], bias_rows[2:3], ub_rows], axis=0)
    small = lax.psum(small, ("dp", "head"))
    shard = lax.axis_index("dp")

    def cut(values):
        width = D // shards
        return lax.dynamic_slice_in_dim(values, shard * width, width, 1)

    ub_out = lax.dynamic_slice_in_dim(small[8:12].reshape(FF), shard * (FF // shards), FF // shards, 0)
    return (
        block_out[None],
        grad_inputs[None],
        cut(jnp.stack([small[0], small[2]])),
        cut(jnp.stack([small[1], small[3]])),
        qkv_part.astype(F32).T,
        cut(small[6:8]),
        out_part.astype(F32).T,
        cut(small[4:6]),
        up_part.astype(F32).T,
        ub_out,
        down_out,
    )


MESH = pl.DeviceIdType.MESH
BLOCK = 256

BUFFERS = (
    ("xv", (256, D), BF),
    ("dv", (256, D), BF),
    ("wqkv", (D, 3 * D), BF),
    ("wout", (D, D), BF),
    ("wup", (D, FF), BF),
    ("big", (3 * SLOT, SLOT), BF),
    ("wqo", (D, D), BF),
    ("wuo", (D, D), BF),
    ("wdo", (D, D), BF),
    ("woo", (256, D), BF),
    ("nall", (SLOT, D), BF),
    ("dall", (SLOT, D), BF),
    ("sall", (SLOT, D), BF),
    ("lall", (SLOT, D), BF),
    ("qb", (SLOT, 256), BF),
    ("kb", (SLOT, 256), BF),
    ("vb", (SLOT, 256), BF),
    ("mix", (SLOT, 256), BF),
    ("exact", (SLOT, 256), F32),
    ("lse", (SLOT, 128), F32),
    ("mixs", (4, 384, 128), BF),
    ("mixin", (4, 384, 128), BF),
    ("gh", (256, D), F32),
    ("act", (SLOT, D), BF),
    ("gup", (SLOT, D), BF),
    ("kin", (4, 384, 128), BF),
    ("vin", (4, 384, 128), BF),
    ("ks_", (4, 384, 128), BF),
    ("vs_", (4, 384, 128), BF),
    ("qs_", (4, 384, 128), BF),
    ("qin", (4, 384, 128), BF),
    ("pdy", (8, 96, 256), BF),
    ("pdz", (8, 96, 512), BF),
    ("pup", (6, D, 128), BF),
    ("pou", (8, 144, 128), BF),
    ("pqk", (12, 48, D), BF),
    ("ydy", (4, 96, 256), BF),
    ("ydz", (1, 96, 512), BF),
    ("yup", (6, D, 128), BF),
    ("you", (4, 144, 128), BF),
    ("yqk", (12, 48, D), BF),
    ("zdy", (4, 96, 256), BF),
    ("zdz", (4, 2, 96, 512), BF),
    ("zup", (12, D, 128), BF),
    ("zou", (4, 144, 128), BF),
    ("zqk", (24, 48, D), BF),
    ("vec", (8, D), F32),
    ("bias_rows", (24, 128), F32),
    ("small", (2, 4, 16, 128), F32),
    ("ysm", (4, 16, 128), F32),
    ("zsm", (4, 16, 128), F32),
    ("fsm", (4, 2, 4, 16, 128), F32),
    ("last", (4, 16, 128), F32),
    ("lasty", (2, 8, 128), F32),
    ("lastz", (5, 8, 128), F32),
    ("lastf", (8, 128), F32),
)
SEMAPHORES = (
    ("load", 22), ("give", 8),
    ("ns", 5), ("nr", 5), ("ds", 5), ("dr", 5), ("ss", 5), ("sr", 5), ("ls", 5), ("lr", 5),
    ("ms", 3), ("mr", 3), ("ks", 3), ("kr", 3), ("vs", 3), ("vr", 3), ("qs", 3), ("qr", 3),
    ("ydys", 4), ("ydyr", 4), ("zdys", 4), ("zdyr", 4), ("fdys", 3), ("fdyr", 3),
    ("ydzs", 1), ("ydzr", 1), ("zdzs", 4), ("zdzr", 4), ("fdzs", 3), ("fdzr", 3),
    ("yous", 4), ("your", 4), ("zous", 4), ("zour", 4), ("fous", 3), ("four", 3),
    ("yups", 6), ("yupr", 6), ("zups", 6), ("zupr", 12), ("fups", 9), ("fupr", 9),
    ("yqks", 12), ("yqkr", 12), ("zqks", 12), ("zqkr", 24), ("fqks", 18), ("fqkr", 18),
    ("ysms", 1), ("ysmr", 1), ("zsms", 4), ("zsmr", 4), ("fsms", 3), ("fsmr", 3),
    ("las", 3), ("lar", 3), ("lays", 1), ("layr", 1), ("lazs", 4), ("lazr", 4),
)
INPUTS = ("x", "gains", "shifts", "w_qkv", "qv_bias", "w_out", "biases", "w_up", "up_bias", "w_down", "lengths", "d_out")
IN_PLACE = ("x", "w_qkv", "w_out", "w_up", "w_down", "d_out")
OUTPUTS = (
    ("block_out", (256, D), BF),
    ("grad_inputs", (256, D), F32),
    ("fup", (3, D, 128), BF),
    ("fqk", (6, 48, D), BF),
    ("fdy", (4, 96, 256), BF),
    ("fdz", (4, 96, 512), BF),
    ("fou", (4, 144, 128), BF),
    ("fsum", (16, 128), F32),
)


class Refs:
    pass


def block_rows(block, size=BLOCK, offset=0):
    return pl.ds(pl.multiple_of(block * BLOCK + offset, 128), size)


def one_kernel(*args):
    r = Refs()
    names = [*INPUTS] + ["to_" + o[0] for o in OUTPUTS] + [b[0] for b in OUTPUTS + BUFFERS] + [s[0] for s in SEMAPHORES]
    for name, ref in zip(names, args, strict=True):
        setattr(r, name, ref)
    dp, head = lax.axis_index("dp"), lax.axis_index("head")
    z, y = lax.div(dp, 2), lax.rem(dp, 2)
    px, pc = lax.div(head, 2), lax.rem(head, 2)

    def peer(code):
        return lax.rem(px + (code // 2 if isinstance(code, int) else lax.div(code, 2)), 2) * 2 + lax.rem(
            pc + (code % 2 if isinstance(code, int) else lax.rem(code, 2)), 2
        )

    sib, far, diag = peer(1), peer(2), peer(3)
    other_y = z * 2 + (1 - y)

    def z_shard(k):
        return lax.rem(z + k, 4)

    half = lax.div(z, 2)
    inner = (z == 1) | (z == 2)
    outer = (z == 0) | (z == 3)
    beside = half * 2 + 1 - lax.rem(z, 2)
    z_order = (3 * (1 - half), 2 - half, beside, z)

    sent = []

    def push(src, dst, send, recv, to):
        return pltpu.make_async_remote_copy(
            src_ref=src, dst_ref=dst, send_sem=send, recv_sem=recv, device_id=to, device_id_type=MESH
        )

    def when(cond, body):
        if cond is None:
            body()
        else:
            pl.when(cond)(body)

    given = []

    def give(name):
        copy = pltpu.make_async_copy(getattr(r, name), getattr(r, "to_" + name), r.give.at[len(given)])
        copy.start()
        given.append(copy)

    def start(make, cond=None):
        when(cond, lambda: make().start())
        sent.append((make, cond))

    loads = {}

    def load(name, src, dst):
        loads.setdefault(name, []).append(pltpu.make_async_copy(src, dst, r.load.at[sum(map(len, loads.values()))]))

    load("x", r.x, r.xv)
    load("d", r.d_out, r.dv)
    load("wqkv", r.w_qkv, r.wqkv)
    load("wout", r.w_out, r.wout)
    load("wup", r.w_up, r.wup)
    load("wdown", r.w_down, r.big.at[:, 0:D])
    load("woo", r.w_out.at[pl.ds(pl.multiple_of(head * 192, 64), 192), :], r.woo.at[0:192, :])
    for j in range(6):
        unit = pl.ds(pl.multiple_of((4 * j + head) * 128, 128), 128)
        load("wuo", r.w_up.at[:, unit], r.wuo.at[:, j * 128 : (j + 1) * 128])
        load("wdo", r.w_down.at[unit, :], r.wdo.at[j * 128 : (j + 1) * 128, :])
    for copies in loads.values():
        for copy in copies:
            copy.start()

    def loaded(name):
        for copy in loads[name]:
            copy.wait()

    barrier = pltpu.get_barrier_semaphore()
    for to in [(dp, sib), (dp, far), (dp, diag), (other_y, head)] + [(z_shard(k) * 2 + y, head) for k in (1, 2, 3)]:
        pl.semaphore_signal(barrier, inc=1, device_id=to, device_id_type=MESH)

    gains = r.gains[...].astype(F32)
    shifts = r.shifts[...].astype(F32)
    biases = r.biases[...].astype(F32)
    onlane = lanes_of()
    lengths = r.lengths[...]
    whole = lengths[:, 0:1] == SLOT
    total = jnp.sum(lengths, axis=1, keepdims=True)

    def piece_rows(block, offset, size):
        return pl.ds(pl.multiple_of(block * BLOCK + offset, 32), size)

    def gather(buf, send, recv, cut=128):
        pieces = ((0, cut), (cut, BLOCK - cut))

        def copy_of(index):
            if index == 0:
                rows, to = block_rows(head), sib
            elif index < 3:
                rows, to = piece_rows(head, *pieces[index - 1]), far
            else:
                rows, to = piece_rows(far, *pieces[index - 3]), sib
            return push(buf.at[rows, :], buf.at[rows, :], send.at[index], recv.at[index], (dp, to))

        def begin(these=(1, 2, 0)):
            for index in these:
                copy_of(index).start()

        def wait(index):
            copy_of(index).wait_recv()

        def relay(these=(1, 2)):
            for index in these:
                wait(index)
                copy_of(index + 2).start()

        def rest():
            for index in (3, 4):
                wait(index)

        def drain():
            for index in range(5):
                copy_of(index).wait_send()

        return begin, wait, relay, rest, drain

    n_begin, n_wait, n_relay, n_rest, n_drain = gather(r.nall, r.ns, r.nr)
    d_begin, d_wait, d_relay, d_rest, d_drain = gather(r.dall, r.ds, r.dr, 160)
    s_begin, s_wait, s_relay, s_rest, s_drain = gather(r.sall, r.ss, r.sr)
    l_begin, l_wait, l_relay, l_rest, l_drain = gather(r.lall, r.ls, r.lr)

    loaded("x")
    first = norm_parts(r.xv[...].astype(F32), gains[0:1, :], shifts[0:1, :])[2]
    r.nall[block_rows(head), :] = first.astype(BF)
    pl.semaphore_wait(barrier, 7)
    n_begin()
    position = head * BLOCK + lax.broadcasted_iota(jnp.int32, (BLOCK, 1), 0)
    loaded("d")
    r.dall[block_rows(head), :] = (r.dv[...].astype(F32) * jnp.where(position < total, 1.0, 0.0)).astype(BF)
    d_begin((1, 0))
    loaded("wqkv")
    aligned = lax.div(3 * head, 2) * 128
    odd = jnp.where(lax.rem(head, 2) == 1, 1.0, 0.0)
    on_heads = jnp.where(onlane < 192, 1.0, 0.0)

    def own_window(values):
        moved = pltpu.roll(values, 192, 1)
        return (values * (1.0 - odd) + moved * odd) * on_heads

    r.vec[0:2, :] = r.qv_bias[...].astype(F32)
    pair_bias = own_window(r.vec[:, pl.ds(pl.multiple_of(aligned, 128), 256)])
    bias = jnp.concatenate([pair_bias[0:1], jnp.zeros((1, 256), F32), pair_bias[1:2]], axis=1)
    for part in range(3):
        window = pl.ds(pl.multiple_of(part * D + aligned, 128), 256)
        r.wqo[:, part * 256 : (part + 1) * 256] = own_window(r.wqkv[:, window].astype(F32)).astype(BF)

    aux_k = jnp.where((onlane >= 196) & (onlane < 199), 1.0, 0.0)
    aux_v = jnp.where((onlane >= 192) & (onlane < 199) & (onlane != 195), 1.0, 0.0)
    on_aux = jnp.where(onlane >= 192, 1.0, 0.0)

    def project(block):
        rows = block_rows(block)
        projected = (nn(r.nall[rows, :], r.wqo[...]) + bias).astype(BF).astype(F32)
        r.qb[rows, :] = (projected[:, :256] * 0.125 + lane_is(192 + block)).astype(BF)
        off = jnp.where((onlane >= 192) & (onlane < 196) & (onlane != 192 + block), 1.0, 0.0)
        r.kb[rows, :] = (projected[:, 256:512] + (aux_k + off * jnp.where(whole, 0.0, FAR))).astype(BF)
        r.vb[rows, :] = (projected[:, 512:] + aux_v).astype(BF)

    project(head)
    n_wait(0)
    project(sib)
    n_relay()
    project(far)
    n_rest()
    project(diag)

    def packed(values):
        third = values[:, 128:]
        return jnp.concatenate([values[:, :128], third[:128] + pltpu.roll(third[128:], 64, 1)], axis=0).astype(BF)

    def unpack(source, dst, base):
        for group in range(4):
            lane = group * 192
            dst[base : base + 256, lane : lane + 128] = source[group, 0:256, :]
            dst[base : base + 128, lane + 128 : lane + 192] = source[group, 256:384, 0:64]
            dst[base + 128 : base + 256, lane + 128 : lane + 192] = source[group, 256:384, 64:128]

    def mix_copy(code):
        return push(r.mixs.at[code], r.mixin.at[head], r.ms.at[code - 1], r.mr.at[code - 1], (dp, peer(code)))

    small_lane = lax.broadcasted_iota(jnp.int32, (1, 128), 1)

    def attend(step, carry):
        code = 3 - step
        block = peer(code)
        rows = block_rows(block)
        queries = r.qb[rows, :]
        mixed = jnp.zeros((BLOCK, 256), F32)
        tops = []
        for n in range(3):
            scores = nt(queries * (head_mask(n) + on_aux).astype(BF), r.kb[...])
            top = jnp.max(scores, axis=1, keepdims=True)
            weights = jnp.exp(scores - top).astype(BF)
            mixed += nn(weights, r.vb[...] * (head_mask(n) + lane_is(192 + n)).astype(BF))
            tops.append(top)
        lse = jnp.zeros((BLOCK, 128), F32)
        scale = jnp.zeros((BLOCK, 256), F32)
        for n in range(3):
            row_sum = jnp.sum(mixed * lane_is(192 + n), axis=1, keepdims=True)
            lse += (tops[n] + jnp.log(row_sum)) * jnp.where(small_lane == n, 1.0, 0.0)
            scale += (1.0 / row_sum) * head_mask(n)
        place = block * BLOCK + lax.broadcasted_iota(jnp.int32, (BLOCK, 1), 0)
        mixed = jnp.where(place < total, mixed * scale, r.vb[rows, :].astype(F32) * on_heads)
        r.exact[rows, :] = mixed
        r.lse[rows, :] = lse
        r.mix[rows, :] = mixed.astype(BF)
        r.mixs[code] = packed(mixed)

        @pl.when(step < 3)
        def _():
            mix_copy(code).start()

        @pl.when(step == 1)
        def _():
            d_begin((2,))

        return carry

    lax.fori_loop(0, 4, attend, 0)
    r.mixin[head] = r.mixs[0]
    d_relay((1,))

    loaded("wout")
    loaded("wup")
    loaded("wdown")
    for code in (3, 2, 1):
        mix_copy(code).wait_recv()
    unpack(r.mixin, r.wqo, 0)
    hidden = r.xv[...].astype(F32) + nn(r.wqo[0:256, :], r.wout[...]) + biases[0:1, :]
    unit, inverse, normed = norm_parts(hidden, gains[1:2, :], shifts[1:2, :])
    second = normed.astype(BF)
    r.sall[block_rows(head), :] = second
    s_begin()
    grad_low = r.dall[block_rows(head), :]
    up_bias = r.up_bias[...].astype(F32)
    r.bias_rows[...] = up_bias
    down = jnp.zeros((BLOCK, D), F32)
    back = jnp.zeros((BLOCK, D), F32)
    for tile in range(4):
        cut = slice(tile * D, (tile + 1) * D)
        up = nn(second, r.wup[:, cut]) + jnp.concatenate([up_bias[6 * tile + i : 6 * tile + i + 1] for i in range(6)], axis=1)
        value, slope = gelu_parts(up)
        w_down = r.big[cut, 0:D]
        down += nn(value.astype(BF), w_down)
        grad_up = nt(grad_low, w_down) * slope
        back += nt(grad_up.astype(BF), r.wup[:, cut])
    r.block_out[...] = (hidden + down + biases[1:2, :]).astype(BF)
    give("block_out")
    grad_block = grad_low.astype(F32)
    grad_hidden = grad_block + norm_back(back, unit, inverse, gains[1:2, :])
    r.gh[...] = grad_hidden
    r.lall[block_rows(head), :] = grad_hidden.astype(BF)
    l_begin()
    r.vec[...] = jnp.zeros_like(r.vec)
    r.vec[1:2, :] = jnp.sum(back * unit, axis=0, keepdims=True)
    r.vec[3:4, :] = jnp.sum(back, axis=0, keepdims=True)
    r.vec[6:7, :] = jnp.sum(grad_hidden, axis=0, keepdims=True)
    r.vec[7:8, :] = jnp.sum(grad_block, axis=0, keepdims=True)

    loaded("wuo")
    loaded("wdo")
    loaded("woo")
    own_bias = jnp.concatenate([r.bias_rows[pl.ds(4 * j + head, 1), :] for j in range(6)], axis=1)

    def feed(step, sums):
        @pl.when(step == 1)
        def _():
            d_wait(0)
            s_wait(0)

        @pl.when(step == 2)
        def _():
            d_relay((2,))
            s_relay()

        @pl.when(step == 3)
        def _():
            d_rest()
            s_rest()

        rows = block_rows(peer(step))
        up = nn(r.sall[rows, :], r.wuo[...]) + own_bias
        value, slope = gelu_parts(up)
        r.act[rows, :] = value.astype(BF)
        grad_up = nt(r.dall[rows, :], r.wdo[...]) * slope
        r.gup[rows, :] = grad_up.astype(BF)
        return sums + jnp.sum(grad_up, axis=0, keepdims=True)

    sums = lax.fori_loop(0, 4, feed, jnp.zeros((1, D), F32))
    def parts_of(name):
        refs = [getattr(r, part + name) for part in ("p", "y", "z", "f")]
        return refs + [getattr(r, part + name + end) for part in ("y", "z", "f") for end in ("s", "r")]

    def finals(fin, fs, fr):
        def f_copy(code):
            place = far if code == 3 else head
            to = far if code == 2 else sib
            return push(fin.at[place], fin.at[place], fs.at[code - 1], fr.at[code - 1], (dp, to))

        def begin():
            for code in (2, 1):
                start(lambda code=code: f_copy(code))

        def relay():
            f_copy(2).wait_recv()
            start(lambda: f_copy(3))

        def rest():
            f_copy(1).wait_recv()
            f_copy(3).wait_recv()

        return begin, relay, rest

    def add_to(ref, at, more):
        ref[at] = (ref[at].astype(F32) + more.astype(F32)).astype(BF)

    def y_first(name):
        own, ybuf, zbuf, fin, ys, yr, zs, zr, fs, fr = parts_of(name)
        f_begin, relay, rest = finals(fin, fs, fr)

        def y_copy(t):
            src = own.at[z_order[t] * 2 + (1 - y)]
            return push(src, ybuf.at[t], ys.at[t], yr.at[t], (other_y, head))

        def near_copy(t):
            return push(own.at[z_order[t] * 2 + y], zbuf.at[t], zs.at[t], zr.at[t], (beside * 2 + y, head))

        def across_copy(t):
            shard = z_order[t] * 2 + y
            return push(own.at[shard], zbuf.at[3], zs.at[t], zr.at[3], (shard, head))

        def begin():
            for t in range(4):
                start(lambda t=t: y_copy(t))

        def pair(t):
            y_copy(t).wait_recv()
            add_to(own, z_order[t] * 2 + y, ybuf[t])
            if t == 2:
                near_copy(t).start()
            elif t < 2:
                pl.when(outer)(lambda: near_copy(t).start())

        def fold(t):
            @pl.when(inner)
            def _():
                near_copy(t).wait_recv()
                add_to(own, z_order[t] * 2 + y, zbuf[t])
                across_copy(t).start()

        def total_up():
            near_copy(2).wait_recv()
            across_copy(0).wait_recv()
            fin[head] = (own[dp].astype(F32) + zbuf[2].astype(F32) + zbuf[3].astype(F32)).astype(BF)
            f_begin()
            sent.append((lambda: near_copy(2), None))
            for t in (0, 1):
                sent.append((lambda t=t: near_copy(t), outer))
                sent.append((lambda t=t: across_copy(t), inner))

        return begin, pair, fold, total_up, relay, rest

    def z_first(name):
        own, ybuf, zbuf, fin, ys, yr, zs, zr, fs, fr = parts_of(name)
        f_begin, relay, rest = finals(fin, fs, fr)

        def both(t):
            return pl.ds(z_order[t] * 2, 2)

        def near_copy(t):
            return push(own.at[both(t)], zbuf.at[t], zs.at[t], zr.at[t], (beside * 2 + y, head))

        def across_copy(t):
            return push(own.at[both(t)], zbuf.at[3], zs.at[t], zr.at[3], (z_order[t] * 2 + y, head))

        def y_copy():
            return push(own.at[z * 2 + (1 - y)], ybuf.at[0], ys.at[0], yr.at[0], (other_y, head))

        def begin():
            for t in (0, 1):
                start(lambda t=t: near_copy(t), outer)
            start(lambda: near_copy(2))

        def fold(t):
            @pl.when(inner)
            def _():
                near_copy(t).wait_recv()
                add_to(own, both(t), zbuf[t])
                across_copy(t).start()

        def pair():
            near_copy(2).wait_recv()
            across_copy(0).wait_recv()
            add_to(own, both(3), zbuf[2].astype(F32) + zbuf[3].astype(F32))
            y_copy().start()

        def total_up():
            y_copy().wait_recv()
            fin[head] = (own[dp].astype(F32) + ybuf[0].astype(F32)).astype(BF)
            f_begin()
            for t in (0, 1):
                sent.append((lambda t=t: across_copy(t), inner))
            sent.append((y_copy, None))

        return begin, fold, pair, total_up, relay, rest

    def irregular(name, count, per_shard, number_of, owner_of):
        own, ybuf, zbuf, fin, ys, yr, zs, zr, fs, fr = parts_of(name)

        def facts(j):
            number = number_of(j)
            shard = lax.div(number, per_shard)
            return shard, lax.div(shard, 2), lax.rem(shard, 2), lax.rem(number, per_shard)

        def y_copy(j):
            return push(own.at[j], ybuf.at[j], ys.at[j], yr.at[j], (other_y, head))

        def near_copy(j):
            slot = jnp.where(facts(j)[1] == beside, count + facts(j)[3], j)
            return push(own.at[j], zbuf.at[slot], zs.at[j], zr.at[slot], (beside * 2 + y, head))

        def near_arrival(j):
            return push(own.at[j], zbuf.at[j], zs.at[j], zr.at[j], (beside * 2 + y, head))

        def across_copy(j):
            shard, _, _, place = facts(j)
            return push(own.at[j], zbuf.at[count + per_shard + place], zs.at[j], zr.at[count + per_shard + place], (shard, head))

        def last_arrival(j, base):
            place = base + facts(j)[3]
            return push(own.at[j], zbuf.at[place], zs.at[j], zr.at[place], (dp, sib)), place

        def f_copy(code, place):
            index = (code - 1) * per_shard + place
            to = far if code == 2 else sib
            return push(fin.at[place], fin.at[place], fs.at[index], fr.at[index], (dp, to))

        def begin(these=range(count)):
            for j in these:
                start(lambda j=j: y_copy(j), facts(j)[2] != y)

        def mine(j):
            return facts(j)[2] == y

        def other_half(j):
            return lax.div(facts(j)[1], 2) != half

        def to_near(j):
            return mine(j) & ((facts(j)[1] == beside) | (other_half(j) & outer))

        def to_across(j):
            return mine(j) & other_half(j) & inner

        def fold(j):
            @pl.when(to_across(j))
            def _():
                near_arrival(j).wait_recv()
                add_to(own, j, zbuf[j])
                across_copy(j).start()

        def pair(j):
            @pl.when(mine(j))
            def _():
                y_copy(j).wait_recv()
                add_to(own, j, ybuf[j])

            pl.when(to_near(j))(lambda: near_copy(j).start())

        def total_up(these=range(count)):
            for j in these:
                sent.append((lambda j=j: near_copy(j), to_near(j)))
                sent.append((lambda j=j: across_copy(j), to_across(j)))
                shard, _, _, place = facts(j)

                def body(j=j, place=place):
                    value = own[j].astype(F32)
                    for base in (count, count + per_shard):
                        copy, slot = last_arrival(j, base)
                        copy.wait_recv()
                        value += zbuf[slot].astype(F32)
                    fin[place] = value.astype(BF)
                    f_copy(2, place).start()
                    f_copy(1, place).start()

                pl.when(shard == dp)(body)

        def relay():
            for place in range(per_shard):
                owner = owner_of(per_shard * dp + place)
                for code in (1, 2):
                    sent.append((lambda code=code, place=place: f_copy(code, place), owner == head))

                def body(place=place):
                    f_copy(2, place).wait_recv()
                    f_copy(3, place).start()

                pl.when(owner == far)(body)
                sent.append((lambda place=place: f_copy(3, place), owner == far))

        def rest():
            for place in range(per_shard):
                owner = owner_of(per_shard * dp + place)
                for code, source in ((1, sib), (3, diag)):
                    pl.when(owner == source)(lambda code=code, place=place: f_copy(code, place).wait_recv())

        return begin, pair, fold, total_up, relay, rest

    dy_begin, dy_pair, dy_fold, dy_total, dy_relay, dy_rest = y_first("dy")
    dz_begin, dz_fold, dz_pair, dz_total, dz_relay, dz_rest = z_first("dz")
    ou_begin, ou_pair, ou_fold, ou_total, ou_relay, ou_rest = y_first("ou")
    up_begin, up_pair, up_fold, up_total, up_relay, up_rest = irregular(
        "up", 6, 3, lambda j: 4 * j + head, lambda number: lax.rem(number, 4)
    )
    qk_begin, qk_pair, qk_fold, qk_total, qk_relay, qk_rest = irregular(
        "qk",
        12,
        6,
        lambda j: ((j // 4) * 8 + 2 * head + j // 2 % 2) * 2 + j % 2,
        lambda number: lax.div(lax.rem(lax.div(number, 2), 8), 2),
    )

    r.pdz[...] = tn(r.dall[...], r.act[:, 256:]).astype(BF).reshape(8, 96, 512)
    dz_begin()
    r.pdy[...] = tn(r.dall[...], r.act[:, :256]).astype(BF).reshape(8, 96, 256)
    dy_begin()
    up_grad = tn(r.sall[...], r.gup[...]).astype(BF)
    for j in range(6):
        r.pup[j] = up_grad[:, j * 128 : (j + 1) * 128]
    up_begin()

    r.fsm[head] = jnp.zeros((2, 4, 16, 128), F32)
    for j in range(6):
        number = 4 * j + head
        shard = lax.div(number, 3)
        r.fsm[head, lax.rem(shard, 2), lax.div(shard, 2), pl.ds(8 + lax.rem(number, 3), 1), :] = sums[
            :, j * 128 : (j + 1) * 128
        ]

    q_aug, g_aug = r.act, r.gup
    tile_lane = lanes_of(128)
    spot_row, spot_lane = (lax.broadcasted_iota(jnp.int32, (128, 128), axis) for axis in (0, 1))
    spots = [
        jnp.where((spot_lane == 68 + lax.div(spot_row, 3)) & (lax.rem(spot_row, 3) == n) & (spot_row < 9), 1.0, 0.0)
        for n in range(3)
    ]
    spots = [spot.astype(BF) for spot in spots]

    def aux_of(columns):
        high, middle, low = split_three(columns)
        return (high + pltpu.roll(middle, 3, 1) + pltpu.roll(low, 6, 1)).astype(BF)

    def write_aug(dst, rows, source, aux, keep):
        left = source[:, :128]
        right = source[:, 128:].astype(F32)
        for n in range(3):
            if n < 2:
                part = left * jnp.where(lax.div(tile_lane, 64) == n, 1.0, 0.0).astype(BF)
            else:
                part = jnp.zeros((256, 128), BF)
            dst[rows, n * 256 : n * 256 + 128] = part
            mask = jnp.where(tile_lane < 64, 1.0 if n == 2 else 0.0, keep)
            dst[rows, n * 256 + 128 : (n + 1) * 256] = (right * mask + nn(aux, spots[n])).astype(BF)

    def augment_q(block, carry):
        rows = pl.ds(pl.multiple_of(block * 256, 256), 256)
        write_aug(q_aug, rows, r.qb[rows, :], aux_of(-r.lse[rows, :]), 1.0)
        return carry

    lax.fori_loop(0, 4, augment_q, 0)
    sum_row, sum_lane = (lax.broadcasted_iota(jnp.int32, (256, 128), axis) for axis in (0, 1))
    head_sums = jnp.where((lax.div(sum_row, 64) == sum_lane) & (sum_row < 192), 1.0, 0.0).astype(BF)
    r.woo[192:256, :] = jnp.zeros((64, D), BF)
    l_relay((1,))
    dy_pair(0)
    dy_pair(1)
    s_drain()
    d_drain()
    dv, dq, dk = (r.sall.at[:, part * 256 : (part + 1) * 256] for part in range(3))
    gm = r.dall.at[:, 0:256]
    l_wait(0)
    l_relay((2,))
    dz_fold(0)
    dy_pair(2)
    dy_pair(3)
    l_rest()
    gm[...] = nt(r.lall[...], r.woo[...]).astype(BF)

    out_grad = tn(r.lall[...], r.mix[...]).reshape(8, 96, 256)
    r.pou[:, 0:96, :] = out_grad[:, :, :128].astype(BF)
    third = out_grad[:, :, 128:].reshape(8, 2, 48, 128)
    moved = pltpu.roll(third[:, 1].reshape(384, 128), 64, 1).reshape(8, 48, 128)
    r.pou[:, 96:144, :] = (third[:, 0] + moved).astype(BF)
    ou_begin()

    def augment_g(block, carry):
        rows = pl.ds(pl.multiple_of(block * 256, 256), 256)
        grads = gm[rows, :]
        product = grads.astype(F32) * r.exact[rows, :]
        inner = jnp.zeros((256, 128), F32)
        for part in split_three(product):
            inner += nn(part.astype(BF), head_sums)
        write_aug(g_aug, rows, grads, aux_of(-inner), 0.0)
        return carry

    lax.fori_loop(0, 4, augment_g, 0)
    dz_fold(1)

    def k_copy(code):
        return push(r.ks_.at[code], r.kin.at[head], r.ks.at[code - 1], r.kr.at[code - 1], (dp, peer(code)))

    def v_copy(code):
        return push(r.vs_.at[code], r.vin.at[head], r.vs.at[code - 1], r.vr.at[code - 1], (dp, peer(code)))

    def q_copy(code):
        return push(r.qs_.at[code], r.qin.at[head], r.qs.at[code - 1], r.qr.at[code - 1], (dp, peer(code)))

    def attend_back(step, carry):
        code = 3 - step
        block = peer(code)
        rows = block_rows(block)
        value_grad = jnp.zeros((BLOCK, 256), F32)
        for n in range(3):
            mask = head_mask(n)
            lanes = slice(n * 256, (n + 1) * 256)
            probs = jnp.exp(nt(r.kb[rows, :], q_aug[:, lanes]))
            grad_scores = (probs * nt(r.vb[rows, :], g_aug[:, lanes])).astype(BF)
            r.big[pl.ds(pl.multiple_of(n * SLOT + block * BLOCK, 256), BLOCK), :] = grad_scores
            value_grad += nn(probs.astype(BF), g_aug[:, lanes]) * mask
        dv[rows, :] = value_grad.astype(BF)
        r.vs_[code] = packed(value_grad)

        @pl.when(step < 3)
        def _():
            v_copy(code).start()

        @pl.when(step == 2)
        def _():
            dz_pair()
            dy_fold(0)
            up_pair(0)
            up_pair(1)

        @pl.when(step == 3)
        def _():
            dy_fold(1)
            up_pair(2)

        return carry

    lax.fori_loop(0, 4, attend_back, 0)
    r.vin[head] = r.vs_[0]
    r.pqk[8:12] = tn(dv[...], r.nall[...])[:192].astype(BF).reshape(4, 48, D)
    qk_begin(range(8, 12))
    up_pair(3)

    def query_back(step, carry):
        code = 3 - step
        block = peer(code)
        rows = block_rows(block)
        query_grad = jnp.zeros((BLOCK, 256), F32)
        for n in range(3):
            part = r.big[n * SLOT : (n + 1) * SLOT, pl.ds(pl.multiple_of(block * BLOCK, 256), BLOCK)]
            query_grad += tn(part, r.kb[...] * head_mask(n).astype(BF))
        query_grad = query_grad * 0.125
        dq[rows, :] = query_grad.astype(BF)
        r.qs_[code] = packed(query_grad)

        @pl.when(step < 3)
        def _():
            q_copy(code).start()

        return carry

    lax.fori_loop(0, 4, query_back, 0)
    r.qin[head] = r.qs_[0]
    r.pqk[0:4] = tn(dq[...], r.nall[...])[:192].astype(BF).reshape(4, 48, D)
    qk_begin(range(4))
    up_pair(4)
    up_pair(5)

    def key_back(step, carry):
        code = 3 - step
        block = peer(code)
        rows = block_rows(block)
        key_grad = jnp.zeros((BLOCK, 256), F32)
        for n in range(3):
            part = r.big[pl.ds(pl.multiple_of(n * SLOT + block * BLOCK, 256), BLOCK), :]
            key_grad += nn(part, q_aug[:, n * 256 : (n + 1) * 256]) * head_mask(n)
        dk[rows, :] = key_grad.astype(BF)
        r.ks_[code] = packed(key_grad)

        @pl.when(step < 3)
        def _():
            k_copy(code).start()

        return carry

    lax.fori_loop(0, 4, key_back, 0)
    r.kin[head] = r.ks_[0]
    r.pqk[4:8] = tn(dk[...], r.nall[...])[:192].astype(BF).reshape(4, 48, D)
    qk_begin(range(4, 8))
    query_sum = jnp.sum(dq[...].astype(F32), axis=0, keepdims=True)
    value_sum = jnp.sum(dv[...].astype(F32), axis=0, keepdims=True)
    for group in range(4):
        mine = jnp.where(head == group, 1.0, 0.0)
        r.vec[4:5, group * 192 : (group + 1) * 192] = query_sum[:, :192] * mine
        r.vec[5:6, group * 192 : (group + 1) * 192] = value_sum[:, :192] * mine
    for shard in range(8):
        r.fsm[head, shard % 2, shard // 2, 0:8, 0:96] = r.vec[:, shard * 96 : (shard + 1) * 96]

    def small_y():
        return push(r.small.at[1 - y], r.ysm, r.ysms.at[0], r.ysmr.at[0], (other_y, head))

    def small_z(k):
        return push(
            r.small.at[y, z_shard(k)], r.zsm.at[k], r.zsms.at[k], r.zsmr.at[k], (z_shard(k) * 2 + y, head)
        )

    def small_f(code):
        return push(r.fsm.at[head], r.fsm.at[head], r.fsms.at[code - 1], r.fsmr.at[code - 1], (dp, peer(code)))

    for code in (2, 3, 1):
        start(lambda code=code: small_f(code))
    for t in range(4):
        ou_pair(t)
    for j in range(8, 12):
        qk_pair(j)
    for j in range(6):
        up_fold(j)
    dy_total()
    dz_total()
    for j in range(4):
        qk_pair(j)

    for code in (3, 2, 1):
        k_copy(code).wait_recv()
        v_copy(code).wait_recv()
        q_copy(code).wait_recv()
    unpack(r.qin, r.wuo, 0)
    unpack(r.kin, r.wuo, 256)
    unpack(r.vin, r.wuo, 512)
    grad_first = nt(r.wuo[0:256, :], r.wqkv[:, 0:D])
    grad_first += nt(r.wuo[256:512, :], r.wqkv[:, D : 2 * D])
    grad_first += nt(r.wuo[512:768, :], r.wqkv[:, 2 * D :])
    ou_fold(0)
    ou_fold(1)
    for code in (1, 2, 3):
        small_f(code).wait_recv()
    r.small[...] = r.fsm[0] + r.fsm[1] + r.fsm[2] + r.fsm[3]
    start(small_y)
    for j in range(8, 12):
        qk_fold(j)
    unit, inverse, _ = norm_parts(r.xv[...].astype(F32), gains[0:1, :], shifts[0:1, :])
    r.grad_inputs[...] = r.gh[...] + norm_back(grad_first, unit, inverse, gains[0:1, :])
    give("grad_inputs")
    pair = jnp.concatenate(
        [jnp.sum(grad_first * unit, axis=0, keepdims=True), jnp.sum(grad_first, axis=0, keepdims=True)], axis=0
    )
    r.last[head] = jnp.zeros((16, 128), F32)
    for shard in range(8):
        at = shard % 2 * 8 + shard // 2 * 2
        r.last[head, at : at + 2, 0:96] = pair[:, shard * 96 : (shard + 1) * 96]

    def last_head(code):
        return push(r.last.at[head], r.last.at[head], r.las.at[code - 1], r.lar.at[code - 1], (dp, peer(code)))

    def last_y():
        return push(r.lasty.at[1 - y], r.lastz.at[4], r.lays.at[0], r.layr.at[0], (other_y, head))

    def last_z(k):
        return push(r.lastz.at[0], r.lastz.at[k], r.lazs.at[k], r.lazr.at[k], (z_shard(k) * 2 + y, head))

    for code in (2, 3, 1):
        start(lambda code=code: last_head(code))
    for j in range(4, 8):
        qk_pair(j)
    up_total()
    for j in range(4):
        qk_fold(j)
    small_y().wait_recv()
    r.small[y] = r.small[y] + r.ysm[...]
    for k in (1, 2, 3):
        start(lambda k=k: small_z(k))
    for code in (1, 2, 3):
        last_head(code).wait_recv()
    over_head = r.last[0] + r.last[1] + r.last[2] + r.last[3]
    r.lasty[0] = over_head[0:8]
    r.lasty[1] = over_head[8:16]
    start(last_y)
    dy_relay()
    dz_relay()
    for j in range(4, 8):
        qk_fold(j)
    ou_total()
    qk_total(range(8, 12))
    last_y().wait_recv()
    r.lastz[0] = r.lasty[y] + r.lastz[4]
    for k in (1, 2, 3):
        start(lambda k=k: last_z(k))
    qk_total(range(4))
    up_relay()
    ou_relay()
    qk_total(range(4, 8))
    for k in (1, 2, 3):
        last_z(k).wait_recv()
    dy_rest()
    give("fdy")
    dz_rest()
    give("fdz")
    qk_relay()
    up_rest()
    give("fup")
    ou_rest()
    give("fou")
    qk_rest()
    give("fqk")
    for k in (1, 2, 3):
        small_z(k).wait_recv()
    r.fsum[...] = r.small[y, z] + r.zsm[1] + r.zsm[2] + r.zsm[3]
    r.lastf[...] = r.lastz[0] + r.lastz[1] + r.lastz[2] + r.lastz[3]
    r.fsum[0:1, :] = r.lastf[pl.ds(2 * z, 1), :]
    r.fsum[2:3, :] = r.lastf[pl.ds(2 * z + 1, 1), :]
    give("fsum")
    n_drain()
    l_drain()
    for make, cond in sent:
        when(cond, lambda make=make: make().wait_send())
    for code in (1, 2, 3):
        mix_copy(code).wait_send()
        k_copy(code).wait_send()
        v_copy(code).wait_send()
        q_copy(code).wait_send()
    for copy in given:
        copy.wait()


def emit_kernel(
    block_in, inputs_in, fup, fqk, fdy, fdz, fou, fsum,
    block_out, grad_inputs, gains, shifts, qkv, qv_bias, out, out_biases, up, up_bias, down,
    block_v, inputs_v, fup_v, fqk_v, fdy_v, fdz_v, fou_v, fsum_v, up_v, qkv_v, down_v, out_v, gains_v, shifts_v, qv_v, ob_v, ub_v, sems,
):
    count = []

    def begin(src, dst):
        count.append(pltpu.make_async_copy(src, dst, sems.at[len(count)]))
        count[-1].start()
        return count[-1]

    pairs = (
        (fdy, fdy_v), (fdz, fdz_v), (fup, fup_v), (inputs_in, inputs_v), (block_in, block_v), (fqk, fqk_v), (fou, fou_v),
        (fsum, fsum_v),
    )
    arrivals = [begin(src, dst) for src, dst in pairs]
    results = []
    arrivals[0].wait()
    arrivals[1].wait()
    for group in range(4):
        for j in range(6):
            place = (4 * j + group) * 128
            source, at = (fdy_v, j * 128) if j < 2 else (fdz_v, j * 128 - 256)
            down_v[:, place : place + 128] = source[group, :, at : at + 128].astype(F32)
    results.append(begin(down_v, down))
    arrivals[7].wait()
    for index, (ref, dst) in enumerate(((gains_v, gains), (shifts_v, shifts), (qv_v, qv_bias), (ob_v, out_biases))):
        ref[...] = fsum_v[2 * index : 2 * index + 2, 0:96]
        results.append(begin(ref, dst))
    ub_v[...] = fsum_v[8:11, :]
    results.append(begin(ub_v, up_bias))
    arrivals[2].wait()
    for i in range(3):
        up_v[:, i * 128 : (i + 1) * 128] = fup_v[i].astype(F32)
    results.append(begin(up_v, up))
    for arrival, src, dst in ((3, inputs_v, grad_inputs), (4, block_v, block_out)):
        arrivals[arrival].wait()
        results.append(begin(src, dst))
    arrivals[5].wait()
    qkv_v[...] = fqk_v[...].reshape(288, D).astype(F32)
    results.append(begin(qkv_v, qkv))
    arrivals[6].wait()
    for group in range(4):
        piece, lane = fou_v[group].astype(F32), group * 192
        out_v[:, lane : lane + 128] = piece[0:96]
        out_v[0:48, lane + 128 : lane + 192] = piece[96:144, 0:64]
        out_v[48:96, lane + 128 : lane + 192] = piece[96:144, 64:128]
    results.append(begin(out_v, out))
    for copy in results:
        copy.wait()


def per_device(x, norm_gains, norm_shifts, w_qkv, qv_bias, w_out, out_biases, w_up, up_bias, w_down, lengths, d_out):
    values = dict(
        x=x[0], gains=norm_gains, shifts=norm_shifts, w_qkv=w_qkv, qv_bias=qv_bias, w_out=w_out, biases=out_biases,
        w_up=w_up, up_bias=up_bias.reshape(24, 128), w_down=w_down, lengths=lengths, d_out=d_out[0],
    )
    place = {True: pl.BlockSpec(memory_space=pl.ANY), False: pl.BlockSpec(memory_space=pltpu.VMEM)}
    block_out, grad_inputs, fup, fqk, fdy, fdz, fou, fsum = pl.pallas_call(
        one_kernel,
        out_shape=[jax.ShapeDtypeStruct(shape, kind) for _, shape, kind in OUTPUTS],
        in_specs=[place[name in IN_PLACE] for name in INPUTS],
        out_specs=[place[True]] * len(OUTPUTS),
        scratch_shapes=[pltpu.VMEM(shape, kind) for _, shape, kind in OUTPUTS + BUFFERS]
        + [pltpu.SemaphoreType.DMA((count,)) for _, count in SEMAPHORES],
        compiler_params=pltpu.CompilerParams(
            collective_id=0, has_side_effects=True, vmem_limit_bytes=VMEM_LIMIT
        ),
        name="block",
    )(*(values[name] for name in INPUTS))
    anywhere = pl.BlockSpec(memory_space=pl.ANY)
    shapes = [(256, D), (256, D), (2, 96), (2, 96), (288, D), (2, 96), (96, D), (2, 96), (D, 384), (3, 128), (96, FF)]
    outs = pl.pallas_call(
        emit_kernel,
        out_shape=[jax.ShapeDtypeStruct(shape, F32 if n else BF) for n, shape in enumerate(shapes)],
        in_specs=[anywhere] * 8,
        out_specs=[anywhere] * len(shapes),
        scratch_shapes=[pltpu.VMEM(shape, kind) for _, shape, kind in OUTPUTS]
        + [pltpu.VMEM(shape, F32) for shape in ((D, 384), (288, D), (96, FF), (96, D))]
        + [pltpu.VMEM(shape, F32) for shape in ((2, 96),) * 4 + ((3, 128),)]
        + [pltpu.SemaphoreType.DMA((19,))],
        compiler_params=pltpu.CompilerParams(vmem_limit_bytes=VMEM_LIMIT),
        name="emit",
    )(block_out, grad_inputs, fup, fqk, fdy, fdz, fou, fsum)
    return (
        outs[0][None], outs[1][None], outs[2], outs[3], outs[4].T, outs[5], outs[6].T, outs[7], outs[8],
        outs[9].reshape(384), outs[10].T,
    )


def solution(mesh):
    split = P("dp", "head", None)
    placed = (split,) + (P(),) * 9 + (P("dp", None), split)
    return jax.shard_map(
        per_device if dict(mesh.shape) == {"dp": 8, "head": 4} else general_device,
        mesh=mesh,
        in_specs=placed,
        out_specs=(split, split) + (P(None, "dp"),) * 7 + (P("dp"), P(None, "dp")),
        check_vma=False,
    )
```
